16 devices in a mesh: col: 4 (over z, y), row: 4 (over x, core).
Axes of the slice: x: 2, y: 2, z: 2, core: 2. Of those that a mesh axis runs over, the one named last changes fastest.
Arguments:
- vel_u: float32 [31, 128, 2048], P(None, 'row', 'col')
- vel_v: float32 [31, 128, 2048], P(None, 'row', 'col')
- temperature: float32 [31, 128, 2048], P(None, 'row', 'col')
- salinity: float32 [31, 128, 2048], P(None, 'row', 'col')
- surf_eta: float32 [128, 2048], P('row', 'col')
- trans_u: float32 [128, 2048], P('row', 'col')
- trans_v: float32 [128, 2048], P('row', 'col')
- bottom_depth: float32 [128, 2048], P('row', 'col')
- level_count: int32 [128, 2048], P('row', 'col')
- avg_weights: float32 [30], replicated
Outputs:
- output 1: float32 [128, 2048], P('row', 'col')
- output 2: float32 [128, 2048], P('row', 'col')
- output 3: float32 [128, 2048], P('row', 'col')
- output 4: float32 [31, 128, 2048], P(None, 'row', 'col')
- output 5: float32 [31, 128, 2048], P(None, 'row', 'col')
- output 6: float32 [31, 128, 2048], P(None, 'row', 'col')
- output 7: float32 [31, 128, 2048], P(None, 'row', 'col')
All inputs are finite; a program needn't handle non-finite values.
Results may differ from the reference program's by a relative error of at most 0.001.
Values sent between devices are 32-bit elements.
A program may use at most 1 GiB of HBM per device.

```python
import jax
import jax.numpy as jnp
from jax import lax

LEVELS = 31
SUBCYCLES = 30
GRID_Y = 128
GRID_X = 2048

TIME_STEP = 1.0
GRAVITY = 16.0
BC_GRAVITY = 4.0
EXPAND_T = 0.2
CONTRACT_S = 0.6
CORIO_F0 = 0.4
CORIO_BETA = 0.4
VISC_R = 2.0
DIFF_R = 0.5


def setup_inputs(seed: int = 0) -> dict:
    keys = jax.random.split(jax.random.key(seed), 10)
    shape3 = (LEVELS, GRID_Y, GRID_X)
    shape2 = (GRID_Y, GRID_X)
    north_open = (jnp.arange(GRID_Y) < GRID_Y - 1).astype(jnp.float32)[:, None]
    vel_u = 0.3 * jax.random.normal(keys[0], shape3, jnp.float32)
    vel_v = 0.3 * jax.random.normal(keys[1], shape3, jnp.float32) * north_open
    temperature = jax.random.normal(keys[2], shape3, jnp.float32)
    salinity = 0.5 * jax.random.normal(keys[3], shape3, jnp.float32)
    surf_eta = 0.1 * jax.random.normal(keys[4], shape2, jnp.float32)
    trans_u = 0.3 * jax.random.normal(keys[5], shape2, jnp.float32)
    trans_v = 0.3 * jax.random.normal(keys[6], shape2, jnp.float32) * north_open
    bottom_depth = jax.random.uniform(keys[7], shape2, jnp.float32, 0.5, 1.5)
    level_count = jax.random.randint(keys[8], shape2, 1, LEVELS + 1, dtype=jnp.int32)
    level_count = level_count.at[0, 0].set(1).at[0, 1].set(LEVELS)
    ramp = (jnp.arange(SUBCYCLES) + 1.0) / SUBCYCLES
    raw_weights = ramp * jax.random.uniform(keys[9], (SUBCYCLES,), jnp.float32, 0.5, 1.5)
    avg_weights = raw_weights / jnp.sum(raw_weights)
    return {'vel_u': vel_u, 'vel_v': vel_v, 'temperature': temperature, 'salinity': salinity, 'surf_eta': surf_eta, 'trans_u': trans_u, 'trans_v': trans_v, 'bottom_depth': bottom_depth, 'level_count': level_count, 'avg_weights': avg_weights}


def pad_halo(field):
    wrapped = jnp.concatenate([field[..., -1:], field, field[..., :1]], axis=-1)
    ghost = jnp.zeros_like(wrapped[..., :1, :])
    return jnp.concatenate([ghost, wrapped, ghost], axis=-2)


def shifted(padded, step_y, step_x):
    n_rows = padded.shape[-2] - 2
    n_cols = padded.shape[-1] - 2
    return padded[..., 1 + step_y:1 + step_y + n_rows, 1 + step_x:1 + step_x + n_cols]


def tri_solve(right_side, active, strength):
    link = strength * active[1:]
    zero_row = jnp.zeros_like(right_side[:1])
    low_links = jnp.concatenate([zero_row, link], axis=0)
    up_links = jnp.concatenate([link, zero_row], axis=0)

    def down(carry, level):
        ratio_prev, value_prev = carry
        low_link, up_link, target = level
        denominator = 1.0 + low_link + up_link + low_link * ratio_prev
        ratio = -up_link / denominator
        value = (target + low_link * value_prev) / denominator
        return (ratio, value), (ratio, value)

    start = (jnp.zeros_like(right_side[0]), jnp.zeros_like(right_side[0]))
    _, (ratios, values) = lax.scan(down, start, (low_links, up_links, right_side))

    def back(below, level):
        ratio, value = level
        solved = value - ratio * below
        return solved, solved

    _, solved_all = lax.scan(back, jnp.zeros_like(right_side[0]), (ratios, values), reverse=True)
    return solved_all


def ocean_columns(u_pad, v_pad, temperature_pad, salinity_pad, count_pad, depth_pad, coriolis_u, coriolis_v):
    n_levels = u_pad.shape[0]
    count_mid = shifted(count_pad, 0, 0)
    levels_u = jnp.minimum(count_mid, shifted(count_pad, 0, 1))
    levels_uw = jnp.minimum(shifted(count_pad, 0, -1), count_mid)
    levels_v = jnp.minimum(count_mid, shifted(count_pad, 1, 0))
    levels_vs = jnp.minimum(shifted(count_pad, -1, 0), count_mid)
    level_index = jnp.arange(n_levels)[:, None, None]
    mask_mid = (level_index < count_mid).astype(jnp.float32)
    mask_u = (level_index < levels_u).astype(jnp.float32)
    mask_uw = (level_index < levels_uw).astype(jnp.float32)
    mask_v = (level_index < levels_v).astype(jnp.float32)
    mask_vs = (level_index < levels_vs).astype(jnp.float32)
    u_mid = shifted(u_pad, 0, 0)
    v_mid = shifted(v_pad, 0, 0)
    u_west = shifted(u_pad, 0, -1)
    v_south = shifted(v_pad, -1, 0)
    v_at_u = 0.25 * (v_mid + shifted(v_pad, 0, 1) + v_south + shifted(v_pad, -1, 1))
    u_at_v = 0.25 * (u_mid + u_west + shifted(u_pad, 1, 0) + shifted(u_pad, 1, -1))
    inertia_u = 0.5 * (u_mid * (shifted(u_pad, 0, 1) - u_west) + v_at_u * (shifted(u_pad, 1, 0) - shifted(u_pad, -1, 0)))
    inertia_v = 0.5 * (u_at_v * (shifted(v_pad, 0, 1) - shifted(v_pad, 0, -1)) + v_mid * (shifted(v_pad, 1, 0) - v_south))
    density = CONTRACT_S * salinity_pad - EXPAND_T * temperature_pad
    pressure = (BC_GRAVITY / n_levels) * (jnp.cumsum(density, axis=0) - 0.5 * density)
    pressure_mid = shifted(pressure, 0, 0)
    u_star = u_mid + TIME_STEP * (coriolis_u * v_at_u - inertia_u - shifted(pressure, 0, 1) + pressure_mid)
    v_star = v_mid + TIME_STEP * (-coriolis_v * u_at_v - inertia_v - shifted(pressure, 1, 0) + pressure_mid)
    u_visc = tri_solve(u_star, mask_u, VISC_R)
    v_visc = tri_solve(v_star, mask_v, VISC_R)
    count_u = jnp.maximum(jnp.sum(mask_u, axis=0), 1.0)
    count_v = jnp.maximum(jnp.sum(mask_v, axis=0), 1.0)
    depth_mid = shifted(depth_pad, 0, 0)
    depth_u = 0.5 * (depth_mid + shifted(depth_pad, 0, 1))
    depth_v = 0.5 * (depth_mid + shifted(depth_pad, 1, 0))
    force_u = depth_u * jnp.sum(mask_u * (u_visc - u_mid), axis=0) / count_u / TIME_STEP
    force_v = depth_v * jnp.sum(mask_v * (v_visc - v_mid), axis=0) / count_v / TIME_STEP
    shear_u = u_visc - jnp.sum(mask_u * u_visc, axis=0) / count_u
    shear_v = v_visc - jnp.sum(mask_v * v_visc, axis=0) / count_v
    wet_u = (levels_u > 0).astype(jnp.float32)
    wet_v = (levels_v > 0).astype(jnp.float32)

    def advect(tracer_pad):
        tracer_mid = shifted(tracer_pad, 0, 0)
        flux_east = mask_u * u_mid * (tracer_mid + shifted(tracer_pad, 0, 1))
        flux_west = mask_uw * u_west * (shifted(tracer_pad, 0, -1) + tracer_mid)
        flux_north = mask_v * v_mid * (tracer_mid + shifted(tracer_pad, 1, 0))
        flux_south = mask_vs * v_south * (shifted(tracer_pad, -1, 0) + tracer_mid)
        return tracer_mid - 0.5 * TIME_STEP * (flux_east - flux_west + flux_north - flux_south)

    temperature_new = tri_solve(advect(temperature_pad), mask_mid, DIFF_R)
    salinity_new = tri_solve(advect(salinity_pad), mask_mid, DIFF_R)
    return (shear_u, shear_v, mask_u, mask_v, depth_u, depth_v, wet_u, wet_v, force_u, force_v, temperature_new, salinity_new)


def fast_update(stack_pad, force_u, force_v, depth_u, depth_v, wet_u, wet_v, coriolis_u, coriolis_v, dt_fast):
    eta_pad = stack_pad[0]
    trans_u_pad = stack_pad[1]
    trans_v_pad = stack_pad[2]
    eta_ext = eta_pad[1:, 1:] - dt_fast * (trans_u_pad[1:, 1:] - trans_u_pad[1:, :-1] + trans_v_pad[1:, 1:] - trans_v_pad[:-1, 1:])
    eta_new = eta_ext[:-1, :-1]
    trans_u_old = shifted(trans_u_pad, 0, 0)
    trans_v_old = shifted(trans_v_pad, 0, 0)
    v_at_u = 0.25 * (trans_v_old + shifted(trans_v_pad, 0, 1) + shifted(trans_v_pad, -1, 0) + shifted(trans_v_pad, -1, 1))
    u_at_v = 0.25 * (trans_u_old + shifted(trans_u_pad, 0, -1) + shifted(trans_u_pad, 1, 0) + shifted(trans_u_pad, 1, -1))
    trans_u_new = wet_u * (trans_u_old + dt_fast * (coriolis_u * v_at_u + force_u - GRAVITY * depth_u * (eta_ext[:-1, 1:] - eta_new)))
    trans_v_new = wet_v * (trans_v_old + dt_fast * (force_v - coriolis_v * u_at_v - GRAVITY * depth_v * (eta_ext[1:, :-1] - eta_new)))
    return eta_new, trans_u_new, trans_v_new


def reference(vel_u, vel_v, temperature, salinity, surf_eta, trans_u, trans_v, bottom_depth, level_count, avg_weights):
    n_rows = surf_eta.shape[0]
    dt_fast = TIME_STEP / avg_weights.shape[0]
    row_pos = jnp.arange(n_rows).astype(jnp.float32)[:, None]
    coriolis_u = CORIO_F0 + CORIO_BETA * ((row_pos + 0.5) / n_rows - 0.5)
    coriolis_v = CORIO_F0 + CORIO_BETA * ((row_pos + 1.0) / n_rows - 0.5)
    columns = ocean_columns(pad_halo(vel_u), pad_halo(vel_v), pad_halo(temperature), pad_halo(salinity), pad_halo(level_count), pad_halo(bottom_depth), coriolis_u, coriolis_v)
    shear_u, shear_v, mask_u, mask_v, depth_u, depth_v, wet_u, wet_v, force_u, force_v, temperature_new, salinity_new = columns

    def subcycle(carry, weight):
        eta_old, trans_u_old, trans_v_old, acc_u, acc_v = carry
        stack_pad = pad_halo(jnp.stack([eta_old, trans_u_old, trans_v_old]))
        eta_new, trans_u_new, trans_v_new = fast_update(stack_pad, force_u, force_v, depth_u, depth_v, wet_u, wet_v, coriolis_u, coriolis_v, dt_fast)
        return (eta_new, trans_u_new, trans_v_new, acc_u + weight * trans_u_new, acc_v + weight * trans_v_new), None

    zero_field = jnp.zeros_like(surf_eta)
    final, _ = lax.scan(subcycle, (surf_eta, trans_u, trans_v, zero_field, zero_field), avg_weights)
    eta_fin, trans_u_fin, trans_v_fin, bar_u, bar_v = final
    vel_u_new = mask_u * (shear_u + bar_u / depth_u)
    vel_v_new = mask_v * (shear_v + bar_v / depth_v)
    return (eta_fin, trans_u_fin, trans_v_fin, vel_u_new, vel_v_new, temperature_new, salinity_new)
```

```python
import functools

import jax
import jax.numpy as jnp
import numpy as np
from jax import lax
from jax.experimental import pallas as pl
from jax.experimental.pallas import tpu as pltpu
from jax.sharding import PartitionSpec as P

TIME_STEP = 1.0
GRAVITY = 16.0
BC_GRAVITY = 4.0
EXPAND_T = 0.2
CONTRACT_S = 0.6
CORIO_F0 = 0.4
CORIO_BETA = 0.4
VISC_R = 2.0
DIFF_R = 0.5

LEV = 31
SLOT = 32
NR = 32
NC = 512
NT = 4
L = 128
R0 = 8
PR = 48
XR = 112
XO = 40
MESH = pl.DeviceIdType.MESH
f32 = jnp.float32


def solve_table(n_levels):
    rows = []
    for s in (VISC_R, DIFF_R):
        scale, carry, link, last = np.zeros((4, SLOT))
        ratio = 0.0
        for k in range(n_levels):
            low = s if k else 0.0
            full = 1.0 + low + s - low * ratio
            end = 1.0 + low - low * ratio
            scale[k], carry[k], link[k], last[k] = 1.0 / full, low / full, s / full, full / end
            ratio = s / full
        rows += [scale, carry, link, last]
    return np.concatenate(rows).astype(np.float32)


def ocean_kernel(axes, n_col, n_row, n_sub, *refs):
    (u_h, v_h, t_h, s_h, eta_h, tu_h, tv_h, dep_h, cnt_h, w_s, tab_s,
     eta_o, tu_o, tv_o, gu_o, gv_o, cu_o, cv_o, cc_o, xu_o, xv_o, xt_o, xs_o,
     bu, bv, bt, bs, xu, xv, xt, xs, cnt_i, pc, pp, ce,
     pw, pe, rw, re, x, xf, qw, qe, we, ww, fw, fe, fre, frw,
     fu4, fv4, cu, cv, cvs, hu, hv, su, sv,
     ca, cb, cc, cd, cg, ch, cm, cn, tt, ss, au, av,
     lsem, ssem, rsem, osem) = refs
    col = lax.axis_index('col')
    row = lax.axis_index('row')
    east = lax.rem(col + 1, n_col)
    west = lax.rem(col + n_col - 1, n_col)
    has_s = row > 0
    has_n = row < n_row - 1

    def dev(c, r):
        at = {'col': c, 'row': r}
        return tuple(at[name] for name in axes)

    bufs = (bu, bv, bt, bs)
    loads = []
    for f, (src, dst) in enumerate(zip((u_h, v_h, t_h, s_h), bufs)):
        for t in range(NT):
            loads.append(pltpu.make_async_copy(src.at[:, :, L * t:L * t + L], dst.at[t, 0:LEV, R0:R0 + NR, :], lsem.at[len(loads)]))
    flat_loads = []
    for f, src in enumerate((eta_h, tu_h, tv_h)):
        for t in range(NT):
            flat_loads.append(pltpu.make_async_copy(src.at[:, L * t:L * t + L], x.at[f, t, XO:XO + NR, :], lsem.at[len(loads) + len(flat_loads)]))
    for t in range(NT):
        flat_loads.append(pltpu.make_async_copy(dep_h.at[:, L * t:L * t + L], bv.at[t, LEV, R0:R0 + NR, :], lsem.at[len(loads) + len(flat_loads)]))
    for t in range(NT):
        flat_loads.append(pltpu.make_async_copy(cnt_h.at[:, L * t:L * t + L], cnt_i.at[t], lsem.at[len(loads) + len(flat_loads)]))
    for cp in flat_loads + loads:
        cp.start()

    zero = functools.partial(jnp.zeros, dtype=f32)
    for f in range(4):
        for t in range(NT + 1):
            x[f, t, 0:8, :] = zero((8, L))
            x[f, t, XR - 8:XR, :] = zero((8, L))
    for t in range(NT + 1):
        tt[t, XR - 8:XR, :] = zero((8, L))
    for t in range(NT):
        bt[t, LEV, R0:R0 + NR, :] = zero((NR, L))
        bs[t, LEV, R0:R0 + NR, :] = zero((NR, L))
        for a in (xu, xv, xt, xs):
            a[t, 0] = zero((NR, L))

    @pl.when(jnp.logical_not(has_s))
    def _():
        for b in bufs:
            b[:, :, R0 - 8:R0, :] = zero((NT, SLOT, 8, L))
        re[R0 - 8:R0, :] = zero((8, L))
        x[:, 0:NT, 8:XO, :] = zero((4, NT, NR, L))
        xf[:, 0:NT, 8:XO, :] = zero((2, NT, NR, L))
        for a in (we, ww, fre, frw):
            a[0] = zero((NR, L))

    @pl.when(jnp.logical_not(has_n))
    def _():
        for b in bufs:
            b[:, :, R0 + NR:PR, :] = zero((NT, SLOT, 8, L))
        rw[R0 + NR:PR, :] = zero((8, L))
        x[:, 0:NT, XO + NR:XO + 2 * NR, :] = zero((4, NT, NR, L))
        xf[:, 0:NT, XO + NR:XO + 2 * NR, :] = zero((2, NT, NR, L))
        for a in (we, ww, fre, frw):
            a[2] = zero((NR, L))

    barrier = pltpu.get_barrier_semaphore()

    def signal(c, r):
        pl.semaphore_signal(barrier, inc=1, device_id=dev(c, r), device_id_type=MESH)

    signal(west, row)
    signal(east, row)

    @pl.when(has_s)
    def _():
        for c in (west, col, east):
            signal(c, row - 1)

    @pl.when(has_n)
    def _():
        for c in (west, col, east):
            signal(c, row + 1)

    edge = jnp.logical_or(row == 0, row == n_row - 1)

    @pl.when(edge)
    def _():
        pl.semaphore_wait(barrier, 5)

    @pl.when(jnp.logical_not(edge))
    def _():
        pl.semaphore_wait(barrier, 8)

    n_copies = 0

    def remote(src, dst, c, r, sends, receives):
        nonlocal n_copies
        i = n_copies
        n_copies += 1
        return (pltpu.make_async_remote_copy(src, dst, ssem.at[i], rsem.at[i], device_id=dev(c, r), device_id_type=MESH), sends, receives)

    def maybe(cond, fn):
        if cond is None:
            fn()
        else:
            pl.when(cond)(fn)

    def start(group):
        for cp, sends, _ in group:
            maybe(sends, cp.start)

    def arrive(group):
        for cp, _, receives in group:
            maybe(receives, cp.wait_recv)

    def drain(group):
        for cp, sends, _ in group:
            maybe(sends, cp.wait_send)

    def rows_of(b):
        return [remote(b.at[:, :, R0 + NR - 1:R0 + NR, :], b.at[:, :, R0 - 1:R0, :], col, row + 1, has_n, has_s),
                remote(b.at[:, :, R0:R0 + 1, :], b.at[:, :, R0 + NR:R0 + NR + 1, :], col, row - 1, has_s, has_n)]

    def wide_of(b, lanes_w, lanes_e, from_e, from_w):
        own = b.at[:, 0:NT, XO:XO + NR, :]
        return [remote(own, b.at[:, 0:NT, 8:XO, :], col, row + 1, has_n, has_s),
                remote(own, b.at[:, 0:NT, XO + NR:XO + 2 * NR, :], col, row - 1, has_s, has_n),
                remote(lanes_w, from_e.at[1], west, row, None, None),
                remote(lanes_e, from_w.at[1], east, row, None, None),
                remote(lanes_w, from_e.at[2], west, row - 1, has_s, has_n),
                remote(lanes_e, from_w.at[2], east, row - 1, has_s, has_n),
                remote(lanes_w, from_e.at[0], west, row + 1, has_n, has_s),
                remote(lanes_e, from_w.at[0], east, row + 1, has_n, has_s)]

    row_group = rows_of(bu) + rows_of(bv) + rows_of(bt) + rows_of(bs)
    lane_group = [remote(pw, re.at[R0:R0 + NR, :], west, row, None, None),
                  remote(pe, rw.at[R0:R0 + NR, :], east, row, None, None),
                  remote(pe.at[0:1, :], rw.at[R0 + NR:R0 + NR + 1, :], east, row - 1, has_s, has_n),
                  remote(pw.at[NR - 1:NR, :], re.at[R0 - 1:R0, :], west, row + 1, has_n, has_s)]
    wide_group = wide_of(x, qw, qe, we, ww)
    force_group = wide_of(xf, fw, fe, fre, frw)

    lane = lax.broadcasted_iota(jnp.int32, (NR, L), 1)

    for cp in flat_loads:
        cp.wait()
    for t in range(NT):
        count = cnt_i[t].astype(f32)
        bu[t, LEV, R0:R0 + NR, :] = count
        x[3, t, XO:XO + NR, :] = jnp.where(count > 0.0, bv[t, LEV, R0:R0 + NR, :], 0.0)

    def roll(a, shift):
        return pltpu.roll(a, shift, 1) if not (isinstance(shift, int) and shift % L == 0) else a

    def pack_wide(b, n_fields):
        first = last = zero((NR, L))
        for f in range(n_fields):
            mine = (lane >= 32 * f) & (lane < 32 * f + 32)
            first = jnp.where(mine, roll(b[f, 0, XO:XO + NR, :], 32 * f), first)
            last = jnp.where(mine, roll(b[f, NT - 1, XO:XO + NR, :], (32 * f + 32) % L), last)
        return first, last

    first, last = pack_wide(x, 4)
    qw[...] = first
    qe[...] = last

    for cp in loads:
        cp.wait()
    first = last = zero((NR, L))
    for f, b in enumerate(bufs):
        for k in range(SLOT):
            p = SLOT * f + k
            first = jnp.where(lane == p, roll(b[0, k, R0:R0 + NR, :], p), first)
            last = jnp.where(lane == p, roll(b[NT - 1, k, R0:R0 + NR, :], (p + 1) % L), last)
    pw[...] = first
    pe[...] = last
    start(row_group)
    start(lane_group)
    start(wide_group)

    row_pos = (row * NR + lax.broadcasted_iota(jnp.int32, (NR, L), 0)).astype(f32)
    total_rows = NR * n_row
    fu4[...] = 0.25 * (CORIO_F0 + CORIO_BETA * ((row_pos + 0.5) / total_rows - 0.5))
    fv4[...] = 0.25 * (CORIO_F0 + CORIO_BETA * ((row_pos + 1.0) / total_rows - 0.5))

    def to_east(tiles, halo):
        rolled = [roll(a, L - 1) for a in tiles] + [halo]
        return [jnp.where(lane == L - 1, rolled[t + 1], rolled[t]) for t in range(NT)]

    def to_west(tiles, halo):
        rolled = [halo] + [roll(a, 1) for a in tiles]
        return [jnp.where(lane == 0, rolled[t], rolled[t + 1]) for t in range(NT)]

    def east_lane(f, k, lo=R0):
        return pltpu.roll(re[lo:lo + NR, :], L - 1 - (SLOT * f + k), 1)

    def west_lane(f, k, lo=R0):
        return pltpu.roll(rw[lo:lo + NR, :], lax.rem(L - (SLOT * f + k), L), 1)

    arrive(row_group)
    arrive(lane_group)

    def level(b, k, lo=R0):
        return [b[t, k, lo:lo + NR, :] for t in range(NT)]

    c_mid, d_mid = level(bu, LEV), level(bv, LEV)
    c_east = to_east(c_mid, east_lane(0, LEV))
    d_east = to_east(d_mid, east_lane(1, LEV))
    c_north, c_south = level(bu, LEV, R0 + 1), level(bu, LEV, R0 - 1)
    d_north = level(bv, LEV, R0 + 1)
    for t in range(NT):
        cu[t] = jnp.minimum(c_mid[t], c_east[t])
        cv[t] = jnp.minimum(c_mid[t], c_north[t])
        cvs[t] = jnp.minimum(c_mid[t], c_south[t])
        hu[t] = 0.5 * (d_mid[t] + d_east[t])
        hv[t] = 0.5 * (d_mid[t] + d_north[t])
        cu_o[t] = jnp.minimum(c_mid[t], c_east[t])
        cv_o[t] = jnp.minimum(c_mid[t], c_north[t])
        cc_o[t] = c_mid[t]

    for t in range(NT):
        pc[t] = zero((NR + 8, L))
    ce[...] = zero((NR, L))
    p_scale = BC_GRAVITY / LEV

    def momentum_down(k, _):
        prev = jnp.maximum(k - 1, 0)
        scale, carry = tab_s[k], tab_s[SLOT + k]
        um, un, us = level(bu, k), level(bu, k, R0 + 1), level(bu, k, R0 - 1)
        vm, vn, vs = level(bv, k), level(bv, k, R0 + 1), level(bv, k, R0 - 1)
        ue = to_east(um, east_lane(0, k))
        uw = to_west(um, west_lane(0, k))
        unw = to_west(un, west_lane(0, k, R0 + 1))
        ve = to_east(vm, east_lane(1, k))
        vw = to_west(vm, west_lane(1, k))
        vse = to_east(vs, east_lane(1, k, R0 - 1))
        pm = []
        for t in range(NT):
            density = CONTRACT_S * bs[t, k, R0:PR, :] - EXPAND_T * bt[t, k, R0:PR, :]
            total = pc[t] + density
            pc[t] = total
            pressure = p_scale * (total - 0.5 * density)
            pp[t] = pressure
            pm.append(pressure[:NR])
        density = CONTRACT_S * east_lane(3, k) - EXPAND_T * east_lane(2, k)
        total = ce[...] + density
        ce[...] = total
        pe_ = to_east(pm, p_scale * (total - 0.5 * density))
        for t in range(NT):
            pn = pp[t, 1:NR + 1, :]
            vb4 = (vm[t] + ve[t]) + (vs[t] + vse[t])
            ub4 = (um[t] + uw[t]) + (un[t] + unw[t])
            u_star = um[t] + vb4 * (fu4[...] - 0.125 * (un[t] - us[t])) - um[t] * (0.5 * (ue[t] - uw[t])) + (pm[t] - pe_[t])
            v_star = vm[t] - ub4 * (fv4[...] + 0.125 * (ve[t] - vw[t])) - vm[t] * (0.5 * (vn[t] - vs[t])) + (pm[t] - pn)
            xu[t, k] = scale * u_star + carry * xu[t, prev]
            xv[t, k] = scale * v_star + carry * xv[t, prev]
        return 0

    lax.fori_loop(0, LEV, momentum_down, 0)

    for t in range(NT):
        def momentum_up(i, state, t=t):
            k = LEV - 1 - i
            link, last_ = tab_s[2 * SLOT + k], tab_s[3 * SLOT + k]
            kf = k.astype(f32)
            out = []
            for sweep, b, count, (below, sum_x, sum_0) in ((xu, bu, cu, state[:3]), (xv, bv, cv, state[3:])):
                value = sweep[t, k]
                active = count[t] > kf
                solved = jnp.where(count[t] > kf + 1.0, value + link * below, jnp.where(active, last_ * value, 0.0))
                sweep[t, k] = solved
                out += [solved, sum_x + solved, sum_0 + jnp.where(active, b[t, k, R0:R0 + NR, :], 0.0)]
            return tuple(out)

        z = zero((NR, L))
        _, ux, u0, _, vx, v0 = lax.fori_loop(0, LEV, momentum_up, (z,) * 6)
        for q, h, mean, count, total, start_ in ((0, hu, su, cu, ux, u0), (1, hv, sv, cv, vx, v0)):
            n_active = jnp.maximum(count[t], 1.0)
            mean[t] = total / n_active
            xf[q, t, XO:XO + NR, :] = h[t] * (total - start_) / n_active / TIME_STEP

    stores = [pltpu.make_async_copy(a, o, osem.at[i]) for i, (a, o) in enumerate(((xu, xu_o), (xv, xv_o), (xt, xt_o), (xs, xs_o)))]
    first, last = pack_wide(xf, 2)
    fw[...] = first
    fe[...] = last
    start(force_group)
    stores[0].start()
    stores[1].start()

    c_west0 = jnp.minimum(west_lane(0, LEV), bu[0, LEV, R0:R0 + NR, :])

    def tracer_down(k, _):
        prev = jnp.maximum(k - 1, 0)
        scale, carry = tab_s[4 * SLOT + k], tab_s[5 * SLOT + k]
        kf = k.astype(f32)
        um = [jnp.where(cu[t] > kf, bu[t, k, R0:R0 + NR, :], 0.0) for t in range(NT)]
        vm = [jnp.where(cv[t] > kf, bv[t, k, R0:R0 + NR, :], 0.0) for t in range(NT)]
        vs = [jnp.where(cvs[t] > kf, bv[t, k, R0 - 1:R0 - 1 + NR, :], 0.0) for t in range(NT)]
        uw0 = jnp.where(c_west0 > kf, west_lane(0, k), 0.0)
        for f, b, sweep in ((2, bt, xt), (3, bs, xs)):
            q = level(b, k)
            qe_ = to_east(q, east_lane(f, k))
            f_east = [um[t] * (q[t] + qe_[t]) for t in range(NT)]
            f_west = to_west(f_east, uw0 * (west_lane(f, k) + q[0]))
            for t in range(NT):
                f_north = vm[t] * (q[t] + b[t, k, R0 + 1:R0 + 1 + NR, :])
                f_south = vs[t] * (b[t, k, R0 - 1:R0 - 1 + NR, :] + q[t])
                new = q[t] - 0.5 * TIME_STEP * (f_east[t] - f_west[t] + f_north - f_south)
                sweep[t, k] = jnp.where(bu[t, LEV, R0:R0 + NR, :] > kf, scale * new + carry * sweep[t, prev], new)
        return 0

    lax.fori_loop(0, LEV, tracer_down, 0)
    stores[2].start()
    stores[3].start()

    arrive(wide_group)
    drain(wide_group)
    arrive(force_group)

    def unpack_wide(b, from_e, from_w, n_fields):
        for f in range(n_fields):
            for seg in range(3):
                b[f, NT, 8 + NR * seg:8 + NR * seg + NR, :] = jnp.where(lane < L // 2, roll(from_e[seg], (L - 32 * f) % L), roll(from_w[seg], (96 - 32 * f) % L))

    unpack_wide(x, we, ww, 4)
    unpack_wide(xf, fre, frw, 2)
    dt_fast = TIME_STEP / n_sub
    XT = NT + 1

    def ring_east(tiles, last_lane):
        rolled = [roll(a, L - 1) for a in tiles]
        return [jnp.where(last_lane, rolled[(t + 1) % XT], rolled[t]) for t in range(XT)]

    def ring_west(tiles, first_lane):
        rolled = [roll(a, 1) for a in tiles]
        return [jnp.where(first_lane, rolled[(t - 1) % XT], rolled[t]) for t in range(XT)]

    for seg in range(3):
        lo = 8 + NR * seg
        pos = (row * NR + NR * (seg - 1) + lax.broadcasted_iota(jnp.int32, (NR, L), 0)).astype(f32)
        f_u = CORIO_F0 + CORIO_BETA * ((pos + 0.5) / total_rows - 0.5)
        f_v = CORIO_F0 + CORIO_BETA * ((pos + 1.0) / total_rows - 0.5)
        d = [x[3, t, lo:lo + NR, :] for t in range(XT)]
        d_e = ring_east(d, lane == L - 1)
        for t in range(XT):
            d_n = x[3, t, lo + 1:lo + 1 + NR, :]
            wet = jnp.where((d[t] > 0.0) & (d_e[t] > 0.0), 1.0, 0.0)
            cm[t, lo:lo + NR, :] = wet
            ca[t, lo:lo + NR, :] = (0.25 * dt_fast) * f_u * wet
            cb[t, lo:lo + NR, :] = (dt_fast * GRAVITY * 0.5) * (d[t] + d_e[t]) * wet
            cc[t, lo:lo + NR, :] = dt_fast * xf[0, t, lo:lo + NR, :] * wet
            wet = jnp.where((d[t] > 0.0) & (d_n > 0.0), 1.0, 0.0)
            cn[t, lo:lo + NR, :] = wet
            cd[t, lo:lo + NR, :] = (0.25 * dt_fast) * f_v * wet
            cg[t, lo:lo + NR, :] = (dt_fast * GRAVITY * 0.5) * (d[t] + d_n) * wet
            ch[t, lo:lo + NR, :] = dt_fast * xf[1, t, lo:lo + NR, :] * wet

    for t in range(NT):
        au[t] = zero((NR, L))
        av[t] = zero((NR, L))

    def subcycle(lo, hi, chunk, n, _):
        lane_c = lax.broadcasted_iota(jnp.int32, (chunk, L), 1)
        first_lane, last_lane = lane_c == 0, lane_c == L - 1
        weight = w_s[n]
        for r in range(lo, hi, chunk):
            u_t = [x[1, t, r:r + chunk, :] for t in range(XT)]
            u_w = ring_west(u_t, first_lane)
            for t in range(XT):
                v_t, v_s = x[2, t, r:r + chunk, :], x[2, t, r - 1:r - 1 + chunk, :]
                x[0, t, r:r + chunk, :] = x[0, t, r:r + chunk, :] - dt_fast * ((u_t[t] - u_w[t]) + (v_t - v_s))
                tt[t, r:r + chunk, :] = u_t[t] + u_w[t]
                ss[t, r:r + chunk, :] = v_t + v_s
        for r in range(lo, hi, chunk):
            e_t = [x[0, t, r:r + chunk, :] for t in range(XT)]
            e_e = ring_east(e_t, last_lane)
            s_t = [ss[t, r:r + chunk, :] for t in range(XT)]
            s_e = ring_east(s_t, last_lane)
            for t in range(XT):
                at = (t, slice(r, r + chunk))
                up = (t, slice(r + 1, r + 1 + chunk))
                e_n = x[0, t, r + 1:r + 1 + chunk, :]
                x[1, t, r:r + chunk, :] = cm[at] * x[1, t, r:r + chunk, :] + ca[at] * (s_t[t] + s_e[t]) + cc[at] - cb[at] * (e_e[t] - e_t[t])
                x[2, t, r:r + chunk, :] = cn[at] * x[2, t, r:r + chunk, :] - cd[at] * (tt[at] + tt[up]) + ch[at] - cg[at] * (e_n - e_t[t])
        for t in range(NT):
            au[t] += weight * x[1, t, XO:XO + NR, :]
            av[t] += weight * x[2, t, XO:XO + NR, :]
        return 0

    done = 0
    for side in (4, 3, 2, 1):
        until = n_sub - 8 * (side - 1)
        rows = NR + 16 * side
        chunk = {4: 32, 3: 40, 2: 32, 1: 24}[side]
        lax.fori_loop(done, until, functools.partial(subcycle, XO - 8 * side, XO - 8 * side + rows, chunk), 0)
        done = until

    for t in range(NT):
        cols = slice(L * t, L * t + L)
        eta_o[:, cols] = x[0, t, XO:XO + NR, :]
        tu_o[:, cols] = x[1, t, XO:XO + NR, :]
        tv_o[:, cols] = x[2, t, XO:XO + NR, :]
        gu_o[t] = au[t] / hu[t] - su[t]
        gv_o[t] = av[t] / hv[t] - sv[t]

    for group in (row_group, lane_group, force_group):
        drain(group)
    for cp in stores:
        cp.wait()


def final_kernel(tab_s, xu, xv, xt, xs, gu, gv, cu, cv, cc, u_o, v_o, t_o, s_o):
    rows = u_o.shape[1]
    g_u, g_v, c_u, c_v, c_c = gu[0], gv[0], cu[0], cv[0], cc[0]

    def up(i, state):
        k = LEV - 1 - i
        kf = k.astype(f32)
        link, last = tab_s[6 * SLOT + k], tab_s[7 * SLOT + k]
        u_o[k] = jnp.where(c_u > kf, xu[0, k] + g_u, 0.0)
        v_o[k] = jnp.where(c_v > kf, xv[0, k] + g_v, 0.0)
        inner, active = c_c > kf + 1.0, c_c > kf
        out = []
        for sweep, o, below in ((xt, t_o, state[0]), (xs, s_o, state[1])):
            value = sweep[0, k]
            solved = jnp.where(inner, value + link * below, jnp.where(active, last * value, value))
            o[k] = solved
            out.append(solved)
        return tuple(out)

    z = jnp.zeros((rows, L), f32)
    lax.fori_loop(0, LEV, up, (z, z))


def solution(mesh):
    n_col = mesh.shape['col']
    n_row = mesh.shape['row']

    def step(vel_u, vel_v, value_a11, salinity, surf_eta, trans_u, trans_v, bottom_depth, level_count, avg_weights):
        n_sub = avg_weights.shape[0]
        table = jnp.asarray(solve_table(LEV))
        hbm = pl.BlockSpec(memory_space=pl.ANY)
        vmem = pl.BlockSpec(memory_space=pltpu.VMEM)
        smem = pl.BlockSpec(memory_space=pltpu.SMEM)
        flat = jax.ShapeDtypeStruct((NR, NC), f32)
        tile = jax.ShapeDtypeStruct((NT, NR, L), f32)
        sweep = jax.ShapeDtypeStruct((NT, SLOT, NR, L), f32)
        V = pltpu.VMEM
        wide = (NT + 1, XR, L)
        scratch = ([V((NT, SLOT, PR, L), f32)] * 4 + [V((NT, SLOT, NR, L), f32)] * 4
                   + [V((NT, NR, L), jnp.int32), V((NT, NR + 8, L), f32), V((NT, NR + 8, L), f32), V((NR, L), f32)]
                   + [V((NR, L), f32)] * 2 + [V((PR, L), f32)] * 2
                   + [V((4,) + wide, f32), V((2,) + wide, f32)] + [V((NR, L), f32)] * 2 + [V((3, NR, L), f32)] * 2
                   + [V((NR, L), f32)] * 2 + [V((3, NR, L), f32)] * 2
                   + [V((NR, L), f32)] * 2 + [V((NT, NR, L), f32)] * 7
                   + [V(wide, f32)] * 10 + [V((NT, NR, L), f32)] * 2
                   + [pltpu.SemaphoreType.DMA((40,)), pltpu.SemaphoreType.DMA((28,)), pltpu.SemaphoreType.DMA((28,)), pltpu.SemaphoreType.DMA((4,))])
        outs = pl.pallas_call(
            functools.partial(ocean_kernel, tuple(mesh.axis_names), n_col, n_row, n_sub),
            out_shape=[flat] * 3 + [tile] * 5 + [sweep] * 4,
            in_specs=[hbm] * 9 + [smem] * 2,
            out_specs=[vmem] * 8 + [hbm] * 4,
            scratch_shapes=scratch,
            compiler_params=pltpu.CompilerParams(collective_id=0, has_side_effects=True, vmem_limit_bytes=56 * 1024 * 1024),
        )(vel_u, vel_v, value_a11, salinity, surf_eta, trans_u, trans_v, bottom_depth, level_count, avg_weights, table)
        eta, tu, tv, gu, gv, cu, cv, cc, xu, xv, xt, xs = outs

        part = 16
        big = pl.BlockSpec((1, SLOT, part, L), lambda t, r: (t, 0, r, 0))
        small = pl.BlockSpec((1, part, L), lambda t, r: (t, r, 0))
        out = pl.BlockSpec((LEV, part, L), lambda t, r: (0, r, t))
        cube = jax.ShapeDtypeStruct((LEV, NR, NC), f32)
        u_new, v_new, t_new, s_new = pl.pallas_call(
            final_kernel,
            grid=(NT, NR // part),
            out_shape=[cube] * 4,
            in_specs=[smem] + [big] * 4 + [small] * 5,
            out_specs=[out] * 4,
        )(table, xu, xv, xt, xs, gu, gv, cu, cv, cc)
        return (eta, tu, tv, u_new, v_new, t_new, s_new)

    cube = P(None, 'row', 'col')
    flat = P('row', 'col')
    return jax.shard_map(step, mesh=mesh, in_specs=(cube, cube, cube, cube, flat, flat, flat, flat, flat, P()), out_specs=(flat, flat, flat, cube, cube, cube, cube), check_vma=False)
```

```python
import functools

import jax
import jax.numpy as jnp
import numpy as np
from jax import lax
from jax.experimental import pallas as pl
from jax.experimental.pallas import tpu as pltpu
from jax.sharding import PartitionSpec as P

TIME_STEP = 1.0
GRAVITY = 16.0
BC_GRAVITY = 4.0
EXPAND_T = 0.2
CONTRACT_S = 0.6
CORIO_F0 = 0.4
CORIO_BETA = 0.4
VISC_R = 2.0
DIFF_R = 0.5

LEV = 31
SLOT = 32
NR = 32
NC = 512
NT = 4
L = 128
R0 = 8
PR = 48
XR = 112
XO = 40
MESH = pl.DeviceIdType.MESH
f32 = jnp.float32
UNROLL = 4


def solve_table(n_levels):
    rows = []
    for s in (VISC_R, DIFF_R):
        scale, carry, link, last = np.zeros((4, SLOT))
        ratio = 0.0
        for k in range(n_levels):
            low = s if k else 0.0
            full = 1.0 + low + s - low * ratio
            end = 1.0 + low - low * ratio
            scale[k], carry[k], link[k], last[k] = 1.0 / full, low / full, s / full, full / end
            ratio = s / full
        rows += [scale, carry, link, last]
    return np.concatenate(rows).astype(np.float32)


def ocean_kernel(axes, n_col, n_row, n_sub, *refs):
    (u_h, v_h, t_h, s_h, eta_h, tu_h, tv_h, dep_h, cnt_h, w_h, tab_h,
     eta_o, tu_o, tv_o, gu_o, gv_o, cu_o, cv_o, cc_o, xu_o, xv_o, xt_o, xs_o,
     bu, bv, bt, bs, xu, xv, xt, xs, cnt_i, pc, pp, ce,
     pw, pe, rw, re, x, xf, qw, qe, we, ww, fw, fe, fre, frw,
     fu4, fv4, cu, cv, cvs, hu, hv, su, sv,
     ca, cb, cc, cd, cg, ch, cm, cn, tt, ss, au, av,
     w_s, tab_s, lsem, ssem, rsem, osem) = refs
    col = lax.axis_index('col')
    row = lax.axis_index('row')
    east = lax.rem(col + 1, n_col)
    west = lax.rem(col + n_col - 1, n_col)
    has_s = row > 0
    has_n = row < n_row - 1

    def dev(c, r):
        at = {'col': c, 'row': r}
        return tuple(at[name] for name in axes)

    bufs = (bu, bv, bt, bs)
    loads = []
    for f, (src, dst) in enumerate(zip((u_h, v_h, t_h, s_h), bufs)):
        for t in range(NT):
            loads.append(pltpu.make_async_copy(src.at[:, :, L * t:L * t + L], dst.at[t, 0:LEV, R0:R0 + NR, :], lsem.at[len(loads)]))
    flat_loads = []
    for f, src in enumerate((eta_h, tu_h, tv_h)):
        for t in range(NT):
            flat_loads.append(pltpu.make_async_copy(src.at[:, L * t:L * t + L], x.at[f, t, XO:XO + NR, :], lsem.at[len(loads) + len(flat_loads)]))
    for t in range(NT):
        flat_loads.append(pltpu.make_async_copy(dep_h.at[:, L * t:L * t + L], bv.at[t, LEV, R0:R0 + NR, :], lsem.at[len(loads) + len(flat_loads)]))
    for t in range(NT):
        flat_loads.append(pltpu.make_async_copy(cnt_h.at[:, L * t:L * t + L], cnt_i.at[t], lsem.at[len(loads) + len(flat_loads)]))
    scalar_loads = [pltpu.make_async_copy(w_h, w_s, lsem.at[36]), pltpu.make_async_copy(tab_h, tab_s, lsem.at[37])]
    edge_loads = [loads[NT * f + t] for f in range(4) for t in (0, NT - 1)]
    mid_loads = [loads[NT * f + t] for f in range(4) for t in range(1, NT - 1)]
    for cp in edge_loads + flat_loads + mid_loads + scalar_loads:
        cp.start()

    zero = functools.partial(jnp.zeros, dtype=f32)
    for f in range(4):
        for t in range(NT + 1):
            x[f, t, 0:8, :] = zero((8, L))
            x[f, t, XR - 8:XR, :] = zero((8, L))
    for t in range(NT + 1):
        tt[t, XR - 8:XR, :] = zero((8, L))
    for t in range(NT):
        bt[t, LEV, R0:R0 + NR, :] = zero((NR, L))
        bs[t, LEV, R0:R0 + NR, :] = zero((NR, L))
        for a in (xu, xv, xt, xs):
            a[t, 0] = zero((NR, L))

    @pl.when(jnp.logical_not(has_s))
    def _():
        for b in bufs:
            b[:, :, R0 - 8:R0, :] = zero((NT, SLOT, 8, L))
        re[R0 - 8:R0, :] = zero((8, L))
        x[:, 0:NT, 8:XO, :] = zero((4, NT, NR, L))
        xf[:, 0:NT, 8:XO, :] = zero((2, NT, NR, L))
        for a in (we, ww, fre, frw):
            a[0] = zero((NR, L))

    @pl.when(jnp.logical_not(has_n))
    def _():
        for b in bufs:
            b[:, :, R0 + NR:PR, :] = zero((NT, SLOT, 8, L))
        rw[R0 + NR:PR, :] = zero((8, L))
        x[:, 0:NT, XO + NR:XO + 2 * NR, :] = zero((4, NT, NR, L))
        xf[:, 0:NT, XO + NR:XO + 2 * NR, :] = zero((2, NT, NR, L))
        for a in (we, ww, fre, frw):
            a[2] = zero((NR, L))

    barrier = pltpu.get_barrier_semaphore()

    def signal(c, r):
        pl.semaphore_signal(barrier, inc=1, device_id=dev(c, r), device_id_type=MESH)

    signal(west, row)
    signal(east, row)

    @pl.when(has_s)
    def _():
        for c in (west, col, east):
            signal(c, row - 1)

    @pl.when(has_n)
    def _():
        for c in (west, col, east):
            signal(c, row + 1)

    edge = jnp.logical_or(row == 0, row == n_row - 1)

    @pl.when(edge)
    def _():
        pl.semaphore_wait(barrier, 5)

    @pl.when(jnp.logical_not(edge))
    def _():
        pl.semaphore_wait(barrier, 8)

    n_copies = 0

    def remote(src, dst, c, r, sends, receives):
        nonlocal n_copies
        i = n_copies
        n_copies += 1
        return (pltpu.make_async_remote_copy(src, dst, ssem.at[i], rsem.at[i], device_id=dev(c, r), device_id_type=MESH), sends, receives)

    def maybe(cond, fn):
        if cond is None:
            fn()
        else:
            pl.when(cond)(fn)

    def start(group):
        for cp, sends, _ in group:
            maybe(sends, cp.start)

    def arrive(group):
        for cp, _, receives in group:
            maybe(receives, cp.wait_recv)

    def drain(group):
        for cp, sends, _ in group:
            maybe(sends, cp.wait_send)

    def rows_of(b):
        return [remote(b.at[:, :, R0 + NR - 1:R0 + NR, :], b.at[:, :, R0 - 1:R0, :], col, row + 1, has_n, has_s),
                remote(b.at[:, :, R0:R0 + 1, :], b.at[:, :, R0 + NR:R0 + NR + 1, :], col, row - 1, has_s, has_n)]

    def wide_of(b, lanes_w, lanes_e, from_e, from_w):
        own = b.at[:, 0:NT, XO:XO + NR, :]
        return [remote(own, b.at[:, 0:NT, 8:XO, :], col, row + 1, has_n, has_s),
                remote(own, b.at[:, 0:NT, XO + NR:XO + 2 * NR, :], col, row - 1, has_s, has_n),
                remote(lanes_w, from_e.at[1], west, row, None, None),
                remote(lanes_e, from_w.at[1], east, row, None, None),
                remote(lanes_w, from_e.at[2], west, row - 1, has_s, has_n),
                remote(lanes_e, from_w.at[2], east, row - 1, has_s, has_n),
                remote(lanes_w, from_e.at[0], west, row + 1, has_n, has_s),
                remote(lanes_e, from_w.at[0], east, row + 1, has_n, has_s)]

    row_group = rows_of(bu) + rows_of(bv) + rows_of(bt) + rows_of(bs)
    lane_group = [remote(pw, re.at[R0:R0 + NR, :], west, row, None, None),
                  remote(pe, rw.at[R0:R0 + NR, :], east, row, None, None),
                  remote(pe.at[0:1, :], rw.at[R0 + NR:R0 + NR + 1, :], east, row - 1, has_s, has_n),
                  remote(pw.at[NR - 1:NR, :], re.at[R0 - 1:R0, :], west, row + 1, has_n, has_s)]
    wide_group = wide_of(x, qw, qe, we, ww)
    force_group = wide_of(xf, fw, fe, fre, frw)

    lane = lax.broadcasted_iota(jnp.int32, (NR, L), 1)

    for cp in flat_loads:
        cp.wait()
    for t in range(NT):
        count = cnt_i[t].astype(f32)
        bu[t, LEV, R0:R0 + NR, :] = count
        x[3, t, XO:XO + NR, :] = jnp.where(count > 0.0, bv[t, LEV, R0:R0 + NR, :], 0.0)

    def roll(a, shift):
        return pltpu.roll(a, shift, 1) if not (isinstance(shift, int) and shift % L == 0) else a

    def pack_wide(b, n_fields):
        first = last = zero((NR, L))
        for f in range(n_fields):
            mine = (lane >= 32 * f) & (lane < 32 * f + 32)
            first = jnp.where(mine, roll(b[f, 0, XO:XO + NR, :], 32 * f), first)
            last = jnp.where(mine, roll(b[f, NT - 1, XO:XO + NR, :], (32 * f + 32) % L), last)
        return first, last

    first, last = pack_wide(x, 4)
    qw[...] = first
    qe[...] = last

    for cp in edge_loads:
        cp.wait()
    first = last = zero((NR, L))
    for f, b in enumerate(bufs):
        for k in range(SLOT):
            p = SLOT * f + k
            first = jnp.where(lane == p, roll(b[0, k, R0:R0 + NR, :], p), first)
            last = jnp.where(lane == p, roll(b[NT - 1, k, R0:R0 + NR, :], (p + 1) % L), last)
    pw[...] = first
    pe[...] = last
    for cp in mid_loads:
        cp.wait()
    start(row_group)
    start(lane_group)
    start(wide_group)
    for cp in scalar_loads:
        cp.wait()

    row_pos = (row * NR + lax.broadcasted_iota(jnp.int32, (NR, L), 0)).astype(f32)
    total_rows = NR * n_row
    fu4[...] = 0.25 * (CORIO_F0 + CORIO_BETA * ((row_pos + 0.5) / total_rows - 0.5))
    fv4[...] = 0.25 * (CORIO_F0 + CORIO_BETA * ((row_pos + 1.0) / total_rows - 0.5))

    def to_east(tiles, halo):
        rolled = [roll(a, L - 1) for a in tiles] + [halo]
        return [jnp.where(lane == L - 1, rolled[t + 1], rolled[t]) for t in range(NT)]

    def to_west(tiles, halo):
        rolled = [halo] + [roll(a, 1) for a in tiles]
        return [jnp.where(lane == 0, rolled[t], rolled[t + 1]) for t in range(NT)]

    def east_lane(f, k, lo=R0):
        return pltpu.roll(re[lo:lo + NR, :], L - 1 - (SLOT * f + k), 1)

    def west_lane(f, k, lo=R0):
        return pltpu.roll(rw[lo:lo + NR, :], lax.rem(L - (SLOT * f + k), L), 1)

    arrive(row_group)
    arrive(lane_group)

    def level(b, k, lo=R0):
        return [b[t, k, lo:lo + NR, :] for t in range(NT)]

    c_mid, d_mid = level(bu, LEV), level(bv, LEV)
    c_east = to_east(c_mid, east_lane(0, LEV))
    d_east = to_east(d_mid, east_lane(1, LEV))
    c_north, c_south = level(bu, LEV, R0 + 1), level(bu, LEV, R0 - 1)
    d_north = level(bv, LEV, R0 + 1)
    for t in range(NT):
        cu[t] = jnp.minimum(c_mid[t], c_east[t])
        cv[t] = jnp.minimum(c_mid[t], c_north[t])
        cvs[t] = jnp.minimum(c_mid[t], c_south[t])
        hu[t] = 0.5 * (d_mid[t] + d_east[t])
        hv[t] = 0.5 * (d_mid[t] + d_north[t])
        cu_o[t] = jnp.minimum(c_mid[t], c_east[t])
        cv_o[t] = jnp.minimum(c_mid[t], c_north[t])
        cc_o[t] = c_mid[t]

    def each_level(fn, unroll=UNROLL):
        def some(i, _):
            base = i * unroll
            for j in range(unroll):
                fn(base + j, base + j - 1 if j else jnp.maximum(base - 1, 0))
            return 0

        lax.fori_loop(0, SLOT // unroll, some, 0)

    for t in range(NT):
        pc[t] = zero((NR + 8, L))
    ce[...] = zero((NR, L))
    p_scale = BC_GRAVITY / LEV

    def momentum_down(k, prev):
        scale, carry = tab_s[k], tab_s[SLOT + k]
        um, un, us = level(bu, k), level(bu, k, R0 + 1), level(bu, k, R0 - 1)
        vm, vn, vs = level(bv, k), level(bv, k, R0 + 1), level(bv, k, R0 - 1)
        ue = to_east(um, east_lane(0, k))
        uw = to_west(um, west_lane(0, k))
        unw = to_west(un, west_lane(0, k, R0 + 1))
        ve = to_east(vm, east_lane(1, k))
        vw = to_west(vm, west_lane(1, k))
        vse = to_east(vs, east_lane(1, k, R0 - 1))
        pm = []
        for t in range(NT):
            density = CONTRACT_S * bs[t, k, R0:PR, :] - EXPAND_T * bt[t, k, R0:PR, :]
            total = pc[t] + density
            pc[t] = total
            pressure = p_scale * (total - 0.5 * density)
            pp[t] = pressure
            pm.append(pressure[:NR])
        density = CONTRACT_S * east_lane(3, k) - EXPAND_T * east_lane(2, k)
        total = ce[...] + density
        ce[...] = total
        pe_ = to_east(pm, p_scale * (total - 0.5 * density))
        for t in range(NT):
            pn = pp[t, 1:NR + 1, :]
            vb4 = (vm[t] + ve[t]) + (vs[t] + vse[t])
            ub4 = (um[t] + uw[t]) + (un[t] + unw[t])
            u_star = um[t] + vb4 * (fu4[...] - 0.125 * (un[t] - us[t])) - um[t] * (0.5 * (ue[t] - uw[t])) + (pm[t] - pe_[t])
            v_star = vm[t] - ub4 * (fv4[...] + 0.125 * (ve[t] - vw[t])) - vm[t] * (0.5 * (vn[t] - vs[t])) + (pm[t] - pn)
            xu[t, k] = scale * u_star + carry * xu[t, prev]
            xv[t, k] = scale * v_star + carry * xv[t, prev]

    each_level(momentum_down)

    def momentum_up(t, _):
        z = zero((NR, L))
        state = [[z, z, z], [z, z, z]]
        for k in range(LEV - 1, -1, -1):
            link, last_ = tab_s[2 * SLOT + k], tab_s[3 * SLOT + k]
            for q, (sweep, b, count) in enumerate(((xu, bu, cu), (xv, bv, cv))):
                below, sum_x, sum_0 = state[q]
                value = sweep[t, k]
                active = count[t] > float(k)
                solved = jnp.where(count[t] > float(k + 1), value + link * below, jnp.where(active, last_ * value, 0.0))
                sweep[t, k] = solved
                state[q] = [solved, sum_x + solved, sum_0 + jnp.where(active, b[t, k, R0:R0 + NR, :], 0.0)]
        for q, (h, mean, count) in enumerate(((hu, su, cu), (hv, sv, cv))):
            _, total, start_ = state[q]
            n_active = jnp.maximum(count[t], 1.0)
            mean[t] = total / n_active
            xf[q, t, XO:XO + NR, :] = h[t] * (total - start_) / n_active / TIME_STEP
        return 0

    lax.fori_loop(0, NT, momentum_up, 0)

    stores = [pltpu.make_async_copy(a, o, osem.at[i]) for i, (a, o) in enumerate(((xu, xu_o), (xv, xv_o), (xt, xt_o), (xs, xs_o)))]
    first, last = pack_wide(xf, 2)
    fw[...] = first
    fe[...] = last
    start(force_group)
    stores[0].start()
    stores[1].start()

    c_west0 = jnp.minimum(west_lane(0, LEV), bu[0, LEV, R0:R0 + NR, :])

    def tracer_down(k, prev):
        scale, carry = tab_s[4 * SLOT + k], tab_s[5 * SLOT + k]
        kf = k.astype(f32)
        um = [jnp.where(cu[t] > kf, bu[t, k, R0:R0 + NR, :], 0.0) for t in range(NT)]
        vm = [jnp.where(cv[t] > kf, bv[t, k, R0:R0 + NR, :], 0.0) for t in range(NT)]
        vs = [jnp.where(cvs[t] > kf, bv[t, k, R0 - 1:R0 - 1 + NR, :], 0.0) for t in range(NT)]
        uw0 = jnp.where(c_west0 > kf, west_lane(0, k), 0.0)
        for f, b, sweep in ((2, bt, xt), (3, bs, xs)):
            q = level(b, k)
            qe_ = to_east(q, east_lane(f, k))
            f_east = [um[t] * (q[t] + qe_[t]) for t in range(NT)]
            f_west = to_west(f_east, uw0 * (west_lane(f, k) + q[0]))
            for t in range(NT):
                f_north = vm[t] * (q[t] + b[t, k, R0 + 1:R0 + 1 + NR, :])
                f_south = vs[t] * (b[t, k, R0 - 1:R0 - 1 + NR, :] + q[t])
                new = q[t] - 0.5 * TIME_STEP * (f_east[t] - f_west[t] + f_north - f_south)
                sweep[t, k] = jnp.where(bu[t, LEV, R0:R0 + NR, :] > kf, scale * new + carry * sweep[t, prev], new)

    each_level(tracer_down)
    stores[2].start()
    stores[3].start()

    arrive(wide_group)
    drain(wide_group)
    arrive(force_group)

    def unpack_wide(b, from_e, from_w, n_fields):
        for f in range(n_fields):
            for seg in range(3):
                b[f, NT, 8 + NR * seg:8 + NR * seg + NR, :] = jnp.where(lane < L // 2, roll(from_e[seg], (L - 32 * f) % L), roll(from_w[seg], (96 - 32 * f) % L))

    unpack_wide(x, we, ww, 4)
    unpack_wide(xf, fre, frw, 2)
    dt_fast = TIME_STEP / n_sub
    XT = NT + 1

    def ring_east(tiles, last_lane):
        rolled = [roll(a, L - 1) for a in tiles]
        return [jnp.where(last_lane, rolled[(t + 1) % XT], rolled[t]) for t in range(XT)]

    def ring_west(tiles, first_lane):
        rolled = [roll(a, 1) for a in tiles]
        return [jnp.where(first_lane, rolled[(t - 1) % XT], rolled[t]) for t in range(XT)]

    for seg in range(3):
        lo = 8 + NR * seg
        pos = (row * NR + NR * (seg - 1) + lax.broadcasted_iota(jnp.int32, (NR, L), 0)).astype(f32)
        f_u = CORIO_F0 + CORIO_BETA * ((pos + 0.5) / total_rows - 0.5)
        f_v = CORIO_F0 + CORIO_BETA * ((pos + 1.0) / total_rows - 0.5)
        d = [x[3, t, lo:lo + NR, :] for t in range(XT)]
        d_e = ring_east(d, lane == L - 1)
        for t in range(XT):
            d_n = x[3, t, lo + 1:lo + 1 + NR, :]
            wet = jnp.where((d[t] > 0.0) & (d_e[t] > 0.0), 1.0, 0.0)
            cm[t, lo:lo + NR, :] = wet
            ca[t, lo:lo + NR, :] = (0.25 * dt_fast) * f_u * wet
            cb[t, lo:lo + NR, :] = (dt_fast * GRAVITY * 0.5) * (d[t] + d_e[t]) * wet
            cc[t, lo:lo + NR, :] = dt_fast * xf[0, t, lo:lo + NR, :] * wet
            wet = jnp.where((d[t] > 0.0) & (d_n > 0.0), 1.0, 0.0)
            cn[t, lo:lo + NR, :] = wet
            cd[t, lo:lo + NR, :] = (0.25 * dt_fast) * f_v * wet
            cg[t, lo:lo + NR, :] = (dt_fast * GRAVITY * 0.5) * (d[t] + d_n) * wet
            ch[t, lo:lo + NR, :] = dt_fast * xf[1, t, lo:lo + NR, :] * wet

    for t in range(NT):
        au[t] = zero((NR, L))
        av[t] = zero((NR, L))

    def subcycle(lo, hi, chunk, n, _):
        lane_c = lax.broadcasted_iota(jnp.int32, (chunk, L), 1)
        first_lane, last_lane = lane_c == 0, lane_c == L - 1
        weight = w_s[n]
        for r in range(lo, hi, chunk):
            u_t = [x[1, t, r:r + chunk, :] for t in range(XT)]
            u_w = ring_west(u_t, first_lane)
            for t in range(XT):
                v_t, v_s = x[2, t, r:r + chunk, :], x[2, t, r - 1:r - 1 + chunk, :]
                x[0, t, r:r + chunk, :] = x[0, t, r:r + chunk, :] - dt_fast * ((u_t[t] - u_w[t]) + (v_t - v_s))
                tt[t, r:r + chunk, :] = u_t[t] + u_w[t]
                ss[t, r:r + chunk, :] = v_t + v_s
        for r in range(lo, hi, chunk):
            e_t = [x[0, t, r:r + chunk, :] for t in range(XT)]
            e_e = ring_east(e_t, last_lane)
            s_t = [ss[t, r:r + chunk, :] for t in range(XT)]
            s_e = ring_east(s_t, last_lane)
            for t in range(XT):
                at = (t, slice(r, r + chunk))
                up = (t, slice(r + 1, r + 1 + chunk))
                e_n = x[0, t, r + 1:r + 1 + chunk, :]
                x[1, t, r:r + chunk, :] = cm[at] * x[1, t, r:r + chunk, :] + ca[at] * (s_t[t] + s_e[t]) + cc[at] - cb[at] * (e_e[t] - e_t[t])
                x[2, t, r:r + chunk, :] = cn[at] * x[2, t, r:r + chunk, :] - cd[at] * (tt[at] + tt[up]) + ch[at] - cg[at] * (e_n - e_t[t])
        for t in range(NT):
            au[t] += weight * x[1, t, XO:XO + NR, :]
            av[t] += weight * x[2, t, XO:XO + NR, :]
        return 0

    done = 0
    for side in (4, 3, 2, 1):
        until = n_sub - 8 * (side - 1)
        rows = NR + 16 * side
        chunk = {4: 32, 3: 40, 2: 32, 1: 24}[side]
        lax.fori_loop(done, until, functools.partial(subcycle, XO - 8 * side, XO - 8 * side + rows, chunk), 0)
        done = until

    for t in range(NT):
        cols = slice(L * t, L * t + L)
        eta_o[:, cols] = x[0, t, XO:XO + NR, :]
        tu_o[:, cols] = x[1, t, XO:XO + NR, :]
        tv_o[:, cols] = x[2, t, XO:XO + NR, :]
        gu_o[t] = au[t] / hu[t] - su[t]
        gv_o[t] = av[t] / hv[t] - sv[t]

    for group in (row_group, lane_group, force_group):
        drain(group)
    for cp in stores:
        cp.wait()


def final_kernel(tab_s, xu, xv, xt, xs, gu, gv, cu, cv, cc, u_o, v_o, t_o, s_o):
    rows = u_o.shape[1]
    g_u, g_v, c_u, c_v, c_c = gu[0], gv[0], cu[0], cv[0], cc[0]

    state = [jnp.zeros((rows, L), f32)] * 2
    for k in range(LEV - 1, -1, -1):
        kf = float(k)
        link, last = tab_s[6 * SLOT + k], tab_s[7 * SLOT + k]
        u_o[k] = jnp.where(c_u > kf, xu[0, k] + g_u, 0.0)
        v_o[k] = jnp.where(c_v > kf, xv[0, k] + g_v, 0.0)
        inner, active = c_c > kf + 1.0, c_c > kf
        for q, (sweep, o) in enumerate(((xt, t_o), (xs, s_o))):
            value = sweep[0, k]
            solved = jnp.where(inner, value + link * state[q], jnp.where(active, last * value, value))
            o[k] = solved
            state[q] = solved


def solution(mesh):
    n_col = mesh.shape['col']
    n_row = mesh.shape['row']

    def step(vel_u, vel_v, value_a11, salinity, surf_eta, trans_u, trans_v, bottom_depth, level_count, avg_weights):
        n_sub = avg_weights.shape[0]
        table = jnp.asarray(solve_table(LEV))
        hbm = pl.BlockSpec(memory_space=pl.ANY)
        vmem = pl.BlockSpec(memory_space=pltpu.VMEM)
        smem = pl.BlockSpec(memory_space=pltpu.SMEM)
        flat = jax.ShapeDtypeStruct((NR, NC), f32)
        tile = jax.ShapeDtypeStruct((NT, NR, L), f32)
        sweep = jax.ShapeDtypeStruct((NT, SLOT, NR, L), f32)
        V = pltpu.VMEM
        wide = (NT + 1, XR, L)
        scratch = ([V((NT, SLOT, PR, L), f32)] * 4 + [V((NT, SLOT, NR, L), f32)] * 4
                   + [V((NT, NR, L), jnp.int32), V((NT, NR + 8, L), f32), V((NT, NR + 8, L), f32), V((NR, L), f32)]
                   + [V((NR, L), f32)] * 2 + [V((PR, L), f32)] * 2
                   + [V((4,) + wide, f32), V((2,) + wide, f32)] + [V((NR, L), f32)] * 2 + [V((3, NR, L), f32)] * 2
                   + [V((NR, L), f32)] * 2 + [V((3, NR, L), f32)] * 2
                   + [V((NR, L), f32)] * 2 + [V((NT, NR, L), f32)] * 7
                   + [V(wide, f32)] * 10 + [V((NT, NR, L), f32)] * 2
                   + [pltpu.SMEM((n_sub,), f32), pltpu.SMEM((8 * SLOT,), f32)]
                   + [pltpu.SemaphoreType.DMA((40,)), pltpu.SemaphoreType.DMA((28,)), pltpu.SemaphoreType.DMA((28,)), pltpu.SemaphoreType.DMA((4,))])
        outs = pl.pallas_call(
            functools.partial(ocean_kernel, tuple(mesh.axis_names), n_col, n_row, n_sub),
            out_shape=[flat] * 3 + [tile] * 5 + [sweep] * 4,
            in_specs=[hbm] * 11,
            out_specs=[vmem] * 8 + [hbm] * 4,
            scratch_shapes=scratch,
            compiler_params=pltpu.CompilerParams(collective_id=0, has_side_effects=True, vmem_limit_bytes=56 * 1024 * 1024),
        )(vel_u, vel_v, value_a11, salinity, surf_eta, trans_u, trans_v, bottom_depth, level_count, avg_weights, table)
        eta, tu, tv, gu, gv, cu, cv, cc, xu, xv, xt, xs = outs

        part = 16
        big = pl.BlockSpec((1, SLOT, part, L), lambda t, r: (t, 0, r, 0))
        small = pl.BlockSpec((1, part, L), lambda t, r: (t, r, 0))
        out = pl.BlockSpec((LEV, part, L), lambda t, r: (0, r, t))
        cube = jax.ShapeDtypeStruct((LEV, NR, NC), f32)
        u_new, v_new, t_new, s_new = pl.pallas_call(
            final_kernel,
            grid=(NT, NR // part),
            out_shape=[cube] * 4,
            in_specs=[smem] + [big] * 4 + [small] * 5,
            out_specs=[out] * 4,
        )(table, xu, xv, xt, xs, gu, gv, cu, cv, cc)
        return (eta, tu, tv, u_new, v_new, t_new, s_new)

    cube = P(None, 'row', 'col')
    flat = P('row', 'col')
    return jax.shard_map(step, mesh=mesh, in_specs=(cube, cube, cube, cube, flat, flat, flat, flat, flat, P()), out_specs=(flat, flat, flat, cube, cube, cube, cube), check_vma=False)
```

```python
import functools

import jax
import jax.numpy as jnp
import numpy as np
from jax import lax
from jax.experimental import pallas as pl
from jax.experimental.pallas import tpu as pltpu
from jax.sharding import PartitionSpec as P

TIME_STEP = 1.0
GRAVITY = 16.0
BC_GRAVITY = 4.0
EXPAND_T = 0.2
CONTRACT_S = 0.6
CORIO_F0 = 0.4
CORIO_BETA = 0.4
VISC_R = 2.0
DIFF_R = 0.5

LEV = 31
SLOT = 32
NR = 32
NC = 512
NT = 4
L = 128
R0 = 8
PR = 48
XR = 112
XO = 40
MESH = pl.DeviceIdType.MESH
f32 = jnp.float32
UNROLL = 4


def solve_table(n_levels):
    rows = []
    for s in (VISC_R, DIFF_R):
        scale, carry, link, last = np.zeros((4, SLOT))
        ratio = 0.0
        for k in range(n_levels):
            low = s if k else 0.0
            full = 1.0 + low + s - low * ratio
            end = 1.0 + low - low * ratio
            scale[k], carry[k], link[k], last[k] = 1.0 / full, low / full, s / full, full / end
            ratio = s / full
        rows += [scale, carry, link, last]
    return np.concatenate(rows).astype(np.float32)


def ocean_kernel(axes, n_col, n_row, n_sub, *refs):
    (u_h, v_h, t_h, s_h, eta_h, tu_h, tv_h, dep_h, cnt_h, w_h, tab_h,
     eta_o, tu_o, tv_o, gu_o, gv_o, cu, cv, cc_o, xu, xv, xt, xs,
     bu, bv, bt, bs, bp, cnt_i, rp,
     pw, pe, rw, re, x, xf, qw, qe, we, ww, fw, fe, fre, frw,
     fu4, fv4, hu, hv, su, sv,
     ca, cb, cc, cd, cg, ch, cm, cn, tt, au, av,
     w_s, tab_s, lsem, ssem, rsem) = refs
    col = lax.axis_index('col')
    row = lax.axis_index('row')
    east = lax.rem(col + 1, n_col)
    west = lax.rem(col + n_col - 1, n_col)
    has_s = row > 0
    has_n = row < n_row - 1

    def dev(c, r):
        at = {'col': c, 'row': r}
        return tuple(at[name] for name in axes)

    bufs = (bu, bv, bt, bs)
    barrier = pltpu.get_barrier_semaphore()

    def signal(c, r):
        pl.semaphore_signal(barrier, inc=1, device_id=dev(c, r), device_id_type=MESH)

    signal(west, row)
    signal(east, row)

    @pl.when(has_s)
    def _():
        for c in (west, col, east):
            signal(c, row - 1)

    @pl.when(has_n)
    def _():
        for c in (west, col, east):
            signal(c, row + 1)

    zero = functools.partial(jnp.zeros, dtype=f32)

    loads = []
    for f, (src, dst) in enumerate(zip((u_h, v_h, t_h, s_h), bufs)):
        for t in range(NT):
            loads.append(pltpu.make_async_copy(src.at[:, :, L * t:L * t + L], dst.at[t, 0:LEV, R0:R0 + NR, :], lsem.at[len(loads)]))
    flat_loads = []
    for f, src in enumerate((eta_h, tu_h, tv_h)):
        for t in range(NT):
            flat_loads.append(pltpu.make_async_copy(src.at[:, L * t:L * t + L], x.at[f, t, XO:XO + NR, :], lsem.at[len(loads) + len(flat_loads)]))
    for t in range(NT):
        flat_loads.append(pltpu.make_async_copy(dep_h.at[:, L * t:L * t + L], bv.at[t, LEV, R0:R0 + NR, :], lsem.at[len(loads) + len(flat_loads)]))
    for t in range(NT):
        flat_loads.append(pltpu.make_async_copy(cnt_h.at[:, L * t:L * t + L], cnt_i.at[t], lsem.at[len(loads) + len(flat_loads)]))
    scalar_loads = [pltpu.make_async_copy(w_h, w_s, lsem.at[36]), pltpu.make_async_copy(tab_h, tab_s, lsem.at[37])]
    edge_loads = [loads[NT * f + t] for f in range(4) for t in (0, NT - 1)]
    mid_loads = [loads[NT * f + t] for f in range(4) for t in range(1, NT - 1)]
    for cp in edge_loads + flat_loads + mid_loads + scalar_loads:
        cp.start()

    n_copies = 0

    def remote(src, dst, c, r, sends, receives):
        nonlocal n_copies
        i = n_copies
        n_copies += 1
        return (pltpu.make_async_remote_copy(src, dst, ssem.at[i], rsem.at[i], device_id=dev(c, r), device_id_type=MESH), sends, receives)

    def maybe(cond, fn):
        if cond is None:
            fn()
        else:
            pl.when(cond)(fn)

    def start(group):
        for cp, sends, _ in group:
            maybe(sends, cp.start)

    def arrive(group):
        for cp, _, receives in group:
            maybe(receives, cp.wait_recv)

    def drain(group):
        for cp, sends, _ in group:
            maybe(sends, cp.wait_send)

    def rows_of(b):
        return [remote(b.at[:, :, R0 + NR - 1:R0 + NR, :], b.at[:, :, R0 - 1:R0, :], col, row + 1, has_n, has_s),
                remote(b.at[:, :, R0:R0 + 1, :], b.at[:, :, R0 + NR:R0 + NR + 1, :], col, row - 1, has_s, has_n)]

    def wide_of(b, lanes_w, lanes_e, from_e, from_w):
        own = b.at[:, 0:NT, XO:XO + NR, :]
        return [remote(own, b.at[:, 0:NT, 8:XO, :], col, row + 1, has_n, has_s),
                remote(own, b.at[:, 0:NT, XO + NR:XO + 2 * NR, :], col, row - 1, has_s, has_n),
                remote(lanes_w, from_e.at[1], west, row, None, None),
                remote(lanes_e, from_w.at[1], east, row, None, None),
                remote(lanes_w, from_e.at[2], west, row - 1, has_s, has_n),
                remote(lanes_e, from_w.at[2], east, row - 1, has_s, has_n),
                remote(lanes_w, from_e.at[0], west, row + 1, has_n, has_s),
                remote(lanes_e, from_w.at[0], east, row + 1, has_n, has_s)]

    row_group = rows_of(bu) + rows_of(bv) + rows_of(bt) + rows_of(bs)
    lane_group = [remote(pw, re.at[R0:R0 + NR, :], west, row, None, None),
                  remote(pe, rw.at[R0:R0 + NR, :], east, row, None, None),
                  remote(pe.at[0:1, :], rw.at[R0 + NR:R0 + NR + 1, :], east, row - 1, has_s, has_n),
                  remote(pw.at[NR - 1:NR, :], re.at[R0 - 1:R0, :], west, row + 1, has_n, has_s)]
    wide_group = wide_of(x, qw, qe, we, ww)
    force_group = wide_of(xf, fw, fe, fre, frw)

    lane = lax.broadcasted_iota(jnp.int32, (NR, L), 1)

    for t in range(NT):
        bt[t, LEV, R0:R0 + NR, :] = zero((NR, L))
        bs[t, LEV, R0:R0 + NR, :] = zero((NR, L))
    for cp in flat_loads:
        cp.wait()
    for t in range(NT):
        count = cnt_i[t].astype(f32)
        bu[t, LEV, R0:R0 + NR, :] = count
        x[3, t, XO:XO + NR, :] = jnp.where(count > 0.0, bv[t, LEV, R0:R0 + NR, :], 0.0)

    def roll(a, shift):
        return pltpu.roll(a, shift, 1) if not (isinstance(shift, int) and shift % L == 0) else a

    def pack_wide(b, n_fields):
        first = last = zero((NR, L))
        for f in range(n_fields):
            mine = (lane >= 32 * f) & (lane < 32 * f + 32)
            first = jnp.where(mine, roll(b[f, 0, XO:XO + NR, :], 32 * f), first)
            last = jnp.where(mine, roll(b[f, NT - 1, XO:XO + NR, :], (32 * f + 32) % L), last)
        return first, last

    first, last = pack_wide(x, 4)
    qw[...] = first
    qe[...] = last

    for cp in edge_loads:
        cp.wait()
    first = last = zero((NR, L))
    for f, b in enumerate(bufs):
        for k in range(SLOT):
            p = SLOT * f + k
            first = jnp.where(lane == p, roll(b[0, k, R0:R0 + NR, :], p), first)
            last = jnp.where(lane == p, roll(b[NT - 1, k, R0:R0 + NR, :], (p + 1) % L), last)
    pw[...] = first
    pe[...] = last
    for cp in mid_loads:
        cp.wait()
    edge = jnp.logical_or(row == 0, row == n_row - 1)

    @pl.when(edge)
    def _():
        pl.semaphore_wait(barrier, 5)

    @pl.when(jnp.logical_not(edge))
    def _():
        pl.semaphore_wait(barrier, 8)

    start(row_group)
    start(lane_group)
    start(wide_group)
    for cp in scalar_loads:
        cp.wait()

    for f in range(4):
        for t in range(NT + 1):
            x[f, t, 0:8, :] = zero((8, L))
            x[f, t, XR - 8:XR, :] = zero((8, L))
    for t in range(NT + 1):
        tt[t, XR - 8:XR, :] = zero((8, L))
    for t in range(NT):
        for a in (xu, xv, xt, xs):
            a[t, 0] = zero((NR, L))

    @pl.when(jnp.logical_not(has_s))
    def _():
        for b in bufs:
            b[:, :, R0 - 8:R0, :] = zero((NT, SLOT, 8, L))
        re[R0 - 8:R0, :] = zero((8, L))
        x[:, 0:NT, 8:XO, :] = zero((4, NT, NR, L))
        xf[:, 0:NT, 8:XO, :] = zero((2, NT, NR, L))
        for a in (we, ww, fre, frw):
            a[0] = zero((NR, L))

    @pl.when(jnp.logical_not(has_n))
    def _():
        for b in bufs:
            b[:, :, R0 + NR:PR, :] = zero((NT, SLOT, 8, L))
        rw[R0 + NR:PR, :] = zero((8, L))
        x[:, 0:NT, XO + NR:XO + 2 * NR, :] = zero((4, NT, NR, L))
        xf[:, 0:NT, XO + NR:XO + 2 * NR, :] = zero((2, NT, NR, L))
        for a in (we, ww, fre, frw):
            a[2] = zero((NR, L))


    row_pos = (row * NR + lax.broadcasted_iota(jnp.int32, (NR, L), 0)).astype(f32)
    total_rows = NR * n_row
    fu4[...] = 0.25 * (CORIO_F0 + CORIO_BETA * ((row_pos + 0.5) / total_rows - 0.5))
    fv4[...] = 0.25 * (CORIO_F0 + CORIO_BETA * ((row_pos + 1.0) / total_rows - 0.5))

    def to_east(tiles, halo):
        last_lane = lane[:halo.shape[0]] == L - 1
        rolled = [roll(a, L - 1) for a in tiles] + [halo]
        return [jnp.where(last_lane, rolled[t + 1], rolled[t]) for t in range(NT)]

    def to_west(tiles, halo):
        first_lane = lane[:halo.shape[0]] == 0
        rolled = [halo] + [roll(a, 1) for a in tiles]
        return [jnp.where(first_lane, rolled[t], rolled[t + 1]) for t in range(NT)]

    def east_lane(f, k, lo=R0, n=NR):
        return pltpu.roll(re[lo:lo + n, :], L - 1 - (SLOT * f + k), 1)

    def west_lane(f, k, lo=R0, n=NR):
        return pltpu.roll(rw[lo:lo + n, :], lax.rem(L - (SLOT * f + k), L), 1)

    def level(b, k, lo=R0, n=NR):
        return [b[t, k, lo:lo + n, :] for t in range(NT)]

    def each_level(fn, unroll=UNROLL):
        def some(i, _):
            base = i * unroll
            for j in range(unroll):
                fn(base + j, base + j - 1 if j else jnp.maximum(base - 1, 0))
            return 0

        lax.fori_loop(0, SLOT // unroll, some, 0)

    p_scale = BC_GRAVITY / LEV

    def pressure(t, lo, n):
        total = zero((n, L))
        for k in range(LEV):
            density = CONTRACT_S * bs[t, k, lo:lo + n, :] - EXPAND_T * bt[t, k, lo:lo + n, :]
            total = total + density
            bp[t, k, lo:lo + n, :] = p_scale * (total - 0.5 * density)
        bp[t, LEV, lo:lo + n, :] = zero((n, L))

    def own_pressure(t, _):
        pressure(t, R0, NR)
        return 0

    lax.fori_loop(0, NT, own_pressure, 0)

    def momentum_down(parts, k, prev):
        scale, carry = tab_s[k], tab_s[SLOT + k]
        for lo, n in parts:
            own = slice(lo - R0, lo - R0 + n)
            um, un, us = level(bu, k, lo, n), level(bu, k, lo + 1, n), level(bu, k, lo - 1, n)
            ue = to_east(um, east_lane(0, k, lo, n))
            uw = to_west(um, west_lane(0, k, lo, n))
            unw = to_west(un, west_lane(0, k, lo + 1, n))
            vm, vn, vs = level(bv, k, lo, n), level(bv, k, lo + 1, n), level(bv, k, lo - 1, n)
            ve = to_east(vm, east_lane(1, k, lo, n))
            vw = to_west(vm, west_lane(1, k, lo, n))
            vse = to_east(vs, east_lane(1, k, lo - 1, n))
            pm, pn = level(bp, k, lo, n), level(bp, k, lo + 1, n)
            pe_ = to_east(pm, pltpu.roll(rp[own, :], L - 1 - k, 1))
            for t in range(NT):
                vb4 = (vm[t] + ve[t]) + (vs[t] + vse[t])
                ub4 = (um[t] + uw[t]) + (un[t] + unw[t])
                u_star = um[t] + vb4 * (fu4[own, :] - 0.125 * (un[t] - us[t])) - um[t] * (0.5 * (ue[t] - uw[t])) + (pm[t] - pe_[t])
                v_star = vm[t] - ub4 * (fv4[own, :] + 0.125 * (ve[t] - vw[t])) - vm[t] * (0.5 * (vn[t] - vs[t])) + (pm[t] - pn[t])
                xu[t, k, own, :] = scale * u_star + carry * xu[t, prev, own, :]
                xv[t, k, own, :] = scale * v_star + carry * xv[t, prev, own, :]

    arrive(lane_group)
    density = CONTRACT_S * roll(re[R0:R0 + NR, :], L - 3 * SLOT) - EXPAND_T * roll(re[R0:R0 + NR, :], L - 2 * SLOT)
    total = density
    for step in (1, 2, 4, 8, 16):
        total = total + jnp.where(lane >= step, roll(total, step), 0.0)
    rp[...] = p_scale * (total - 0.5 * density)
    each_level(functools.partial(momentum_down, ((R0 + 8, NR - 16),)))
    arrive(row_group)

    def north_pressure(t, _):
        pressure(t, R0 + NR, 8)
        return 0

    lax.fori_loop(0, NT, north_pressure, 0)
    each_level(functools.partial(momentum_down, ((R0, 8), (R0 + NR - 8, 8))))
    drain(row_group)

    c_mid, d_mid = level(bu, LEV), level(bv, LEV)
    c_east = to_east(c_mid, east_lane(0, LEV))
    d_east = to_east(d_mid, east_lane(1, LEV))
    c_north, c_south = level(bu, LEV, R0 + 1), level(bu, LEV, R0 - 1)
    d_north = level(bv, LEV, R0 + 1)
    for t in range(NT):
        cu[t] = jnp.minimum(c_mid[t], c_east[t])
        cv[t] = jnp.minimum(c_mid[t], c_north[t])
        hu[t] = 0.5 * (d_mid[t] + d_east[t])
        hv[t] = 0.5 * (d_mid[t] + d_north[t])
        cc_o[t] = c_mid[t]
    c_west0 = jnp.minimum(west_lane(0, LEV), c_mid[0])

    def momentum_up(t, _):
        z = zero((NR, L))
        state = [[z, z, z], [z, z, z]]
        for k in range(LEV - 1, -1, -1):
            link, last_ = tab_s[2 * SLOT + k], tab_s[3 * SLOT + k]
            for q, (sweep, b, count) in enumerate(((xu, bu, cu), (xv, bv, cv))):
                below, sum_x, sum_0 = state[q]
                value = sweep[t, k]
                active = count[t] > float(k)
                solved = jnp.where(count[t] > float(k + 1), value + link * below, jnp.where(active, last_ * value, 0.0))
                sweep[t, k] = solved
                start_ = jnp.where(active, b[t, k, R0:R0 + NR, :], 0.0)
                b[t, k, R0:R0 + NR, :] = start_
                state[q] = [solved, sum_x + solved, sum_0 + start_]
        for q, (h, mean, count) in enumerate(((hu, su, cu), (hv, sv, cv))):
            _, total, start_ = state[q]
            n_active = jnp.maximum(count[t], 1.0)
            mean[t] = total / n_active
            xf[q, t, XO:XO + NR, :] = h[t] * (total - start_) / n_active / TIME_STEP
        c_south = jnp.minimum(bu[t, LEV, 0:8, :], pltpu.roll(bu[t, LEV, R0:R0 + 8, :], 7, 0))
        for k in range(LEV):
            bv[t, k, 0:8, :] = jnp.where(c_south > float(k), bv[t, k, 0:8, :], 0.0)
        return 0

    lax.fori_loop(0, NT, momentum_up, 0)

    first, last = pack_wide(xf, 2)
    fw[...] = first
    fe[...] = last
    start(force_group)

    def tracer_down(k, prev):
        scale, carry = tab_s[4 * SLOT + k], tab_s[5 * SLOT + k]
        kf = lax.convert_element_type(k, f32)
        um, vm, vs = level(bu, k), level(bv, k), level(bv, k, R0 - 1)
        uw0 = jnp.where(c_west0 > kf, west_lane(0, k), 0.0)
        for f, b, sweep in ((2, bt, xt), (3, bs, xs)):
            q = level(b, k)
            qe_ = to_east(q, east_lane(f, k))
            f_east = [um[t] * (q[t] + qe_[t]) for t in range(NT)]
            f_west = to_west(f_east, uw0 * (west_lane(f, k) + q[0]))
            for t in range(NT):
                f_north = vm[t] * (q[t] + b[t, k, R0 + 1:R0 + 1 + NR, :])
                f_south = vs[t] * (b[t, k, R0 - 1:R0 - 1 + NR, :] + q[t])
                new = q[t] - 0.5 * TIME_STEP * (f_east[t] - f_west[t] + f_north - f_south)
                sweep[t, k] = jnp.where(bu[t, LEV, R0:R0 + NR, :] > kf, scale * new + carry * sweep[t, prev], new)

    each_level(tracer_down)

    arrive(wide_group)
    drain(wide_group)
    arrive(force_group)

    def unpack_wide(b, from_e, from_w, n_fields):
        for f in range(n_fields):
            for seg in range(3):
                b[f, NT, 8 + NR * seg:8 + NR * seg + NR, :] = jnp.where(lane < L // 2, roll(from_e[seg], (L - 32 * f) % L), roll(from_w[seg], (96 - 32 * f) % L))

    unpack_wide(x, we, ww, 4)
    unpack_wide(xf, fre, frw, 2)
    dt_fast = TIME_STEP / n_sub
    XT = NT + 1

    def ring_east(tiles, last_lane):
        rolled = [roll(a, L - 1) for a in tiles]
        return [jnp.where(last_lane, rolled[(t + 1) % XT], rolled[t]) for t in range(XT)]

    def ring_west(tiles, first_lane):
        rolled = [roll(a, 1) for a in tiles]
        return [jnp.where(first_lane, rolled[(t - 1) % XT], rolled[t]) for t in range(XT)]

    for seg in range(3):
        lo = 8 + NR * seg
        pos = (row * NR + NR * (seg - 1) + lax.broadcasted_iota(jnp.int32, (NR, L), 0)).astype(f32)
        f_u = CORIO_F0 + CORIO_BETA * ((pos + 0.5) / total_rows - 0.5)
        f_v = CORIO_F0 + CORIO_BETA * ((pos + 1.0) / total_rows - 0.5)
        d = [x[3, t, lo:lo + NR, :] for t in range(XT)]
        d_e = ring_east(d, lane == L - 1)
        for t in range(XT):
            d_n = x[3, t, lo + 1:lo + 1 + NR, :]
            wet = jnp.where((d[t] > 0.0) & (d_e[t] > 0.0), 1.0, 0.0)
            cm[t, lo:lo + NR, :] = wet
            ca[t, lo:lo + NR, :] = (0.25 * dt_fast) * f_u * wet
            cb[t, lo:lo + NR, :] = (dt_fast * GRAVITY * 0.5) * (d[t] + d_e[t]) * wet
            cc[t, lo:lo + NR, :] = dt_fast * xf[0, t, lo:lo + NR, :] * wet
            wet = jnp.where((d[t] > 0.0) & (d_n > 0.0), 1.0, 0.0)
            cn[t, lo:lo + NR, :] = wet
            cd[t, lo:lo + NR, :] = (0.25 * dt_fast) * f_v * wet
            cg[t, lo:lo + NR, :] = (dt_fast * GRAVITY * 0.5) * (d[t] + d_n) * wet
            ch[t, lo:lo + NR, :] = dt_fast * xf[1, t, lo:lo + NR, :] * wet

    for t in range(NT):
        au[t] = zero((NR, L))
        av[t] = zero((NR, L))

    def subcycle(lo, hi, chunk, masked, n, _):
        lane_c = lax.broadcasted_iota(jnp.int32, (chunk, L), 1)
        first_lane, last_lane = lane_c == 0, lane_c == L - 1
        weight = w_s[n]
        for r in range(lo, hi, chunk):
            u_t = [x[1, t, r:r + chunk, :] for t in range(XT)]
            u_w = ring_west(u_t, first_lane)
            for t in range(XT):
                v_t, v_s = x[2, t, r:r + chunk, :], x[2, t, r - 1:r - 1 + chunk, :]
                x[0, t, r:r + chunk, :] = x[0, t, r:r + chunk, :] - dt_fast * ((u_t[t] - u_w[t]) + (v_t - v_s))
                tt[t, r:r + chunk, :] = u_t[t] + u_w[t]
        for r in range(hi - chunk, lo - 1, -chunk):
            e_t = [x[0, t, r:r + chunk, :] for t in range(XT)]
            e_e = ring_east(e_t, last_lane)
            v_t = [x[2, t, r:r + chunk, :] for t in range(XT)]
            s_t = [v_t[t] + x[2, t, r - 1:r - 1 + chunk, :] for t in range(XT)]
            s_e = ring_east(s_t, last_lane)
            for t in range(XT):
                at = (t, slice(r, r + chunk))
                up = (t, slice(r + 1, r + 1 + chunk))
                e_n = x[0, t, r + 1:r + 1 + chunk, :]
                u_old = x[1, t, r:r + chunk, :] if masked else cm[at] * x[1, t, r:r + chunk, :]
                v_old = v_t[t] if masked else cn[at] * v_t[t]
                x[1, t, r:r + chunk, :] = u_old + ca[at] * (s_t[t] + s_e[t]) + cc[at] - cb[at] * (e_e[t] - e_t[t])
                x[2, t, r:r + chunk, :] = v_old - cd[at] * (tt[at] + tt[up]) + ch[at] - cg[at] * (e_n - e_t[t])
        for t in range(NT):
            au[t] += weight * x[1, t, XO:XO + NR, :]
            av[t] += weight * x[2, t, XO:XO + NR, :]
        return 0

    done = 0
    for side in (4, 3, 2, 1):
        until = n_sub - 8 * (side - 1)
        rows = NR + 16 * side
        chunk = {4: 32, 3: 40, 2: 32, 1: 24}[side]
        stretch = functools.partial(subcycle, XO - 8 * side, XO - 8 * side + rows, chunk)
        if done == 0:
            stretch(False, 0, 0)
            done = 1
        lax.fori_loop(done, until, functools.partial(stretch, True), 0)
        done = until

    for t in range(NT):
        eta_o[t] = x[0, t, XO:XO + NR, :]
        tu_o[t] = x[1, t, XO:XO + NR, :]
        tv_o[t] = x[2, t, XO:XO + NR, :]
        gu_o[t] = au[t] / hu[t] - su[t]
        gv_o[t] = av[t] / hv[t] - sv[t]

    for group in (lane_group, force_group):
        drain(group)


def final_kernel(tab_s, xu, xv, xt, xs, gu, gv, cu, cv, cc, eta, tu, tv, eta_o, tu_o, tv_o, u_o, v_o, t_o, s_o):
    rows = u_o.shape[1]
    eta_o[...], tu_o[...], tv_o[...] = eta[0], tu[0], tv[0]
    g_u, g_v, c_u, c_v, c_c = gu[0], gv[0], cu[0], cv[0], cc[0]

    state = [jnp.zeros((rows, L), f32)] * 2
    for k in range(LEV - 1, -1, -1):
        kf = float(k)
        link, last = tab_s[6 * SLOT + k], tab_s[7 * SLOT + k]
        u_o[k] = jnp.where(c_u > kf, xu[0, k] + g_u, 0.0)
        v_o[k] = jnp.where(c_v > kf, xv[0, k] + g_v, 0.0)
        inner, active = c_c > kf + 1.0, c_c > kf
        for q, (sweep, o) in enumerate(((xt, t_o), (xs, s_o))):
            value = sweep[0, k]
            solved = jnp.where(inner, value + link * state[q], jnp.where(active, last * value, value))
            o[k] = solved
            state[q] = solved


def solution(mesh):
    n_col = mesh.shape['col']
    n_row = mesh.shape['row']

    def step(vel_u, vel_v, value_a11, salinity, surf_eta, trans_u, trans_v, bottom_depth, level_count, avg_weights):
        n_sub = avg_weights.shape[0]
        table = jnp.asarray(solve_table(LEV))
        hbm = pl.BlockSpec(memory_space=pltpu.HBM)
        vmem = pl.BlockSpec(memory_space=pltpu.VMEM)
        smem = pl.BlockSpec(memory_space=pltpu.SMEM)
        V = pltpu.VMEM
        tile = V((NT, NR, L), f32)
        sweep = V((NT, SLOT, NR, L), f32)
        wide = (NT + 1, XR, L)
        scratch = ([V((NT, SLOT, PR, L), f32)] * 5 + [V((NT, NR, L), jnp.int32), V((NR, L), f32)]
                   + [V((NR, L), f32)] * 2 + [V((PR, L), f32)] * 2
                   + [V((4,) + wide, f32), V((2,) + wide, f32)] + [V((NR, L), f32)] * 2 + [V((3, NR, L), f32)] * 2
                   + [V((NR, L), f32)] * 2 + [V((3, NR, L), f32)] * 2
                   + [V((NR, L), f32)] * 2 + [V((NT, NR, L), f32)] * 4
                   + [V(wide, f32)] * 9 + [V((NT, NR, L), f32)] * 2
                   + [pltpu.SMEM((n_sub,), f32), pltpu.SMEM((8 * SLOT,), f32)]
                   + [pltpu.SemaphoreType.DMA((40,)), pltpu.SemaphoreType.DMA((28,)), pltpu.SemaphoreType.DMA((28,))])
        outs = pl.pallas_call(
            functools.partial(ocean_kernel, tuple(mesh.axis_names), n_col, n_row, n_sub),
            out_shape=[tile] * 8 + [sweep] * 4,
            in_specs=[hbm] * 11,
            out_specs=[vmem] * 12,
            scratch_shapes=scratch,
            compiler_params=pltpu.CompilerParams(collective_id=0, has_side_effects=True, vmem_limit_bytes=32 * 1024 * 1024),
        )(*[pltpu.with_memory_space_constraint(a, pltpu.HBM) for a in (vel_u, vel_v, value_a11, salinity, surf_eta, trans_u, trans_v, bottom_depth, level_count, avg_weights, table)])
        eta, tu, tv, gu, gv, cu, cv, cc, xu, xv, xt, xs = [pltpu.with_memory_space_constraint(o, pltpu.VMEM) for o in outs]

        part = 16
        big = pl.BlockSpec((1, SLOT, part, L), lambda t, r: (t, 0, r, 0))
        small = pl.BlockSpec((1, part, L), lambda t, r: (t, r, 0))
        out = pl.BlockSpec((LEV, part, L), lambda t, r: (0, r, t))
        out_flat = pl.BlockSpec((part, L), lambda t, r: (r, t))
        cube = jax.ShapeDtypeStruct((LEV, NR, NC), f32)
        flat = jax.ShapeDtypeStruct((NR, NC), f32)
        return tuple(pl.pallas_call(
            final_kernel,
            grid=(NT, NR // part),
            out_shape=[flat] * 3 + [cube] * 4,
            in_specs=[smem] + [big] * 4 + [small] * 8,
            out_specs=[out_flat] * 3 + [out] * 4,
            compiler_params=pltpu.CompilerParams(vmem_limit_bytes=24 * 1024 * 1024),
        )(table, xu, xv, xt, xs, gu, gv, cu, cv, cc, eta, tu, tv))

    cube = P(None, 'row', 'col')
    flat = P('row', 'col')
    return jax.shard_map(step, mesh=mesh, in_specs=(cube, cube, cube, cube, flat, flat, flat, flat, flat, P()), out_specs=(flat, flat, flat, cube, cube, cube, cube), check_vma=False)
```

```python
import functools

import jax
import jax.numpy as jnp
import numpy as np
from jax import lax
from jax.experimental import pallas as pl
from jax.experimental.pallas import tpu as pltpu
from jax.sharding import PartitionSpec as P

TIME_STEP = 1.0
GRAVITY = 16.0
BC_GRAVITY = 4.0
EXPAND_T = 0.2
CONTRACT_S = 0.6
CORIO_F0 = 0.4
CORIO_BETA = 0.4
VISC_R = 2.0
DIFF_R = 0.5

LEV = 31
SLOT = 32
NR = 32
NC = 512
NT = 4
L = 128
R0 = 8
PR = 48
XR = 112
XO = 40
MESH = pl.DeviceIdType.MESH
f32 = jnp.float32
UNROLL_M = 4
UNROLL_T = 1


def solve_table(n_levels):
    rows = []
    for s in (VISC_R, DIFF_R):
        scale, carry, link, last = np.zeros((4, SLOT))
        ratio = 0.0
        for k in range(n_levels):
            low = s if k else 0.0
            full = 1.0 + low + s - low * ratio
            end = 1.0 + low - low * ratio
            scale[k], carry[k], link[k], last[k] = 1.0 / full, low / full, s / full, full / end
            ratio = s / full
        rows += [scale, carry, link, last]
    return np.concatenate(rows).astype(np.float32)


def ocean_kernel(axes, n_col, n_row, n_sub, *refs):
    (u_h, v_h, t_h, s_h, eta_h, tu_h, tv_h, dep_h, cnt_h, w_h, tab_h,
     eta_o, tu_o, tv_o, gu_o, gv_o, cu, cv, cc_o, xu, xv, xt, xs,
     bu, bv, bt, bs, bp, cnt_i, rp, s1, s2,
     pk, rw, re, ha, x, xf, qw, qe, we, ww, fw, fe, fre, frw,
     fu4, fv4, hu, hv, su, sv,
     ca, cb, cc, cd, cg, ch, cm, cn, tt, au, av,
     w_s, tab_s, lsem, ssem, rsem) = refs
    col = lax.axis_index('col')
    row = lax.axis_index('row')
    east = lax.rem(col + 1, n_col)
    west = lax.rem(col + n_col - 1, n_col)
    has_s = row > 0
    has_n = row < n_row - 1

    def dev(c, r):
        at = {'col': c, 'row': r}
        return tuple(at[name] for name in axes)

    bufs = (bu, bv, bt, bs)
    barrier = pltpu.get_barrier_semaphore()

    def signal(c, r):
        pl.semaphore_signal(barrier, inc=1, device_id=dev(c, r), device_id_type=MESH)

    signal(west, row)
    signal(east, row)

    @pl.when(has_s)
    def _():
        for c in (west, col, east):
            signal(c, row - 1)

    @pl.when(has_n)
    def _():
        for c in (west, col, east):
            signal(c, row + 1)

    zero = functools.partial(jnp.zeros, dtype=f32)

    loads = []
    for f, (src, dst) in enumerate(zip((u_h, v_h, t_h, s_h), bufs)):
        for t in range(NT):
            loads.append(pltpu.make_async_copy(src.at[:, :, L * t:L * t + L], dst.at[t, 0:LEV, R0:R0 + NR, :], lsem.at[len(loads)]))
    flat_loads = []
    for f, src in enumerate((eta_h, tu_h, tv_h)):
        for t in range(NT):
            flat_loads.append(pltpu.make_async_copy(src.at[:, L * t:L * t + L], x.at[f, t, XO:XO + NR, :], lsem.at[len(loads) + len(flat_loads)]))
    for t in range(NT):
        flat_loads.append(pltpu.make_async_copy(dep_h.at[:, L * t:L * t + L], bv.at[t, LEV, R0:R0 + NR, :], lsem.at[len(loads) + len(flat_loads)]))
    for t in range(NT):
        flat_loads.append(pltpu.make_async_copy(cnt_h.at[:, L * t:L * t + L], cnt_i.at[t], lsem.at[len(loads) + len(flat_loads)]))
    scalar_loads = [pltpu.make_async_copy(w_h, w_s, lsem.at[36]), pltpu.make_async_copy(tab_h, tab_s, lsem.at[37])]
    edge_loads = [loads[NT * f + t] for f in range(4) for t in (0, NT - 1)]
    mid_loads = [loads[NT * f + t] for f in range(4) for t in range(1, NT - 1)]
    for cp in edge_loads + flat_loads + mid_loads + scalar_loads:
        cp.start()

    n_copies = 0

    def remote(src, dst, c, r, sends, receives):
        nonlocal n_copies
        i = n_copies
        n_copies += 1
        return (pltpu.make_async_remote_copy(src, dst, ssem.at[i], rsem.at[i], device_id=dev(c, r), device_id_type=MESH), sends, receives)

    def maybe(cond, fn):
        if cond is None:
            fn()
        else:
            pl.when(cond)(fn)

    def start(group):
        for cp, sends, _ in group:
            maybe(sends, cp.start)

    def arrive(group):
        for cp, _, receives in group:
            maybe(receives, cp.wait_recv)

    def drain(group):
        for cp, sends, _ in group:
            maybe(sends, cp.wait_send)

    def rows_of(src, b):
        out = []
        for t in range(NT):
            cols = slice(L * t, L * t + L)
            out += [remote(src.at[:, NR - 1:NR, cols], b.at[t, 0:LEV, R0 - 1:R0, :], col, row + 1, has_n, has_s),
                    remote(src.at[:, 0:1, cols], b.at[t, 0:LEV, R0 + NR:R0 + NR + 1, :], col, row - 1, has_s, has_n)]
        return out

    def slot_of(b):
        return [remote(b.at[:, LEV, R0 + NR - 1:R0 + NR, :], b.at[:, LEV, R0 - 1:R0, :], col, row + 1, has_n, has_s),
                remote(b.at[:, LEV, R0:R0 + 1, :], b.at[:, LEV, R0 + NR:R0 + NR + 1, :], col, row - 1, has_s, has_n)]

    def wide_of(b, lanes_w, lanes_e, from_e, from_w):
        own = b.at[:, 0:NT, XO:XO + NR, :]
        return [remote(own, b.at[:, 0:NT, 8:XO, :], col, row + 1, has_n, has_s),
                remote(own, b.at[:, 0:NT, XO + NR:XO + 2 * NR, :], col, row - 1, has_s, has_n),
                remote(lanes_w, from_e.at[1], west, row, None, None),
                remote(lanes_e, from_w.at[1], east, row, None, None),
                remote(lanes_w, from_e.at[2], west, row - 1, has_s, has_n),
                remote(lanes_e, from_w.at[2], east, row - 1, has_s, has_n),
                remote(lanes_w, from_e.at[0], west, row + 1, has_n, has_s),
                remote(lanes_e, from_w.at[0], east, row + 1, has_n, has_s)]

    row_group = rows_of(s_h, bs) + rows_of(t_h, bt) + rows_of(u_h, bu) + rows_of(v_h, bv)
    slot_group = slot_of(bu) + slot_of(bv)
    lane_group = [remote(pk, re.at[:, R0:R0 + NR, :], west, row, None, None),
                  remote(pk, rw.at[:, R0:R0 + NR, :], east, row, None, None),
                  remote(pk.at[:, 0:1, :], rw.at[:, R0 + NR:R0 + NR + 1, :], east, row - 1, has_s, has_n),
                  remote(pk.at[:, NR - 1:NR, :], re.at[:, R0 - 1:R0, :], west, row + 1, has_n, has_s)]
    wide_group = wide_of(x, qw, qe, we, ww)
    force_group = wide_of(xf, fw, fe, fre, frw)

    edge = jnp.logical_or(row == 0, row == n_row - 1)

    @pl.when(edge)
    def _():
        pl.semaphore_wait(barrier, 5)

    @pl.when(jnp.logical_not(edge))
    def _():
        pl.semaphore_wait(barrier, 8)

    start(row_group)
    lane_p = lax.broadcasted_iota(jnp.int32, (PR, L), 1)
    lane = lane_p[:NR]

    for t in range(NT):
        bt[t, LEV, R0:R0 + NR, :] = zero((NR, L))
        bs[t, LEV, R0:R0 + NR, :] = zero((NR, L))
    for cp in flat_loads:
        cp.wait()
    for t in range(NT):
        count = cnt_i[t].astype(f32)
        bu[t, LEV, R0:R0 + NR, :] = count
        x[3, t, XO:XO + NR, :] = jnp.where(count > 0.0, bv[t, LEV, R0:R0 + NR, :], 0.0)

    def roll(a, shift):
        return pltpu.roll(a, shift, 1) if not (isinstance(shift, int) and shift % L == 0) else a

    def pack_wide(b, n_fields):
        first = last = zero((NR, L))
        for f in range(n_fields):
            mine = (lane >= 32 * f) & (lane < 32 * f + 32)
            first = jnp.where(mine, roll(b[f, 0, XO:XO + NR, :], 32 * f), first)
            last = jnp.where(mine, roll(b[f, NT - 1, XO:XO + NR, :], (32 * f + 32) % L), last)
        return first, last

    first, last = pack_wide(x, 4)
    qw[...] = first
    qe[...] = last

    pair = lax.shift_right_logical(lane, 1)
    packed = [zero((NR, L))] * 2
    for f, b in enumerate(bufs):
        edge_loads[2 * f].wait()
        edge_loads[2 * f + 1].wait()
        for k in range(SLOT):
            p = SLOT * (f % 2) + k
            both = jnp.where(lane == 0, b[0, k, R0:R0 + NR, :], b[NT - 1, k, R0:R0 + NR, :])
            packed[f // 2] = jnp.where(pair == p, roll(both, (2 * p + 1) % L), packed[f // 2])
    pk[0] = packed[0]
    pk[1] = packed[1]
    start(slot_group)
    start(lane_group)
    start(wide_group)
    for cp in mid_loads:
        cp.wait()
    for cp in scalar_loads:
        cp.wait()

    for f in range(4):
        for t in range(NT + 1):
            x[f, t, 0:8, :] = zero((8, L))
            x[f, t, XR - 8:XR, :] = zero((8, L))
    for t in range(NT + 1):
        tt[t, XR - 8:XR, :] = zero((8, L))
    for t in range(NT):
        for a in (xu, xv, xt, xs):
            a[t, 0] = zero((NR, L))

    @pl.when(jnp.logical_not(has_s))
    def _():
        for b in bufs:
            b[:, :, R0 - 8:R0, :] = zero((NT, SLOT, 8, L))
        re[:, R0 - 8:R0, :] = zero((2, 8, L))
        x[:, 0:NT, 8:XO, :] = zero((4, NT, NR, L))
        xf[:, 0:NT, 8:XO, :] = zero((2, NT, NR, L))
        for a in (we, ww, fre, frw):
            a[0] = zero((NR, L))

    @pl.when(jnp.logical_not(has_n))
    def _():
        for b in bufs:
            b[:, :, R0 + NR:PR, :] = zero((NT, SLOT, 8, L))
        rw[:, R0 + NR:PR, :] = zero((2, 8, L))
        x[:, 0:NT, XO + NR:XO + 2 * NR, :] = zero((4, NT, NR, L))
        xf[:, 0:NT, XO + NR:XO + 2 * NR, :] = zero((2, NT, NR, L))
        for a in (we, ww, fre, frw):
            a[2] = zero((NR, L))


    row_pos = (row * NR + lax.broadcasted_iota(jnp.int32, (NR, L), 0)).astype(f32)
    total_rows = NR * n_row
    fu4[...] = 0.25 * (CORIO_F0 + CORIO_BETA * ((row_pos + 0.5) / total_rows - 0.5))
    fv4[...] = 0.25 * (CORIO_F0 + CORIO_BETA * ((row_pos + 1.0) / total_rows - 0.5))

    def to_east(tiles, halo):
        last_lane = lane_p[:halo.shape[0]] == L - 1
        rolled = [roll(a, L - 1) for a in tiles] + [halo]
        return [jnp.where(last_lane, rolled[t + 1], rolled[t]) for t in range(NT)]

    def to_west(tiles, halo):
        first_lane = lane_p[:halo.shape[0]] == 0
        rolled = [halo] + [roll(a, 1) for a in tiles]
        return [jnp.where(first_lane, rolled[t], rolled[t + 1]) for t in range(NT)]

    def side(f, k, lo=R0, n=NR):
        return pltpu.roll(ha[f // 2, lo:lo + n, :], lax.rem(L - 2 * (SLOT * (f % 2) + k), L), 1)

    def level(b, k, lo=R0, n=NR):
        return [b[t, k, lo:lo + n, :] for t in range(NT)]

    def each_level(fn, unroll):
        def some(i, _):
            base = i * unroll
            for j in range(unroll):
                fn(base + j, base + j - 1 if j else jnp.maximum(base - 1, 0), j % 2)
            return 0

        lax.fori_loop(0, -(-LEV // unroll), some, 0)

    p_scale = BC_GRAVITY / LEV

    def pressure(t, lo, n):
        total = zero((n, L))
        for k in range(LEV):
            density = CONTRACT_S * bs[t, k, lo:lo + n, :] - EXPAND_T * bt[t, k, lo:lo + n, :]
            total = total + density
            bp[t, k, lo:lo + n, :] = p_scale * (total - 0.5 * density)
        bp[t, LEV, lo:lo + n, :] = zero((n, L))

    def own_pressure(t, _):
        pressure(t, R0, NR)
        return 0

    lax.fori_loop(0, NT, own_pressure, 0)

    def momentum_down(k, prev, slot):
        scale, carry = tab_s[k], tab_s[SLOT + k]
        u5, v5 = level(bu, k, R0, NR + 8), level(bv, k, R0 - 8, NR + 8)
        u_side, v_side = side(0, k, R0, NR + 8), side(1, k, R0 - 8, NR + 8)
        uw, ve = to_west(u5, u_side), to_east(v5, v_side)
        um, vm = [a[:NR] for a in u5], [a[8:] for a in v5]
        ue, vw = to_east(um, u_side[:NR]), to_west(vm, v_side[8:])
        pm, pn = level(bp, k), level(bp, k, R0 + 1)
        pe_ = to_east(pm, pltpu.roll(rp[...], L - 1 - 2 * k, 1))
        for t in range(NT):
            u_sum, v_sum = u5[t] + uw[t], v5[t] + ve[t]
            s1[slot, t] = u_sum
            s2[slot, t] = v_sum
            ub4 = u_sum[:NR] + s1[slot, t, 1:NR + 1, :]
            vb4 = v_sum[8:] + s2[slot, t, 7:NR + 7, :]
            un, us = bu[t, k, R0 + 1:R0 + 1 + NR, :], bu[t, k, R0 - 1:R0 - 1 + NR, :]
            vn, vs = bv[t, k, R0 + 1:R0 + 1 + NR, :], bv[t, k, R0 - 1:R0 - 1 + NR, :]
            u_star = um[t] + vb4 * (fu4[...] - 0.125 * (un - us)) - um[t] * (0.5 * (ue[t] - uw[t][:NR])) + (pm[t] - pe_[t])
            v_star = vm[t] - ub4 * (fv4[...] + 0.125 * (ve[t][8:] - vw[t])) - vm[t] * (0.5 * (vn - vs)) + (pm[t] - pn[t])
            xu[t, k] = scale * u_star + carry * xu[t, prev]
            xv[t, k] = scale * v_star + carry * xv[t, prev]

    arrive(lane_group)
    for j in range(2):
        ha[j] = jnp.where(lax.rem(lane_p, 2) == 0, rw[j], roll(re[j], L - 2))
    east_ = roll(ha[1, R0:R0 + NR, :], 1)
    density = CONTRACT_S * roll(east_, L // 2) - EXPAND_T * east_
    total = density
    for step in (2, 4, 8, 16, 32):
        total = total + jnp.where(lane >= step, roll(total, step), 0.0)
    rp[...] = p_scale * (total - 0.5 * density)
    arrive(row_group)
    arrive(slot_group)

    def north_pressure(t, _):
        pressure(t, R0 + NR, 8)
        return 0

    lax.fori_loop(0, NT, north_pressure, 0)
    each_level(momentum_down, UNROLL_M)

    c_mid, d_mid = level(bu, LEV), level(bv, LEV)
    c_east = to_east(c_mid, side(0, LEV))
    d_east = to_east(d_mid, side(1, LEV))
    c_north, c_south = level(bu, LEV, R0 + 1), level(bu, LEV, R0 - 1)
    d_north = level(bv, LEV, R0 + 1)
    for t in range(NT):
        cu[t] = jnp.minimum(c_mid[t], c_east[t])
        cv[t] = jnp.minimum(c_mid[t], c_north[t])
        hu[t] = 0.5 * (d_mid[t] + d_east[t])
        hv[t] = 0.5 * (d_mid[t] + d_north[t])
        cc_o[t] = c_mid[t]
    c_west0 = jnp.minimum(side(0, LEV), c_mid[0])

    def momentum_up(t, _):
        z = zero((NR, L))
        state = [[z, z, z], [z, z, z]]
        for k in range(LEV - 1, -1, -1):
            link, last_ = tab_s[2 * SLOT + k], tab_s[3 * SLOT + k]
            for q, (sweep, b, count) in enumerate(((xu, bu, cu), (xv, bv, cv))):
                below, sum_x, sum_0 = state[q]
                value = sweep[t, k]
                active = count[t] > float(k)
                solved = jnp.where(count[t] > float(k + 1), value + link * below, jnp.where(active, last_ * value, 0.0))
                sweep[t, k] = solved
                start_ = jnp.where(active, b[t, k, R0:R0 + NR, :], 0.0)
                b[t, k, R0:R0 + NR, :] = start_
                state[q] = [solved, sum_x + solved, sum_0 + start_]
        for q, (h, mean, count) in enumerate(((hu, su, cu), (hv, sv, cv))):
            _, total, start_ = state[q]
            n_active = jnp.maximum(count[t], 1.0)
            mean[t] = total / n_active
            xf[q, t, XO:XO + NR, :] = h[t] * (total - start_) / n_active / TIME_STEP
        c_south = jnp.minimum(bu[t, LEV, 0:8, :], pltpu.roll(bu[t, LEV, R0:R0 + 8, :], 7, 0))
        for k in range(LEV):
            bv[t, k, 0:8, :] = jnp.where(c_south > float(k), bv[t, k, 0:8, :], 0.0)
        return 0

    lax.fori_loop(0, NT, momentum_up, 0)

    first, last = pack_wide(xf, 2)
    fw[...] = first
    fe[...] = last
    start(force_group)

    def tracer_down(k, prev, slot):
        scale, carry = tab_s[4 * SLOT + k], tab_s[5 * SLOT + k]
        kf = lax.convert_element_type(k, f32)
        um, vm, vs = level(bu, k), level(bv, k), level(bv, k, R0 - 1)
        uw0 = jnp.where(c_west0 > kf, side(0, k), 0.0)
        for f, b, sweep in ((2, bt, xt), (3, bs, xs)):
            q = level(b, k)
            q_side = side(f, k)
            qe_ = to_east(q, q_side)
            f_east = [um[t] * (q[t] + qe_[t]) for t in range(NT)]
            f_west = to_west(f_east, uw0 * (q_side + q[0]))
            for t in range(NT):
                f_north = vm[t] * (q[t] + b[t, k, R0 + 1:R0 + 1 + NR, :])
                f_south = vs[t] * (b[t, k, R0 - 1:R0 - 1 + NR, :] + q[t])
                new = q[t] - 0.5 * TIME_STEP * (f_east[t] - f_west[t] + f_north - f_south)
                sweep[t, k] = jnp.where(bu[t, LEV, R0:R0 + NR, :] > kf, scale * new + carry * sweep[t, prev], new)

    each_level(tracer_down, UNROLL_T)

    arrive(wide_group)
    drain(wide_group)
    arrive(force_group)

    def unpack_wide(b, from_e, from_w, n_fields):
        for f in range(n_fields):
            for seg in range(3):
                b[f, NT, 8 + NR * seg:8 + NR * seg + NR, :] = jnp.where(lane < L // 2, roll(from_e[seg], (L - 32 * f) % L), roll(from_w[seg], (96 - 32 * f) % L))

    unpack_wide(x, we, ww, 4)
    unpack_wide(xf, fre, frw, 2)
    dt_fast = TIME_STEP / n_sub
    XT = NT + 1

    def ring_east(tiles, last_lane):
        rolled = [roll(a, L - 1) for a in tiles]
        return [jnp.where(last_lane, rolled[(t + 1) % XT], rolled[t]) for t in range(XT)]

    def ring_west(tiles, first_lane):
        rolled = [roll(a, 1) for a in tiles]
        return [jnp.where(first_lane, rolled[(t - 1) % XT], rolled[t]) for t in range(XT)]

    for seg in range(3):
        lo = 8 + NR * seg
        pos = (row * NR + NR * (seg - 1) + lax.broadcasted_iota(jnp.int32, (NR, L), 0)).astype(f32)
        f_u = CORIO_F0 + CORIO_BETA * ((pos + 0.5) / total_rows - 0.5)
        f_v = CORIO_F0 + CORIO_BETA * ((pos + 1.0) / total_rows - 0.5)
        d = [x[3, t, lo:lo + NR, :] for t in range(XT)]
        d_e = ring_east(d, lane == L - 1)
        for t in range(XT):
            d_n = x[3, t, lo + 1:lo + 1 + NR, :]
            wet = jnp.where((d[t] > 0.0) & (d_e[t] > 0.0), 1.0, 0.0)
            cm[t, lo:lo + NR, :] = wet
            ca[t, lo:lo + NR, :] = (0.25 * dt_fast) * f_u * wet
            cb[t, lo:lo + NR, :] = (dt_fast * GRAVITY * 0.5) * (d[t] + d_e[t]) * wet
            cc[t, lo:lo + NR, :] = dt_fast * xf[0, t, lo:lo + NR, :] * wet
            wet = jnp.where((d[t] > 0.0) & (d_n > 0.0), 1.0, 0.0)
            cn[t, lo:lo + NR, :] = wet
            cd[t, lo:lo + NR, :] = (0.25 * dt_fast) * f_v * wet
            cg[t, lo:lo + NR, :] = (dt_fast * GRAVITY * 0.5) * (d[t] + d_n) * wet
            ch[t, lo:lo + NR, :] = dt_fast * xf[1, t, lo:lo + NR, :] * wet

    for t in range(NT):
        au[t] = zero((NR, L))
        av[t] = zero((NR, L))

    def subcycle(lo, hi, chunk, masked, n, _):
        lane_c = lax.broadcasted_iota(jnp.int32, (chunk, L), 1)
        first_lane, last_lane = lane_c == 0, lane_c == L - 1
        weight = w_s[n]
        for r in range(lo, hi, chunk):
            u_t = [x[1, t, r:r + chunk, :] for t in range(XT)]
            u_w = ring_west(u_t, first_lane)
            for t in range(XT):
                v_t, v_s = x[2, t, r:r + chunk, :], x[2, t, r - 1:r - 1 + chunk, :]
                x[0, t, r:r + chunk, :] = x[0, t, r:r + chunk, :] - dt_fast * ((u_t[t] - u_w[t]) + (v_t - v_s))
                tt[t, r:r + chunk, :] = u_t[t] + u_w[t]
        for r in range(hi - chunk, lo - 1, -chunk):
            e_t = [x[0, t, r:r + chunk, :] for t in range(XT)]
            e_e = ring_east(e_t, last_lane)
            v_t = [x[2, t, r:r + chunk, :] for t in range(XT)]
            s_t = [v_t[t] + x[2, t, r - 1:r - 1 + chunk, :] for t in range(XT)]
            s_e = ring_east(s_t, last_lane)
            for t in range(XT):
                at = (t, slice(r, r + chunk))
                up = (t, slice(r + 1, r + 1 + chunk))
                e_n = x[0, t, r + 1:r + 1 + chunk, :]
                u_old = x[1, t, r:r + chunk, :] if masked else cm[at] * x[1, t, r:r + chunk, :]
                v_old = v_t[t] if masked else cn[at] * v_t[t]
                x[1, t, r:r + chunk, :] = u_old + ca[at] * (s_t[t] + s_e[t]) + cc[at] - cb[at] * (e_e[t] - e_t[t])
                x[2, t, r:r + chunk, :] = v_old - cd[at] * (tt[at] + tt[up]) + ch[at] - cg[at] * (e_n - e_t[t])
        for t in range(NT):
            au[t] += weight * x[1, t, XO:XO + NR, :]
            av[t] += weight * x[2, t, XO:XO + NR, :]
        return 0

    done = 0
    for side in (4, 3, 2, 1):
        until = n_sub - 8 * (side - 1)
        rows = NR + 16 * side
        chunk = {4: 32, 3: 40, 2: 32, 1: 24}[side]
        stretch = functools.partial(subcycle, XO - 8 * side, XO - 8 * side + rows, chunk)
        if done == 0:
            stretch(False, 0, 0)
            done = 1
        lax.fori_loop(done, until, functools.partial(stretch, True), 0)
        done = until

    for t in range(NT):
        eta_o[t] = x[0, t, XO:XO + NR, :]
        tu_o[t] = x[1, t, XO:XO + NR, :]
        tv_o[t] = x[2, t, XO:XO + NR, :]
        gu_o[t] = au[t] / hu[t] - su[t]
        gv_o[t] = av[t] / hv[t] - sv[t]

    for group in (row_group, slot_group, lane_group, force_group):
        drain(group)


def final_kernel(tab_s, xu, xv, xt, xs, gu, gv, cu, cv, cc, eta, tu, tv, eta_o, tu_o, tv_o, u_o, v_o, t_o, s_o):
    n = u_o.shape[1]
    rows = pl.ds(pl.multiple_of(pl.program_id(0) * n, n), n)
    for t in range(NT):
        cols = slice(L * t, L * t + L)
        eta_o[:, cols], tu_o[:, cols], tv_o[:, cols] = eta[t, rows], tu[t, rows], tv[t, rows]
    c_u, c_v, c_c, g_u, g_v = [[a[t, rows] for t in range(NT)] for a in (cu, cv, cc, gu, gv)]
    state = [jnp.zeros((n, L), f32)] * (2 * NT)
    for k in range(LEV - 1, -1, -1):
        kf = float(k)
        link, last = tab_s[6 * SLOT + k], tab_s[7 * SLOT + k]
        for t in range(NT):
            cols = slice(L * t, L * t + L)
            u_o[k, :, cols] = jnp.where(c_u[t] > kf, xu[t, k, rows] + g_u[t], 0.0)
            v_o[k, :, cols] = jnp.where(c_v[t] > kf, xv[t, k, rows] + g_v[t], 0.0)
            inner, active = c_c[t] > kf + 1.0, c_c[t] > kf
            for q, (sweep, o) in enumerate(((xt, t_o), (xs, s_o))):
                value = sweep[t, k, rows]
                solved = jnp.where(inner, value + link * state[2 * t + q], jnp.where(active, last * value, value))
                o[k, :, cols] = solved
                state[2 * t + q] = solved


def solution(mesh):
    n_col = mesh.shape['col']
    n_row = mesh.shape['row']

    def step(vel_u, vel_v, value_a11, salinity, surf_eta, trans_u, trans_v, bottom_depth, level_count, avg_weights):
        n_sub = avg_weights.shape[0]
        table = jnp.asarray(solve_table(LEV))
        hbm = pl.BlockSpec(memory_space=pltpu.HBM)
        vmem = pl.BlockSpec(memory_space=pltpu.VMEM)
        smem = pl.BlockSpec(memory_space=pltpu.SMEM)
        V = pltpu.VMEM
        tile = V((NT, NR, L), f32)
        sweep = V((NT, SLOT, NR, L), f32)
        wide = (NT + 1, XR, L)
        scratch = ([V((NT, SLOT, PR, L), f32)] * 5 + [V((NT, NR, L), jnp.int32), V((NR, L), f32)]
                   + [V((2, NT, NR + 8, L), f32)] * 2 + [V((2, NR, L), f32)] + [V((2, PR, L), f32)] * 3
                   + [V((4,) + wide, f32), V((2,) + wide, f32)] + [V((NR, L), f32)] * 2 + [V((3, NR, L), f32)] * 2
                   + [V((NR, L), f32)] * 2 + [V((3, NR, L), f32)] * 2
                   + [V((NR, L), f32)] * 2 + [V((NT, NR, L), f32)] * 4
                   + [V(wide, f32)] * 9 + [V((NT, NR, L), f32)] * 2
                   + [pltpu.SMEM((n_sub,), f32), pltpu.SMEM((8 * SLOT,), f32)]
                   + [pltpu.SemaphoreType.DMA((40,)), pltpu.SemaphoreType.DMA((64,)), pltpu.SemaphoreType.DMA((64,))])
        outs = pl.pallas_call(
            functools.partial(ocean_kernel, tuple(mesh.axis_names), n_col, n_row, n_sub),
            out_shape=[tile] * 8 + [sweep] * 4,
            in_specs=[hbm] * 11,
            out_specs=[vmem] * 12,
            scratch_shapes=scratch,
            compiler_params=pltpu.CompilerParams(collective_id=0, has_side_effects=True, vmem_limit_bytes=32 * 1024 * 1024),
        )(*[pltpu.with_memory_space_constraint(a, pltpu.HBM) for a in (vel_u, vel_v, value_a11, salinity, surf_eta, trans_u, trans_v, bottom_depth, level_count, avg_weights, table)])
        eta, tu, tv, gu, gv, cu, cv, cc, xu, xv, xt, xs = [pltpu.with_memory_space_constraint(o, pltpu.VMEM) for o in outs]

        part = 8
        out = pl.BlockSpec((LEV, part, NC), lambda r: (0, r, 0))
        out_flat = pl.BlockSpec((part, NC), lambda r: (r, 0))
        cube = jax.ShapeDtypeStruct((LEV, NR, NC), f32)
        flat = jax.ShapeDtypeStruct((NR, NC), f32)
        return tuple(pl.pallas_call(
            final_kernel,
            grid=(NR // part,),
            out_shape=[flat] * 3 + [cube] * 4,
            in_specs=[smem] + [vmem] * 12,
            out_specs=[out_flat] * 3 + [out] * 4,
            compiler_params=pltpu.CompilerParams(vmem_limit_bytes=24 * 1024 * 1024),
        )(table, xu, xv, xt, xs, gu, gv, cu, cv, cc, eta, tu, tv))

    cube = P(None, 'row', 'col')
    flat = P('row', 'col')
    return jax.shard_map(step, mesh=mesh, in_specs=(cube, cube, cube, cube, flat, flat, flat, flat, flat, P()), out_specs=(flat, flat, flat, cube, cube, cube, cube), check_vma=False)
```

```python
import functools

import jax
import jax.numpy as jnp
import numpy as np
from jax import lax
from jax.experimental import pallas as pl
from jax.experimental.pallas import tpu as pltpu
from jax.sharding import PartitionSpec as P

TIME_STEP = 1.0
GRAVITY = 16.0
BC_GRAVITY = 4.0
EXPAND_T = 0.2
CONTRACT_S = 0.6
CORIO_F0 = 0.4
CORIO_BETA = 0.4
VISC_R = 2.0
DIFF_R = 0.5

LEV = 31
SLOT = 32
NR = 32
NC = 512
NT = 4
L = 128
R0 = 8
PR = 48
XR = 112
XO = 40
MESH = pl.DeviceIdType.MESH
f32 = jnp.float32
UNROLL_M = 4
UNROLL_T = 1


def solve_table(n_levels):
    rows = []
    for s in (VISC_R, DIFF_R):
        scale, carry, link, last = np.zeros((4, SLOT))
        ratio = 0.0
        for k in range(n_levels):
            low = s if k else 0.0
            full = 1.0 + low + s - low * ratio
            end = 1.0 + low - low * ratio
            scale[k], carry[k], link[k], last[k] = 1.0 / full, low / full, s / full, full / end
            ratio = s / full
        rows += [scale, carry, link, last]
    return np.concatenate(rows).astype(np.float32)


def ocean_kernel(axes, n_col, n_row, n_sub, *refs):
    (u_h, v_h, t_h, s_h, eta_h, tu_h, tv_h, dep_h, cnt_h, w_h, tab_h,
     eta_o, tu_o, tv_o, gu_o, gv_o, cu, cv, cc_o, xu, xv, xt, xs,
     bu, bv, bt, bs, bp, cnt_i, rp, s1, s2,
     pk, rw, re, ha, x, xf, qw, qe, we, ww, fw, fe, fre, frw,
     fu4, fv4, hu, hv, su, sv,
     ca, cb, cc, cd, cg, ch, cm, cn, tt, au, av,
     w_s, tab_s, lsem, ssem, rsem) = refs
    col = lax.axis_index('col')
    row = lax.axis_index('row')
    east = lax.rem(col + 1, n_col)
    west = lax.rem(col + n_col - 1, n_col)
    has_s = row > 0
    has_n = row < n_row - 1

    def dev(c, r):
        at = {'col': c, 'row': r}
        return tuple(at[name] for name in axes)

    bufs = (bu, bv, bt, bs)
    barrier = pltpu.get_barrier_semaphore()

    def signal(c, r):
        pl.semaphore_signal(barrier, inc=1, device_id=dev(c, r), device_id_type=MESH)

    signal(west, row)
    signal(east, row)

    @pl.when(has_s)
    def _():
        for c in (west, col, east):
            signal(c, row - 1)

    @pl.when(has_n)
    def _():
        for c in (west, col, east):
            signal(c, row + 1)

    zero = functools.partial(jnp.zeros, dtype=f32)

    loads = []
    for f, (src, dst) in enumerate(zip((u_h, v_h, t_h, s_h), bufs)):
        for t in range(NT):
            loads.append(pltpu.make_async_copy(src.at[:, :, L * t:L * t + L], dst.at[t, 0:LEV, R0:R0 + NR, :], lsem.at[len(loads)]))
    flat_loads = []
    for f, src in enumerate((eta_h, tu_h, tv_h)):
        for t in range(NT):
            flat_loads.append(pltpu.make_async_copy(src.at[:, L * t:L * t + L], x.at[f, t, XO:XO + NR, :], lsem.at[len(loads) + len(flat_loads)]))
    for t in range(NT):
        flat_loads.append(pltpu.make_async_copy(dep_h.at[:, L * t:L * t + L], bv.at[t, LEV, R0:R0 + NR, :], lsem.at[len(loads) + len(flat_loads)]))
    for t in range(NT):
        flat_loads.append(pltpu.make_async_copy(cnt_h.at[:, L * t:L * t + L], cnt_i.at[t], lsem.at[len(loads) + len(flat_loads)]))
    scalar_loads = [pltpu.make_async_copy(w_h, w_s, lsem.at[36]), pltpu.make_async_copy(tab_h, tab_s, lsem.at[37])]
    edge_loads = [loads[NT * f + t] for f in range(4) for t in (0, NT - 1)]
    mid_loads = [loads[NT * f + t] for f in range(4) for t in range(1, NT - 1)]
    for cp in flat_loads[3 * NT:] + edge_loads + flat_loads[:3 * NT] + mid_loads + scalar_loads:
        cp.start()

    n_copies = 0

    def remote(src, dst, c, r, sends, receives):
        nonlocal n_copies
        i = n_copies
        n_copies += 1
        return (pltpu.make_async_remote_copy(src, dst, ssem.at[i], rsem.at[i], device_id=dev(c, r), device_id_type=MESH), sends, receives)

    def maybe(cond, fn):
        if cond is None:
            fn()
        else:
            pl.when(cond)(fn)

    def start(group):
        for cp, sends, _ in group:
            maybe(sends, cp.start)

    def arrive(group):
        for cp, _, receives in group:
            maybe(receives, cp.wait_recv)

    def drain(group):
        for cp, sends, _ in group:
            maybe(sends, cp.wait_send)

    def rows_of(src, b):
        out = []
        for t in range(NT):
            cols = slice(L * t, L * t + L)
            out += [remote(src.at[:, NR - 1:NR, cols], b.at[t, 0:LEV, R0 - 1:R0, :], col, row + 1, has_n, has_s),
                    remote(src.at[:, 0:1, cols], b.at[t, 0:LEV, R0 + NR:R0 + NR + 1, :], col, row - 1, has_s, has_n)]
        return out

    def slot_of(b):
        return [remote(b.at[:, LEV, R0 + NR - 1:R0 + NR, :], b.at[:, LEV, R0 - 1:R0, :], col, row + 1, has_n, has_s),
                remote(b.at[:, LEV, R0:R0 + 1, :], b.at[:, LEV, R0 + NR:R0 + NR + 1, :], col, row - 1, has_s, has_n)]

    def wide_of(b, lanes_w, lanes_e, from_e, from_w):
        own = b.at[:, 0:NT, XO:XO + NR, :]
        return [remote(own, b.at[:, 0:NT, 8:XO, :], col, row + 1, has_n, has_s),
                remote(own, b.at[:, 0:NT, XO + NR:XO + 2 * NR, :], col, row - 1, has_s, has_n),
                remote(lanes_w, from_e.at[1], west, row, None, None),
                remote(lanes_e, from_w.at[1], east, row, None, None),
                remote(lanes_w, from_e.at[2], west, row - 1, has_s, has_n),
                remote(lanes_e, from_w.at[2], east, row - 1, has_s, has_n),
                remote(lanes_w, from_e.at[0], west, row + 1, has_n, has_s),
                remote(lanes_e, from_w.at[0], east, row + 1, has_n, has_s)]

    row_group = rows_of(u_h, bu) + rows_of(v_h, bv)
    late_group = rows_of(s_h, bs) + rows_of(t_h, bt)
    slot_group = slot_of(bu) + slot_of(bv)
    lane_group = [remote(pk, re.at[:, R0:R0 + NR, :], west, row, None, None),
                  remote(pk, rw.at[:, R0:R0 + NR, :], east, row, None, None),
                  remote(pk.at[:, 0:1, :], rw.at[:, R0 + NR:R0 + NR + 1, :], east, row - 1, has_s, has_n),
                  remote(pk.at[:, NR - 1:NR, :], re.at[:, R0 - 1:R0, :], west, row + 1, has_n, has_s)]
    wide_group = wide_of(x, qw, qe, we, ww)
    force_group = wide_of(xf, fw, fe, fre, frw)

    edge = jnp.logical_or(row == 0, row == n_row - 1)

    @pl.when(edge)
    def _():
        pl.semaphore_wait(barrier, 5)

    @pl.when(jnp.logical_not(edge))
    def _():
        pl.semaphore_wait(barrier, 8)

    start(row_group)
    lane_p = lax.broadcasted_iota(jnp.int32, (PR, L), 1)
    lane = lane_p[:NR]

    for t in range(NT):
        bt[t, LEV, R0:R0 + NR, :] = zero((NR, L))
        bs[t, LEV, R0:R0 + NR, :] = zero((NR, L))
    for cp in flat_loads[3 * NT:]:
        cp.wait()
    for t in range(NT):
        count = cnt_i[t].astype(f32)
        bu[t, LEV, R0:R0 + NR, :] = count
        x[3, t, XO:XO + NR, :] = jnp.where(count > 0.0, bv[t, LEV, R0:R0 + NR, :], 0.0)

    start(slot_group)
    start(late_group)

    def roll(a, shift):
        return pltpu.roll(a, shift, 1) if not (isinstance(shift, int) and shift % L == 0) else a

    pair = lax.shift_right_logical(lane, 1)
    packed = [zero((NR, L))] * 2
    for f, b in enumerate(bufs):
        edge_loads[2 * f].wait()
        edge_loads[2 * f + 1].wait()
        for k in range(SLOT):
            p = SLOT * (f % 2) + k
            both = jnp.where(lane == 0, b[0, k, R0:R0 + NR, :], b[NT - 1, k, R0:R0 + NR, :])
            packed[f // 2] = jnp.where(pair == p, roll(both, (2 * p + 1) % L), packed[f // 2])
    pk[0] = packed[0]
    pk[1] = packed[1]
    start(lane_group)

    def pack_wide(b, n_fields):
        first = last = zero((NR, L))
        for f in range(n_fields):
            mine = (lane >= 32 * f) & (lane < 32 * f + 32)
            first = jnp.where(mine, roll(b[f, 0, XO:XO + NR, :], 32 * f), first)
            last = jnp.where(mine, roll(b[f, NT - 1, XO:XO + NR, :], (32 * f + 32) % L), last)
        return first, last

    for cp in flat_loads[:3 * NT]:
        cp.wait()
    first, last = pack_wide(x, 4)
    qw[...] = first
    qe[...] = last
    start(wide_group)
    for cp in mid_loads:
        cp.wait()
    for cp in scalar_loads:
        cp.wait()

    for f in range(4):
        for t in range(NT + 1):
            x[f, t, 0:8, :] = zero((8, L))
            x[f, t, XR - 8:XR, :] = zero((8, L))
    for t in range(NT + 1):
        tt[t, XR - 8:XR, :] = zero((8, L))
    for t in range(NT):
        for a in (xu, xv, xt, xs):
            a[t, 0] = zero((NR, L))

    @pl.when(jnp.logical_not(has_s))
    def _():
        for b in bufs:
            b[:, :, R0 - 8:R0, :] = zero((NT, SLOT, 8, L))
        re[:, R0 - 8:R0, :] = zero((2, 8, L))
        x[:, 0:NT, 8:XO, :] = zero((4, NT, NR, L))
        xf[:, 0:NT, 8:XO, :] = zero((2, NT, NR, L))
        for a in (we, ww, fre, frw):
            a[0] = zero((NR, L))

    @pl.when(jnp.logical_not(has_n))
    def _():
        for b in bufs:
            b[:, :, R0 + NR:PR, :] = zero((NT, SLOT, 8, L))
        rw[:, R0 + NR:PR, :] = zero((2, 8, L))
        x[:, 0:NT, XO + NR:XO + 2 * NR, :] = zero((4, NT, NR, L))
        xf[:, 0:NT, XO + NR:XO + 2 * NR, :] = zero((2, NT, NR, L))
        for a in (we, ww, fre, frw):
            a[2] = zero((NR, L))


    row_pos = (row * NR + lax.broadcasted_iota(jnp.int32, (NR, L), 0)).astype(f32)
    total_rows = NR * n_row
    fu4[...] = 0.25 * (CORIO_F0 + CORIO_BETA * ((row_pos + 0.5) / total_rows - 0.5))
    fv4[...] = 0.25 * (CORIO_F0 + CORIO_BETA * ((row_pos + 1.0) / total_rows - 0.5))

    def to_east(tiles, halo):
        last_lane = lane_p[:halo.shape[0]] == L - 1
        rolled = [roll(a, L - 1) for a in tiles] + [halo]
        return [jnp.where(last_lane, rolled[t + 1], rolled[t]) for t in range(NT)]

    def to_west(tiles, halo):
        first_lane = lane_p[:halo.shape[0]] == 0
        rolled = [halo] + [roll(a, 1) for a in tiles]
        return [jnp.where(first_lane, rolled[t], rolled[t + 1]) for t in range(NT)]

    def side(f, k, lo=R0, n=NR):
        return pltpu.roll(ha[f // 2, lo:lo + n, :], lax.rem(L - 2 * (SLOT * (f % 2) + k), L), 1)

    def level(b, k, lo=R0, n=NR):
        return [b[t, k, lo:lo + n, :] for t in range(NT)]

    def each_level(fn, unroll):
        def some(i, _):
            base = i * unroll
            for j in range(unroll):
                fn(base + j, base + j - 1 if j else jnp.maximum(base - 1, 0), j % 2)
            return 0

        lax.fori_loop(0, -(-LEV // unroll), some, 0)

    p_scale = BC_GRAVITY / LEV

    def pressure(t, lo, n):
        total = zero((n, L))
        for k in range(LEV):
            density = CONTRACT_S * bs[t, k, lo:lo + n, :] - EXPAND_T * bt[t, k, lo:lo + n, :]
            total = total + density
            bp[t, k, lo:lo + n, :] = p_scale * (total - 0.5 * density)
        bp[t, LEV, lo:lo + n, :] = zero((n, L))

    def own_pressure(t, _):
        pressure(t, R0, NR)
        for k in range(LEV):
            bp[t, k, R0 + NR:PR, :] = zero((8, L))
        return 0

    lax.fori_loop(0, NT, own_pressure, 0)

    def momentum_down(k, prev, slot):
        scale, carry = tab_s[k], tab_s[SLOT + k]
        u5, v5 = level(bu, k, R0, NR + 8), level(bv, k, R0 - 8, NR + 8)
        u_side, v_side = side(0, k, R0, NR + 8), side(1, k, R0 - 8, NR + 8)
        uw, ve = to_west(u5, u_side), to_east(v5, v_side)
        um, vm = [a[:NR] for a in u5], [a[8:] for a in v5]
        ue, vw = to_east(um, u_side[:NR]), to_west(vm, v_side[8:])
        pm, pn = level(bp, k), level(bp, k, R0 + 1)
        pe_ = to_east(pm, pltpu.roll(rp[...], L - 1 - 2 * k, 1))
        for t in range(NT):
            u_sum, v_sum = u5[t] + uw[t], v5[t] + ve[t]
            s1[slot, t] = u_sum
            s2[slot, t] = v_sum
            ub4 = u_sum[:NR] + s1[slot, t, 1:NR + 1, :]
            vb4 = v_sum[8:] + s2[slot, t, 7:NR + 7, :]
            un, us = bu[t, k, R0 + 1:R0 + 1 + NR, :], bu[t, k, R0 - 1:R0 - 1 + NR, :]
            vn, vs = bv[t, k, R0 + 1:R0 + 1 + NR, :], bv[t, k, R0 - 1:R0 - 1 + NR, :]
            u_star = um[t] + vb4 * (fu4[...] - 0.125 * (un - us)) - um[t] * (0.5 * (ue[t] - uw[t][:NR])) + (pm[t] - pe_[t])
            v_star = vm[t] - ub4 * (fv4[...] + 0.125 * (ve[t][8:] - vw[t])) - vm[t] * (0.5 * (vn - vs)) + (pm[t] - pn[t])
            xu[t, k] = scale * u_star + carry * xu[t, prev]
            xv[t, k] = scale * v_star + carry * xv[t, prev]

    arrive(lane_group)
    for j in range(2):
        ha[j] = jnp.where(lax.rem(lane_p, 2) == 0, rw[j], roll(re[j], L - 2))
    east_ = roll(ha[1, R0:R0 + NR, :], 1)
    density = CONTRACT_S * roll(east_, L // 2) - EXPAND_T * east_
    total = density
    for step in (2, 4, 8, 16, 32):
        total = total + jnp.where(lane >= step, roll(total, step), 0.0)
    rp[...] = p_scale * (total - 0.5 * density)
    arrive(row_group)
    arrive(slot_group)
    each_level(momentum_down, UNROLL_M)

    arrive(late_group)
    last_row = lax.broadcasted_iota(jnp.int32, (8, L), 0) == 7

    def north_pressure(t, _):
        pressure(t, R0 + NR, 8)
        sweep = zero((8, L))
        for k in range(LEV):
            sweep = tab_s[SLOT + k] * sweep - tab_s[k] * bp[t, k, R0 + NR - 7:R0 + NR + 1, :]
            xv[t, k, NR - 8:NR, :] += jnp.where(last_row, sweep, 0.0)
        return 0

    lax.fori_loop(0, NT, north_pressure, 0)

    c_mid, d_mid = level(bu, LEV), level(bv, LEV)
    c_east = to_east(c_mid, side(0, LEV))
    d_east = to_east(d_mid, side(1, LEV))
    c_north, c_south = level(bu, LEV, R0 + 1), level(bu, LEV, R0 - 1)
    d_north = level(bv, LEV, R0 + 1)
    for t in range(NT):
        cu[t] = jnp.minimum(c_mid[t], c_east[t])
        cv[t] = jnp.minimum(c_mid[t], c_north[t])
        hu[t] = 0.5 * (d_mid[t] + d_east[t])
        hv[t] = 0.5 * (d_mid[t] + d_north[t])
        cc_o[t] = c_mid[t]
    c_west0 = jnp.minimum(side(0, LEV), c_mid[0])

    def momentum_up(t, _):
        z = zero((NR, L))
        state = [[z, z, z], [z, z, z]]
        for k in range(LEV - 1, -1, -1):
            link, last_ = tab_s[2 * SLOT + k], tab_s[3 * SLOT + k]
            for q, (sweep, b, count) in enumerate(((xu, bu, cu), (xv, bv, cv))):
                below, sum_x, sum_0 = state[q]
                value = sweep[t, k]
                active = count[t] > float(k)
                solved = jnp.where(count[t] > float(k + 1), value + link * below, jnp.where(active, last_ * value, 0.0))
                sweep[t, k] = solved
                start_ = jnp.where(active, b[t, k, R0:R0 + NR, :], 0.0)
                b[t, k, R0:R0 + NR, :] = start_
                state[q] = [solved, sum_x + solved, sum_0 + start_]
        for q, (h, mean, count) in enumerate(((hu, su, cu), (hv, sv, cv))):
            _, total, start_ = state[q]
            n_active = jnp.maximum(count[t], 1.0)
            mean[t] = total / n_active
            xf[q, t, XO:XO + NR, :] = h[t] * (total - start_) / n_active / TIME_STEP
        c_south = jnp.minimum(bu[t, LEV, 0:8, :], pltpu.roll(bu[t, LEV, R0:R0 + 8, :], 7, 0))
        for k in range(LEV):
            bv[t, k, 0:8, :] = jnp.where(c_south > float(k), bv[t, k, 0:8, :], 0.0)
        return 0

    lax.fori_loop(0, NT, momentum_up, 0)

    first, last = pack_wide(xf, 2)
    fw[...] = first
    fe[...] = last
    start(force_group)

    def tracer_down(k, prev, slot):
        scale, carry = tab_s[4 * SLOT + k], tab_s[5 * SLOT + k]
        kf = lax.convert_element_type(k, f32)
        um, vm, vs = level(bu, k), level(bv, k), level(bv, k, R0 - 1)
        uw0 = jnp.where(c_west0 > kf, side(0, k), 0.0)
        for f, b, sweep in ((2, bt, xt), (3, bs, xs)):
            q = level(b, k)
            q_side = side(f, k)
            qe_ = to_east(q, q_side)
            f_east = [um[t] * (q[t] + qe_[t]) for t in range(NT)]
            f_west = to_west(f_east, uw0 * (q_side + q[0]))
            for t in range(NT):
                f_north = vm[t] * (q[t] + b[t, k, R0 + 1:R0 + 1 + NR, :])
                f_south = vs[t] * (b[t, k, R0 - 1:R0 - 1 + NR, :] + q[t])
                new = q[t] - 0.5 * TIME_STEP * (f_east[t] - f_west[t] + f_north - f_south)
                sweep[t, k] = jnp.where(bu[t, LEV, R0:R0 + NR, :] > kf, scale * new + carry * sweep[t, prev], new)

    each_level(tracer_down, UNROLL_T)

    arrive(wide_group)
    drain(wide_group)
    arrive(force_group)

    def unpack_wide(b, from_e, from_w, n_fields):
        for f in range(n_fields):
            for seg in range(3):
                b[f, NT, 8 + NR * seg:8 + NR * seg + NR, :] = jnp.where(lane < L // 2, roll(from_e[seg], (L - 32 * f) % L), roll(from_w[seg], (96 - 32 * f) % L))

    unpack_wide(x, we, ww, 4)
    unpack_wide(xf, fre, frw, 2)
    dt_fast = TIME_STEP / n_sub
    XT = NT + 1

    def ring_east(tiles, last_lane):
        rolled = [roll(a, L - 1) for a in tiles]
        return [jnp.where(last_lane, rolled[(t + 1) % XT], rolled[t]) for t in range(XT)]

    def ring_west(tiles, first_lane):
        rolled = [roll(a, 1) for a in tiles]
        return [jnp.where(first_lane, rolled[(t - 1) % XT], rolled[t]) for t in range(XT)]

    for seg in range(3):
        lo = 8 + NR * seg
        pos = (row * NR + NR * (seg - 1) + lax.broadcasted_iota(jnp.int32, (NR, L), 0)).astype(f32)
        f_u = CORIO_F0 + CORIO_BETA * ((pos + 0.5) / total_rows - 0.5)
        f_v = CORIO_F0 + CORIO_BETA * ((pos + 1.0) / total_rows - 0.5)
        d = [x[3, t, lo:lo + NR, :] for t in range(XT)]
        d_e = ring_east(d, lane == L - 1)
        for t in range(XT):
            d_n = x[3, t, lo + 1:lo + 1 + NR, :]
            wet = jnp.where((d[t] > 0.0) & (d_e[t] > 0.0), 1.0, 0.0)
            cm[t, lo:lo + NR, :] = wet
            ca[t, lo:lo + NR, :] = (0.25 * dt_fast) * f_u * wet
            cb[t, lo:lo + NR, :] = (dt_fast * GRAVITY * 0.5) * (d[t] + d_e[t]) * wet
            cc[t, lo:lo + NR, :] = dt_fast * xf[0, t, lo:lo + NR, :] * wet
            wet = jnp.where((d[t] > 0.0) & (d_n > 0.0), 1.0, 0.0)
            cn[t, lo:lo + NR, :] = wet
            cd[t, lo:lo + NR, :] = (0.25 * dt_fast) * f_v * wet
            cg[t, lo:lo + NR, :] = (dt_fast * GRAVITY * 0.5) * (d[t] + d_n) * wet
            ch[t, lo:lo + NR, :] = dt_fast * xf[1, t, lo:lo + NR, :] * wet

    for t in range(NT):
        au[t] = zero((NR, L))
        av[t] = zero((NR, L))

    def subcycle(lo, hi, chunk, masked, n, _):
        lane_c = lax.broadcasted_iota(jnp.int32, (chunk, L), 1)
        first_lane, last_lane = lane_c == 0, lane_c == L - 1
        weight = w_s[n]
        for r in range(lo, hi, chunk):
            u_t = [x[1, t, r:r + chunk, :] for t in range(XT)]
            u_w = ring_west(u_t, first_lane)
            for t in range(XT):
                v_t, v_s = x[2, t, r:r + chunk, :], x[2, t, r - 1:r - 1 + chunk, :]
                x[0, t, r:r + chunk, :] = x[0, t, r:r + chunk, :] - dt_fast * ((u_t[t] - u_w[t]) + (v_t - v_s))
                tt[t, r:r + chunk, :] = u_t[t] + u_w[t]
        for r in range(hi - chunk, lo - 1, -chunk):
            e_t = [x[0, t, r:r + chunk, :] for t in range(XT)]
            e_e = ring_east(e_t, last_lane)
            v_t = [x[2, t, r:r + chunk, :] for t in range(XT)]
            s_t = [v_t[t] + x[2, t, r - 1:r - 1 + chunk, :] for t in range(XT)]
            s_e = ring_east(s_t, last_lane)
            for t in range(XT):
                at = (t, slice(r, r + chunk))
                up = (t, slice(r + 1, r + 1 + chunk))
                e_n = x[0, t, r + 1:r + 1 + chunk, :]
                u_old = x[1, t, r:r + chunk, :] if masked else cm[at] * x[1, t, r:r + chunk, :]
                v_old = v_t[t] if masked else cn[at] * v_t[t]
                x[1, t, r:r + chunk, :] = u_old + ca[at] * (s_t[t] + s_e[t]) + cc[at] - cb[at] * (e_e[t] - e_t[t])
                x[2, t, r:r + chunk, :] = v_old - cd[at] * (tt[at] + tt[up]) + ch[at] - cg[at] * (e_n - e_t[t])
        for t in range(NT):
            au[t] += weight * x[1, t, XO:XO + NR, :]
            av[t] += weight * x[2, t, XO:XO + NR, :]
        return 0

    done = 0
    for side in (4, 3, 2, 1):
        until = n_sub - 8 * (side - 1)
        rows = NR + 16 * side
        chunk = {4: 32, 3: 40, 2: 32, 1: 24}[side]
        stretch = functools.partial(subcycle, XO - 8 * side, XO - 8 * side + rows, chunk)
        if done == 0:
            stretch(False, 0, 0)
            done = 1
        lax.fori_loop(done, until, functools.partial(stretch, True), 0)
        done = until

    for t in range(NT):
        eta_o[t] = x[0, t, XO:XO + NR, :]
        tu_o[t] = x[1, t, XO:XO + NR, :]
        tv_o[t] = x[2, t, XO:XO + NR, :]
        gu_o[t] = au[t] / hu[t] - su[t]
        gv_o[t] = av[t] / hv[t] - sv[t]

    for group in (row_group, late_group, slot_group, lane_group, force_group):
        drain(group)


def final_kernel(tab_s, xu, xv, xt, xs, gu, gv, cu, cv, cc, eta, tu, tv, eta_h, tu_h, tv_h, u_h, v_h, t_h, s_h, flat_b, u_b, v_b, t_b, s_b, sem):
    flats = []
    for i, (a, o) in enumerate(((eta, eta_h), (tu, tu_h), (tv, tv_h))):
        for t in range(NT):
            flat_b[i, :, L * t:L * t + L] = a[t]
        flats.append(pltpu.make_async_copy(flat_b.at[i], o, sem.at[4, i]))

    def store(b, o, i, r):
        rows = pl.ds(pl.multiple_of(r * 8, 8), 8)
        return pltpu.make_async_copy(b.at[:, rows, :], o.at[:, rows, :], sem.at[i, r])

    def row_tile(r, _):
        rows = pl.ds(pl.multiple_of(r * 8, 8), 8)
        c_u, c_v, c_c, g_u, g_v = [[a[t, rows] for t in range(NT)] for a in (cu, cv, cc, gu, gv)]
        for i, (sweep, count, extra, b, o) in enumerate(((xu, c_u, g_u, u_b, u_h), (xv, c_v, g_v, v_b, v_h))):
            for k in range(LEV):
                for t in range(NT):
                    b[k, rows, L * t:L * t + L] = jnp.where(count[t] > float(k), sweep[t, k, rows] + extra[t], 0.0)
            store(b, o, i, r).start()
        for i, (sweep, b, o) in enumerate(((xt, t_b, t_h), (xs, s_b, s_h))):
            below = [jnp.zeros((8, L), f32)] * NT
            for k in range(LEV - 1, -1, -1):
                link, last = tab_s[6 * SLOT + k], tab_s[7 * SLOT + k]
                for t in range(NT):
                    value = sweep[t, k, rows]
                    below[t] = jnp.where(c_c[t] > float(k + 1), value + link * below[t], jnp.where(c_c[t] > float(k), last * value, value))
                    b[k, rows, L * t:L * t + L] = below[t]
            store(b, o, 2 + i, r).start()
        return 0

    lax.fori_loop(0, NR // 8, row_tile, 0)
    for cp in flats:
        cp.start()
    for cp in flats:
        cp.wait()
    for i, (b, o) in enumerate(((u_b, u_h), (v_b, v_h), (t_b, t_h), (s_b, s_h))):
        for r in range(NR // 8):
            store(b, o, i, r).wait()


def solution(mesh):
    n_col = mesh.shape['col']
    n_row = mesh.shape['row']

    def step(vel_u, vel_v, value_a11, salinity, surf_eta, trans_u, trans_v, bottom_depth, level_count, avg_weights):
        n_sub = avg_weights.shape[0]
        table = jnp.asarray(solve_table(LEV))
        hbm = pl.BlockSpec(memory_space=pltpu.HBM)
        vmem = pl.BlockSpec(memory_space=pltpu.VMEM)
        smem = pl.BlockSpec(memory_space=pltpu.SMEM)
        V = pltpu.VMEM
        tile = V((NT, NR, L), f32)
        sweep = V((NT, SLOT, NR, L), f32)
        wide = (NT + 1, XR, L)
        scratch = ([V((NT, SLOT, PR, L), f32)] * 5 + [V((NT, NR, L), jnp.int32), V((NR, L), f32)]
                   + [V((2, NT, NR + 8, L), f32)] * 2 + [V((2, NR, L), f32)] + [V((2, PR, L), f32)] * 3
                   + [V((4,) + wide, f32), V((2,) + wide, f32)] + [V((NR, L), f32)] * 2 + [V((3, NR, L), f32)] * 2
                   + [V((NR, L), f32)] * 2 + [V((3, NR, L), f32)] * 2
                   + [V((NR, L), f32)] * 2 + [V((NT, NR, L), f32)] * 4
                   + [V(wide, f32)] * 9 + [V((NT, NR, L), f32)] * 2
                   + [pltpu.SMEM((n_sub,), f32), pltpu.SMEM((8 * SLOT,), f32)]
                   + [pltpu.SemaphoreType.DMA((40,)), pltpu.SemaphoreType.DMA((64,)), pltpu.SemaphoreType.DMA((64,))])
        outs = pl.pallas_call(
            functools.partial(ocean_kernel, tuple(mesh.axis_names), n_col, n_row, n_sub),
            out_shape=[tile] * 8 + [sweep] * 4,
            in_specs=[hbm] * 11,
            out_specs=[vmem] * 12,
            scratch_shapes=scratch,
            compiler_params=pltpu.CompilerParams(collective_id=0, has_side_effects=True, vmem_limit_bytes=32 * 1024 * 1024),
        )(*[pltpu.with_memory_space_constraint(a, pltpu.HBM) for a in (vel_u, vel_v, value_a11, salinity, surf_eta, trans_u, trans_v, bottom_depth, level_count, avg_weights, table)])
        eta, tu, tv, gu, gv, cu, cv, cc, xu, xv, xt, xs = [pltpu.with_memory_space_constraint(o, pltpu.VMEM) for o in outs]

        cube = jax.ShapeDtypeStruct((LEV, NR, NC), f32)
        flat = jax.ShapeDtypeStruct((NR, NC), f32)
        return tuple(pl.pallas_call(
            final_kernel,
            out_shape=[flat] * 3 + [cube] * 4,
            in_specs=[smem] + [vmem] * 12,
            out_specs=[hbm] * 7,
            scratch_shapes=[V((3, NR, NC), f32)] + [V((LEV, NR, NC), f32)] * 4 + [pltpu.SemaphoreType.DMA((5, NT))],
            compiler_params=pltpu.CompilerParams(vmem_limit_bytes=24 * 1024 * 1024),
        )(table, xu, xv, xt, xs, gu, gv, cu, cv, cc, eta, tu, tv))

    cube = P(None, 'row', 'col')
    flat = P('row', 'col')
    return jax.shard_map(step, mesh=mesh, in_specs=(cube, cube, cube, cube, flat, flat, flat, flat, flat, P()), out_specs=(flat, flat, flat, cube, cube, cube, cube), check_vma=False)
```

```python
import functools

import jax
import jax.numpy as jnp
import numpy as np
from jax import lax
from jax.experimental import pallas as pl
from jax.experimental.pallas import tpu as pltpu
from jax.sharding import PartitionSpec as P

TIME_STEP = 1.0
GRAVITY = 16.0
BC_GRAVITY = 4.0
EXPAND_T = 0.2
CONTRACT_S = 0.6
CORIO_F0 = 0.4
CORIO_BETA = 0.4
VISC_R = 2.0
DIFF_R = 0.5

LEV = 31
SLOT = 32
NR = 32
NC = 512
NT = 4
L = 128
R0 = 8
PR = 48
XR = 112
XO = 40
MESH = pl.DeviceIdType.MESH
f32 = jnp.float32
UNROLL_M = 4
UNROLL_T = 1


def solve_table(n_levels):
    rows = []
    for s in (VISC_R, DIFF_R):
        scale, carry, link, last = np.zeros((4, SLOT))
        ratio = 0.0
        for k in range(n_levels):
            low = s if k else 0.0
            full = 1.0 + low + s - low * ratio
            end = 1.0 + low - low * ratio
            scale[k], carry[k], link[k], last[k] = 1.0 / full, low / full, s / full, full / end
            ratio = s / full
        rows += [scale, carry, link, last]
    return np.concatenate(rows).astype(np.float32)


def ocean_kernel(axes, n_col, n_row, n_sub, *refs):
    (u_h, v_h, t_h, s_h, eta_h, tu_h, tv_h, dep_h, cnt_h, w_h, tab_h,
     eta_o, tu_o, tv_o, gu_o, gv_o, cu, cv, cc_o, xu, xv, xt, xs,
     bu, bv, bt, bs, bp, cnt_i, rp, s1, s2,
     pw, pe, rw, re, ha, x, xf, qw, qe, we, ww, fw, fe, fre, frw,
     fu4, fv4, hu, hv, su, sv,
     ca, cb, cc, cd, cg, ch, cm, cn, tt, au, av,
     w_s, tab_s, lsem, ssem, rsem) = refs
    col = lax.axis_index('col')
    row = lax.axis_index('row')
    east = lax.rem(col + 1, n_col)
    west = lax.rem(col + n_col - 1, n_col)
    has_s = row > 0
    has_n = row < n_row - 1

    def dev(c, r):
        at = {'col': c, 'row': r}
        return tuple(at[name] for name in axes)

    bufs = (bu, bv, bt, bs)
    barrier = pltpu.get_barrier_semaphore()

    def signal(c, r):
        pl.semaphore_signal(barrier, inc=1, device_id=dev(c, r), device_id_type=MESH)

    signal(west, row)
    signal(east, row)

    @pl.when(has_s)
    def _():
        for c in (west, col, east):
            signal(c, row - 1)

    @pl.when(has_n)
    def _():
        for c in (west, col, east):
            signal(c, row + 1)

    zero = functools.partial(jnp.zeros, dtype=f32)

    loads = []
    for f, (src, dst) in enumerate(zip((u_h, v_h, t_h, s_h), bufs)):
        for t in range(NT):
            loads.append(pltpu.make_async_copy(src.at[:, :, L * t:L * t + L], dst.at[t, 0:LEV, R0:R0 + NR, :], lsem.at[len(loads)]))
    flat_loads = []
    for f, src in enumerate((eta_h, tu_h, tv_h)):
        for t in range(NT):
            flat_loads.append(pltpu.make_async_copy(src.at[:, L * t:L * t + L], x.at[f, t, XO:XO + NR, :], lsem.at[len(loads) + len(flat_loads)]))
    for t in range(NT):
        flat_loads.append(pltpu.make_async_copy(dep_h.at[:, L * t:L * t + L], bv.at[t, LEV, R0:R0 + NR, :], lsem.at[len(loads) + len(flat_loads)]))
    for t in range(NT):
        flat_loads.append(pltpu.make_async_copy(cnt_h.at[:, L * t:L * t + L], cnt_i.at[t], lsem.at[len(loads) + len(flat_loads)]))
    scalar_loads = [pltpu.make_async_copy(w_h, w_s, lsem.at[36]), pltpu.make_async_copy(tab_h, tab_s, lsem.at[37])]
    edge_loads = [loads[NT * f + t] for f in range(4) for t in (0, NT - 1)]
    mid_loads = [loads[NT * f + t] for f in range(4) for t in range(1, NT - 1)]
    for cp in flat_loads[3 * NT:] + edge_loads + flat_loads[:3 * NT] + mid_loads + scalar_loads:
        cp.start()

    n_copies = 0

    def remote(src, dst, c, r, sends, receives):
        nonlocal n_copies
        i = n_copies
        n_copies += 1
        return (pltpu.make_async_remote_copy(src, dst, ssem.at[i], rsem.at[i], device_id=dev(c, r), device_id_type=MESH), sends, receives)

    def maybe(cond, fn):
        if cond is None:
            fn()
        else:
            pl.when(cond)(fn)

    def start(group):
        for cp, sends, _ in group:
            maybe(sends, cp.start)

    def arrive(group):
        for cp, _, receives in group:
            maybe(receives, cp.wait_recv)

    def drain(group):
        for cp, sends, _ in group:
            maybe(sends, cp.wait_send)

    def rows_of(src, b):
        out = []
        for t in range(NT):
            cols = slice(L * t, L * t + L)
            out += [remote(src.at[:, NR - 1:NR, cols], b.at[t, 0:LEV, R0 - 1:R0, :], col, row + 1, has_n, has_s),
                    remote(src.at[:, 0:1, cols], b.at[t, 0:LEV, R0 + NR:R0 + NR + 1, :], col, row - 1, has_s, has_n)]
        return out

    def slot_of(b):
        return [remote(b.at[:, LEV, R0 + NR - 1:R0 + NR, :], b.at[:, LEV, R0 - 1:R0, :], col, row + 1, has_n, has_s),
                remote(b.at[:, LEV, R0:R0 + 1, :], b.at[:, LEV, R0 + NR:R0 + NR + 1, :], col, row - 1, has_s, has_n)]

    def wide_of(b, lanes_w, lanes_e, from_e, from_w):
        own = b.at[:, 0:NT, XO:XO + NR, :]
        return [remote(own, b.at[:, 0:NT, 8:XO, :], col, row + 1, has_n, has_s),
                remote(own, b.at[:, 0:NT, XO + NR:XO + 2 * NR, :], col, row - 1, has_s, has_n),
                remote(lanes_w, from_e.at[1], west, row, None, None),
                remote(lanes_e, from_w.at[1], east, row, None, None),
                remote(lanes_w, from_e.at[2], west, row - 1, has_s, has_n),
                remote(lanes_e, from_w.at[2], east, row - 1, has_s, has_n),
                remote(lanes_w, from_e.at[0], west, row + 1, has_n, has_s),
                remote(lanes_e, from_w.at[0], east, row + 1, has_n, has_s)]

    row_group = rows_of(u_h, bu) + rows_of(v_h, bv)
    late_group = rows_of(s_h, bs) + rows_of(t_h, bt)
    slot_group = slot_of(bu) + slot_of(bv)
    lane_group = [remote(pw, re.at[R0:R0 + NR, :], west, row, None, None),
                  remote(pe, rw.at[R0:R0 + NR, :], east, row, None, None),
                  remote(pe.at[0:1, :], rw.at[R0 + NR:R0 + NR + 1, :], east, row - 1, has_s, has_n),
                  remote(pw.at[NR - 1:NR, :], re.at[R0 - 1:R0, :], west, row + 1, has_n, has_s)]
    wide_group = wide_of(x, qw, qe, we, ww)
    force_group = wide_of(xf, fw, fe, fre, frw)

    edge = jnp.logical_or(row == 0, row == n_row - 1)

    @pl.when(edge)
    def _():
        pl.semaphore_wait(barrier, 5)

    @pl.when(jnp.logical_not(edge))
    def _():
        pl.semaphore_wait(barrier, 8)

    start(row_group)
    lane_p = lax.broadcasted_iota(jnp.int32, (PR, L), 1)
    lane = lane_p[:NR]

    for t in range(NT):
        bt[t, LEV, R0:R0 + NR, :] = zero((NR, L))
        bs[t, LEV, R0:R0 + NR, :] = zero((NR, L))
    for cp in flat_loads[3 * NT:]:
        cp.wait()
    for t in range(NT):
        count = cnt_i[t].astype(f32)
        bu[t, LEV, R0:R0 + NR, :] = count
        x[3, t, XO:XO + NR, :] = jnp.where(count > 0.0, bv[t, LEV, R0:R0 + NR, :], 0.0)

    start(slot_group)
    start(late_group)

    def roll(a, shift):
        return pltpu.roll(a, shift, 1) if not (isinstance(shift, int) and shift % L == 0) else a

    pair = lax.shift_right_logical(lane, 1)
    packed = [zero((NR, L))] * 2
    for f, b in enumerate(bufs):
        edge_loads[2 * f].wait()
        edge_loads[2 * f + 1].wait()
        for k in range(SLOT):
            p = SLOT * (f % 2) + k
            both = jnp.where(lane == 0, b[0, k, R0:R0 + NR, :], b[NT - 1, k, R0:R0 + NR, :])
            packed[f // 2] = jnp.where(pair == p, roll(both, (2 * p + 1) % L), packed[f // 2])
    even = lax.rem(lane_p, 2) == 0
    pw[...] = jnp.where(even[:NR], roll(packed[1], L - 1), packed[0])
    pe[...] = jnp.where(even[:NR], packed[0], roll(packed[1], 1))
    start(lane_group)

    def pack_wide(b, n_fields):
        first = last = zero((NR, L))
        for f in range(n_fields):
            mine = (lane >= 32 * f) & (lane < 32 * f + 32)
            first = jnp.where(mine, roll(b[f, 0, XO:XO + NR, :], 32 * f), first)
            last = jnp.where(mine, roll(b[f, NT - 1, XO:XO + NR, :], (32 * f + 32) % L), last)
        return first, last

    for cp in flat_loads[:3 * NT]:
        cp.wait()
    first, last = pack_wide(x, 4)
    qw[...] = first
    qe[...] = last
    start(wide_group)
    for cp in mid_loads:
        cp.wait()
    for cp in scalar_loads:
        cp.wait()

    for f in range(4):
        for t in range(NT + 1):
            x[f, t, 0:8, :] = zero((8, L))
            x[f, t, XR - 8:XR, :] = zero((8, L))
    for t in range(NT + 1):
        tt[t, XR - 8:XR, :] = zero((8, L))
    for t in range(NT):
        for a in (xu, xv, xt, xs):
            a[t, 0] = zero((NR, L))

    @pl.when(jnp.logical_not(has_s))
    def _():
        for b in bufs:
            b[:, :, R0 - 8:R0, :] = zero((NT, SLOT, 8, L))
        re[R0 - 8:R0, :] = zero((8, L))
        x[:, 0:NT, 8:XO, :] = zero((4, NT, NR, L))
        xf[:, 0:NT, 8:XO, :] = zero((2, NT, NR, L))
        for a in (we, ww, fre, frw):
            a[0] = zero((NR, L))

    @pl.when(jnp.logical_not(has_n))
    def _():
        for b in bufs:
            b[:, :, R0 + NR:PR, :] = zero((NT, SLOT, 8, L))
        rw[R0 + NR:PR, :] = zero((8, L))
        x[:, 0:NT, XO + NR:XO + 2 * NR, :] = zero((4, NT, NR, L))
        xf[:, 0:NT, XO + NR:XO + 2 * NR, :] = zero((2, NT, NR, L))
        for a in (we, ww, fre, frw):
            a[2] = zero((NR, L))


    row_pos = (row * NR + lax.broadcasted_iota(jnp.int32, (NR, L), 0)).astype(f32)
    total_rows = NR * n_row
    fu4[...] = 0.25 * (CORIO_F0 + CORIO_BETA * ((row_pos + 0.5) / total_rows - 0.5))
    fv4[...] = 0.25 * (CORIO_F0 + CORIO_BETA * ((row_pos + 1.0) / total_rows - 0.5))

    def to_east(tiles, halo, ts=range(NT)):
        last_lane = lane_p[:tiles[ts[0]].shape[0]] == L - 1
        rolled = {t: halo if t == NT else roll(tiles[t], L - 1) for t in sorted({t + d for t in ts for d in (0, 1)})}
        return {t: jnp.where(last_lane, rolled[t + 1], rolled[t]) for t in ts}

    def to_west(tiles, halo, ts=range(NT)):
        first_lane = lane_p[:tiles[ts[0]].shape[0]] == 0
        rolled = {t: halo if t < 0 else roll(tiles[t], 1) for t in sorted({t + d for t in ts for d in (-1, 0)})}
        return {t: jnp.where(first_lane, rolled[t - 1], rolled[t]) for t in ts}

    def side(f, k, lo=R0, n=NR):
        return pltpu.roll(ha[f // 2, lo:lo + n, :], lax.rem(L - 2 * (SLOT * (f % 2) + k), L), 1)

    def level(b, k, lo=R0, n=NR):
        return [b[t, k, lo:lo + n, :] for t in range(NT)]

    def each_level(fn, unroll):
        def some(i, _):
            base = i * unroll
            for j in range(unroll):
                fn(base + j, base + j - 1 if j else jnp.maximum(base - 1, 0), j % 2)
            return 0

        lax.fori_loop(0, -(-LEV // unroll), some, 0)

    p_scale = BC_GRAVITY / LEV

    def pressure(t, lo, n):
        total = zero((n, L))
        for k in range(LEV):
            density = CONTRACT_S * bs[t, k, lo:lo + n, :] - EXPAND_T * bt[t, k, lo:lo + n, :]
            total = total + density
            bp[t, k, lo:lo + n, :] = p_scale * (total - 0.5 * density)
        bp[t, LEV, lo:lo + n, :] = zero((n, L))

    def own_pressure(t, _):
        pressure(t, R0, NR)
        for k in range(LEV):
            bp[t, k, R0 + NR:PR, :] = zero((8, L))
        return 0

    lax.fori_loop(0, NT, own_pressure, 0)

    def momentum_down(ts, k, prev, slot):
        scale, carry = tab_s[k], tab_s[SLOT + k]
        u5, v5 = level(bu, k, R0, NR + 8), level(bv, k, R0 - 8, NR + 8)
        u_side = v_side = p_side = jnp.zeros((NR + 8, L), f32)
        if 0 in ts:
            u_side, v_side = side(0, k, R0, NR + 8), side(1, k, R0 - 8, NR + 8)
            p_side = pltpu.roll(rp[...], L - 1 - 2 * k, 1)
        uw, ve = to_west(u5, u_side, ts), to_east(v5, v_side, ts)
        um, vm = [a[:NR] for a in u5], [a[8:] for a in v5]
        ue, vw = to_east(um, u_side[:NR], ts), to_west(vm, v_side[8:], ts)
        pm, pn = level(bp, k), level(bp, k, R0 + 1)
        pe_ = to_east(pm, p_side, ts)
        for t in ts:
            u_sum, v_sum = u5[t] + uw[t], v5[t] + ve[t]
            s1[slot, t] = u_sum
            s2[slot, t] = v_sum
            ub4 = u_sum[:NR] + s1[slot, t, 1:NR + 1, :]
            vb4 = v_sum[8:] + s2[slot, t, 7:NR + 7, :]
            un, us = bu[t, k, R0 + 1:R0 + 1 + NR, :], bu[t, k, R0 - 1:R0 - 1 + NR, :]
            vn, vs = bv[t, k, R0 + 1:R0 + 1 + NR, :], bv[t, k, R0 - 1:R0 - 1 + NR, :]
            u_star = um[t] + vb4 * (fu4[...] - 0.125 * (un - us)) - um[t] * (0.5 * (ue[t] - uw[t][:NR])) + (pm[t] - pe_[t])
            v_star = vm[t] - ub4 * (fv4[...] + 0.125 * (ve[t][8:] - vw[t])) - vm[t] * (0.5 * (vn - vs)) + (pm[t] - pn[t])
            xu[t, k] = scale * u_star + carry * xu[t, prev]
            xv[t, k] = scale * v_star + carry * xv[t, prev]

    arrive(row_group)
    arrive(slot_group)
    each_level(functools.partial(momentum_down, tuple(range(1, NT - 1))), UNROLL_M)
    arrive(lane_group)
    ha[0] = jnp.where(even, rw[...], roll(re[...], L - 2))
    ha[1] = jnp.where(even, roll(rw[...], L - 1), roll(re[...], L - 1))
    east_ = roll(ha[1, R0:R0 + NR, :], 1)
    density = CONTRACT_S * roll(east_, L // 2) - EXPAND_T * east_
    total = density
    for step in (2, 4, 8, 16, 32):
        total = total + jnp.where(lane >= step, roll(total, step), 0.0)
    rp[...] = p_scale * (total - 0.5 * density)
    each_level(functools.partial(momentum_down, (0, NT - 1)), UNROLL_M)

    arrive(late_group)
    last_row = lax.broadcasted_iota(jnp.int32, (8, L), 0) == 7

    def north_pressure(t, _):
        pressure(t, R0 + NR, 8)
        sweep = zero((8, L))
        for k in range(LEV):
            sweep = tab_s[SLOT + k] * sweep - tab_s[k] * bp[t, k, R0 + NR - 7:R0 + NR + 1, :]
            xv[t, k, NR - 8:NR, :] += jnp.where(last_row, sweep, 0.0)
        return 0

    lax.fori_loop(0, NT, north_pressure, 0)

    c_mid, d_mid = level(bu, LEV), level(bv, LEV)
    c_east = to_east(c_mid, side(0, LEV))
    d_east = to_east(d_mid, side(1, LEV))
    c_north, c_south = level(bu, LEV, R0 + 1), level(bu, LEV, R0 - 1)
    d_north = level(bv, LEV, R0 + 1)
    for t in range(NT):
        cu[t] = jnp.minimum(c_mid[t], c_east[t])
        cv[t] = jnp.minimum(c_mid[t], c_north[t])
        hu[t] = 0.5 * (d_mid[t] + d_east[t])
        hv[t] = 0.5 * (d_mid[t] + d_north[t])
        cc_o[t] = c_mid[t]
    c_west0 = jnp.minimum(side(0, LEV), c_mid[0])

    def momentum_up(t, _):
        z = zero((NR, L))
        state = [[z, z, z], [z, z, z]]
        for k in range(LEV - 1, -1, -1):
            link, last_ = tab_s[2 * SLOT + k], tab_s[3 * SLOT + k]
            for q, (sweep, b, count) in enumerate(((xu, bu, cu), (xv, bv, cv))):
                below, sum_x, sum_0 = state[q]
                value = sweep[t, k]
                active = count[t] > float(k)
                solved = jnp.where(count[t] > float(k + 1), value + link * below, jnp.where(active, last_ * value, 0.0))
                sweep[t, k] = solved
                start_ = jnp.where(active, b[t, k, R0:R0 + NR, :], 0.0)
                b[t, k, R0:R0 + NR, :] = start_
                state[q] = [solved, sum_x + solved, sum_0 + start_]
        for q, (h, mean, count) in enumerate(((hu, su, cu), (hv, sv, cv))):
            _, total, start_ = state[q]
            n_active = jnp.maximum(count[t], 1.0)
            mean[t] = total / n_active
            xf[q, t, XO:XO + NR, :] = h[t] * (total - start_) / n_active / TIME_STEP
        c_south = jnp.minimum(bu[t, LEV, 0:8, :], pltpu.roll(bu[t, LEV, R0:R0 + 8, :], 7, 0))
        for k in range(LEV):
            bv[t, k, 0:8, :] = jnp.where(c_south > float(k), bv[t, k, 0:8, :], 0.0)
        return 0

    lax.fori_loop(0, NT, momentum_up, 0)

    first, last = pack_wide(xf, 2)
    fw[...] = first
    fe[...] = last
    start(force_group)

    def tracer_down(k, prev, slot):
        scale, carry = tab_s[4 * SLOT + k], tab_s[5 * SLOT + k]
        kf = lax.convert_element_type(k, f32)
        um, vm, vs = level(bu, k), level(bv, k), level(bv, k, R0 - 1)
        uw0 = jnp.where(c_west0 > kf, side(0, k), 0.0)
        for f, b, sweep in ((2, bt, xt), (3, bs, xs)):
            q = level(b, k)
            q_side = side(f, k)
            qe_ = to_east(q, q_side)
            f_east = [um[t] * (q[t] + qe_[t]) for t in range(NT)]
            f_west = to_west(f_east, uw0 * (q_side + q[0]))
            for t in range(NT):
                f_north = vm[t] * (q[t] + b[t, k, R0 + 1:R0 + 1 + NR, :])
                f_south = vs[t] * (b[t, k, R0 - 1:R0 - 1 + NR, :] + q[t])
                new = q[t] - 0.5 * TIME_STEP * (f_east[t] - f_west[t] + f_north - f_south)
                sweep[t, k] = jnp.where(bu[t, LEV, R0:R0 + NR, :] > kf, scale * new + carry * sweep[t, prev], new)

    each_level(tracer_down, UNROLL_T)

    arrive(wide_group)
    drain(wide_group)
    arrive(force_group)

    def unpack_wide(b, from_e, from_w, n_fields):
        for f in range(n_fields):
            for seg in range(3):
                b[f, NT, 8 + NR * seg:8 + NR * seg + NR, :] = jnp.where(lane < L // 2, roll(from_e[seg], (L - 32 * f) % L), roll(from_w[seg], (96 - 32 * f) % L))

    unpack_wide(x, we, ww, 4)
    unpack_wide(xf, fre, frw, 2)
    dt_fast = TIME_STEP / n_sub
    XT = NT + 1

    def ring_east(tiles, last_lane):
        rolled = [roll(a, L - 1) for a in tiles]
        return [jnp.where(last_lane, rolled[(t + 1) % XT], rolled[t]) for t in range(XT)]

    def ring_west(tiles, first_lane):
        rolled = [roll(a, 1) for a in tiles]
        return [jnp.where(first_lane, rolled[(t - 1) % XT], rolled[t]) for t in range(XT)]

    for seg in range(3):
        lo = 8 + NR * seg
        pos = (row * NR + NR * (seg - 1) + lax.broadcasted_iota(jnp.int32, (NR, L), 0)).astype(f32)
        f_u = CORIO_F0 + CORIO_BETA * ((pos + 0.5) / total_rows - 0.5)
        f_v = CORIO_F0 + CORIO_BETA * ((pos + 1.0) / total_rows - 0.5)
        d = [x[3, t, lo:lo + NR, :] for t in range(XT)]
        d_e = ring_east(d, lane == L - 1)
        for t in range(XT):
            d_n = x[3, t, lo + 1:lo + 1 + NR, :]
            wet = jnp.where((d[t] > 0.0) & (d_e[t] > 0.0), 1.0, 0.0)
            cm[t, lo:lo + NR, :] = wet
            ca[t, lo:lo + NR, :] = (0.25 * dt_fast) * f_u * wet
            cb[t, lo:lo + NR, :] = (dt_fast * GRAVITY * 0.5) * (d[t] + d_e[t]) * wet
            cc[t, lo:lo + NR, :] = dt_fast * xf[0, t, lo:lo + NR, :] * wet
            wet = jnp.where((d[t] > 0.0) & (d_n > 0.0), 1.0, 0.0)
            cn[t, lo:lo + NR, :] = wet
            cd[t, lo:lo + NR, :] = (0.25 * dt_fast) * f_v * wet
            cg[t, lo:lo + NR, :] = (dt_fast * GRAVITY * 0.5) * (d[t] + d_n) * wet
            ch[t, lo:lo + NR, :] = dt_fast * xf[1, t, lo:lo + NR, :] * wet

    for t in range(NT):
        au[t] = zero((NR, L))
        av[t] = zero((NR, L))

    def subcycle(lo, hi, chunk, masked, n, _):
        lane_c = lax.broadcasted_iota(jnp.int32, (chunk, L), 1)
        first_lane, last_lane = lane_c == 0, lane_c == L - 1
        weight = w_s[n]
        for r in range(lo, hi, chunk):
            u_t = [x[1, t, r:r + chunk, :] for t in range(XT)]
            u_w = ring_west(u_t, first_lane)
            for t in range(XT):
                v_t, v_s = x[2, t, r:r + chunk, :], x[2, t, r - 1:r - 1 + chunk, :]
                x[0, t, r:r + chunk, :] = x[0, t, r:r + chunk, :] - dt_fast * ((u_t[t] - u_w[t]) + (v_t - v_s))
                tt[t, r:r + chunk, :] = u_t[t] + u_w[t]
        for r in range(hi - chunk, lo - 1, -chunk):
            e_t = [x[0, t, r:r + chunk, :] for t in range(XT)]
            e_e = ring_east(e_t, last_lane)
            v_t = [x[2, t, r:r + chunk, :] for t in range(XT)]
            s_t = [v_t[t] + x[2, t, r - 1:r - 1 + chunk, :] for t in range(XT)]
            s_e = ring_east(s_t, last_lane)
            for t in range(XT):
                at = (t, slice(r, r + chunk))
                up = (t, slice(r + 1, r + 1 + chunk))
                e_n = x[0, t, r + 1:r + 1 + chunk, :]
                u_old = x[1, t, r:r + chunk, :] if masked else cm[at] * x[1, t, r:r + chunk, :]
                v_old = v_t[t] if masked else cn[at] * v_t[t]
                x[1, t, r:r + chunk, :] = u_old + ca[at] * (s_t[t] + s_e[t]) + cc[at] - cb[at] * (e_e[t] - e_t[t])
                x[2, t, r:r + chunk, :] = v_old - cd[at] * (tt[at] + tt[up]) + ch[at] - cg[at] * (e_n - e_t[t])
        for t in range(NT):
            au[t] += weight * x[1, t, XO:XO + NR, :]
            av[t] += weight * x[2, t, XO:XO + NR, :]
        return 0

    done = 0
    for side in (4, 3, 2, 1):
        until = n_sub - 8 * (side - 1)
        rows = NR + 16 * side
        chunk = {4: 32, 3: 40, 2: 32, 1: 24}[side]
        stretch = functools.partial(subcycle, XO - 8 * side, XO - 8 * side + rows, chunk)
        if done == 0:
            stretch(False, 0, 0)
            done = 1
        lax.fori_loop(done, until, functools.partial(stretch, True), 0)
        done = until

    for t in range(NT):
        eta_o[t] = x[0, t, XO:XO + NR, :]
        tu_o[t] = x[1, t, XO:XO + NR, :]
        tv_o[t] = x[2, t, XO:XO + NR, :]
        gu_o[t] = au[t] / hu[t] - su[t]
        gv_o[t] = av[t] / hv[t] - sv[t]

    for group in (row_group, late_group, slot_group, lane_group, force_group):
        drain(group)


def final_kernel(tab_s, xu, xv, xt, xs, gu, gv, cu, cv, cc, eta, tu, tv, eta_h, tu_h, tv_h, u_h, v_h, t_h, s_h, flat_b, u_b, v_b, t_b, s_b, sem):
    flats = []
    for i, (a, o) in enumerate(((eta, eta_h), (tu, tu_h), (tv, tv_h))):
        for t in range(NT):
            flat_b[i, :, L * t:L * t + L] = a[t]
        flats.append(pltpu.make_async_copy(flat_b.at[i], o, sem.at[4, i]))

    def store(b, o, i, r):
        rows = pl.ds(pl.multiple_of(r * 8, 8), 8)
        return pltpu.make_async_copy(b.at[:, rows, :], o.at[:, rows, :], sem.at[i, r])

    def row_tile(r, _):
        rows = pl.ds(pl.multiple_of(r * 8, 8), 8)
        c_u, c_v, c_c, g_u, g_v = [[a[t, rows] for t in range(NT)] for a in (cu, cv, cc, gu, gv)]
        for i, (sweep, count, extra, b, o) in enumerate(((xu, c_u, g_u, u_b, u_h), (xv, c_v, g_v, v_b, v_h))):
            for k in range(LEV):
                for t in range(NT):
                    b[k, rows, L * t:L * t + L] = jnp.where(count[t] > float(k), sweep[t, k, rows] + extra[t], 0.0)
            store(b, o, i, r).start()
        for i, (sweep, b, o) in enumerate(((xt, t_b, t_h), (xs, s_b, s_h))):
            below = [jnp.zeros((8, L), f32)] * NT
            for k in range(LEV - 1, -1, -1):
                link, last = tab_s[6 * SLOT + k], tab_s[7 * SLOT + k]
                for t in range(NT):
                    value = sweep[t, k, rows]
                    below[t] = jnp.where(c_c[t] > float(k + 1), value + link * below[t], jnp.where(c_c[t] > float(k), last * value, value))
                    b[k, rows, L * t:L * t + L] = below[t]
            store(b, o, 2 + i, r).start()
        return 0

    lax.fori_loop(0, NR // 8, row_tile, 0)
    for cp in flats:
        cp.start()
    for cp in flats:
        cp.wait()
    for i, (b, o) in enumerate(((u_b, u_h), (v_b, v_h), (t_b, t_h), (s_b, s_h))):
        for r in range(NR // 8):
            store(b, o, i, r).wait()


def solution(mesh):
    n_col = mesh.shape['col']
    n_row = mesh.shape['row']

    def step(vel_u, vel_v, value_a11, salinity, surf_eta, trans_u, trans_v, bottom_depth, level_count, avg_weights):
        n_sub = avg_weights.shape[0]
        table = jnp.asarray(solve_table(LEV))
        hbm = pl.BlockSpec(memory_space=pltpu.HBM)
        vmem = pl.BlockSpec(memory_space=pltpu.VMEM)
        smem = pl.BlockSpec(memory_space=pltpu.SMEM)
        V = pltpu.VMEM
        tile = V((NT, NR, L), f32)
        sweep = V((NT, SLOT, NR, L), f32)
        wide = (NT + 1, XR, L)
        scratch = ([V((NT, SLOT, PR, L), f32)] * 5 + [V((NT, NR, L), jnp.int32), V((NR, L), f32)]
                   + [V((2, NT, NR + 8, L), f32)] * 2 + [V((NR, L), f32)] * 2 + [V((PR, L), f32)] * 2 + [V((2, PR, L), f32)]
                   + [V((4,) + wide, f32), V((2,) + wide, f32)] + [V((NR, L), f32)] * 2 + [V((3, NR, L), f32)] * 2
                   + [V((NR, L), f32)] * 2 + [V((3, NR, L), f32)] * 2
                   + [V((NR, L), f32)] * 2 + [V((NT, NR, L), f32)] * 4
                   + [V(wide, f32)] * 9 + [V((NT, NR, L), f32)] * 2
                   + [pltpu.SMEM((n_sub,), f32), pltpu.SMEM((8 * SLOT,), f32)]
                   + [pltpu.SemaphoreType.DMA((40,)), pltpu.SemaphoreType.DMA((64,)), pltpu.SemaphoreType.DMA((64,))])
        outs = pl.pallas_call(
            functools.partial(ocean_kernel, tuple(mesh.axis_names), n_col, n_row, n_sub),
            out_shape=[tile] * 8 + [sweep] * 4,
            in_specs=[hbm] * 11,
            out_specs=[vmem] * 12,
            scratch_shapes=scratch,
            compiler_params=pltpu.CompilerParams(collective_id=0, has_side_effects=True, vmem_limit_bytes=32 * 1024 * 1024),
        )(*[pltpu.with_memory_space_constraint(a, pltpu.HBM) for a in (vel_u, vel_v, value_a11, salinity, surf_eta, trans_u, trans_v, bottom_depth, level_count, avg_weights, table)])
        eta, tu, tv, gu, gv, cu, cv, cc, xu, xv, xt, xs = [pltpu.with_memory_space_constraint(o, pltpu.VMEM) for o in outs]

        cube = jax.ShapeDtypeStruct((LEV, NR, NC), f32)
        flat = jax.ShapeDtypeStruct((NR, NC), f32)
        return tuple(pl.pallas_call(
            final_kernel,
            out_shape=[flat] * 3 + [cube] * 4,
            in_specs=[smem] + [vmem] * 12,
            out_specs=[hbm] * 7,
            scratch_shapes=[V((3, NR, NC), f32)] + [V((LEV, NR, NC), f32)] * 4 + [pltpu.SemaphoreType.DMA((5, NT))],
            compiler_params=pltpu.CompilerParams(vmem_limit_bytes=24 * 1024 * 1024),
        )(table, xu, xv, xt, xs, gu, gv, cu, cv, cc, eta, tu, tv))

    cube = P(None, 'row', 'col')
    flat = P('row', 'col')
    return jax.shard_map(step, mesh=mesh, in_specs=(cube, cube, cube, cube, flat, flat, flat, flat, flat, P()), out_specs=(flat, flat, flat, cube, cube, cube, cube), check_vma=False)
```

```python
import functools

import jax
import jax.numpy as jnp
import numpy as np
from jax import lax
from jax.experimental import pallas as pl
from jax.experimental.pallas import tpu as pltpu
from jax.sharding import PartitionSpec as P

TIME_STEP = 1.0
GRAVITY = 16.0
BC_GRAVITY = 4.0
EXPAND_T = 0.2
CONTRACT_S = 0.6
CORIO_F0 = 0.4
CORIO_BETA = 0.4
VISC_R = 2.0
DIFF_R = 0.5

LEV = 31
SLOT = 32
NR = 32
NC = 512
NT = 4
L = 128
R0 = 8
PR = 48
XR = 112
XO = 40
MESH = pl.DeviceIdType.MESH
f32 = jnp.float32
UNROLL_M = 4
UNROLL_T = 1
GROUPS = (28, 24, 20, 16, 12, 8, 4, 2, 0)


def solve_table(n_levels):
    rows = []
    for s in (VISC_R, DIFF_R):
        scale, carry, link, last = np.zeros((4, SLOT))
        ratio = 0.0
        for k in range(n_levels):
            low = s if k else 0.0
            full = 1.0 + low + s - low * ratio
            end = 1.0 + low - low * ratio
            scale[k], carry[k], link[k], last[k] = 1.0 / full, low / full, s / full, full / end
            ratio = s / full
        rows += [scale, carry, link, last]
    return np.concatenate(rows).astype(np.float32)


def ocean_kernel(axes, n_col, n_row, n_sub, *refs):
    (u_h, v_h, t_h, s_h, eta_h, tu_h, tv_h, dep_h, cnt_h, w_h, tab_h,
     eta_o, tu_o, tv_o, gu_o, gv_o, cu, cv, cc_o, xu, xv, xt, xs,
     bu, bv, bt, bs, bp, cnt_i, rp, s1, s2,
     pw, pe, rw, re, ha, x, xf, qw, qe, we, ww, fw, fe, fre, frw,
     fu4, fv4, hu, hv, su, sv,
     ca, cb, cc, cd, cg, ch, cm, cn, tt, au, av,
     w_s, tab_s, lsem, ssem, rsem) = refs
    col = lax.axis_index('col')
    row = lax.axis_index('row')
    east = lax.rem(col + 1, n_col)
    west = lax.rem(col + n_col - 1, n_col)
    has_s = row > 0
    has_n = row < n_row - 1

    def dev(c, r):
        at = {'col': c, 'row': r}
        return tuple(at[name] for name in axes)

    bufs = (bu, bv, bt, bs)
    barrier = pltpu.get_barrier_semaphore()

    def signal(c, r):
        pl.semaphore_signal(barrier, inc=1, device_id=dev(c, r), device_id_type=MESH)

    signal(west, row)
    signal(east, row)

    @pl.when(has_s)
    def _():
        for c in (west, col, east):
            signal(c, row - 1)

    @pl.when(has_n)
    def _():
        for c in (west, col, east):
            signal(c, row + 1)

    zero = functools.partial(jnp.zeros, dtype=f32)

    loads = []
    for f, (src, dst) in enumerate(zip((u_h, v_h, t_h, s_h), bufs)):
        for t in range(NT):
            loads.append(pltpu.make_async_copy(src.at[:, :, L * t:L * t + L], dst.at[t, 0:LEV, R0:R0 + NR, :], lsem.at[len(loads)]))
    flat_loads = []
    for f, src in enumerate((eta_h, tu_h, tv_h)):
        for t in range(NT):
            flat_loads.append(pltpu.make_async_copy(src.at[:, L * t:L * t + L], x.at[f, t, XO:XO + NR, :], lsem.at[len(loads) + len(flat_loads)]))
    for t in range(NT):
        flat_loads.append(pltpu.make_async_copy(dep_h.at[:, L * t:L * t + L], bv.at[t, LEV, R0:R0 + NR, :], lsem.at[len(loads) + len(flat_loads)]))
    for t in range(NT):
        flat_loads.append(pltpu.make_async_copy(cnt_h.at[:, L * t:L * t + L], cnt_i.at[t], lsem.at[len(loads) + len(flat_loads)]))
    scalar_loads = [pltpu.make_async_copy(w_h, w_s, lsem.at[36]), pltpu.make_async_copy(tab_h, tab_s, lsem.at[37])]
    edge_loads = [loads[NT * f + t] for f in range(4) for t in (0, NT - 1)]
    mid_loads = [loads[NT * f + t] for f in range(4) for t in range(1, NT - 1)]
    for cp in flat_loads[3 * NT:] + edge_loads + flat_loads[:3 * NT] + mid_loads + scalar_loads:
        cp.start()

    n_copies = 0

    def remote(src, dst, c, r, sends, receives):
        nonlocal n_copies
        i = n_copies
        n_copies += 1
        return (pltpu.make_async_remote_copy(src, dst, ssem.at[i], rsem.at[i], device_id=dev(c, r), device_id_type=MESH), sends, receives)

    def maybe(cond, fn):
        if cond is None:
            fn()
        else:
            pl.when(cond)(fn)

    def start(group):
        for cp, sends, _ in group:
            maybe(sends, cp.start)

    def arrive(group):
        for cp, _, receives in group:
            maybe(receives, cp.wait_recv)

    def drain(group):
        for cp, sends, _ in group:
            maybe(sends, cp.wait_send)

    def rows_of(src, b):
        out = []
        for t in range(NT):
            cols = slice(L * t, L * t + L)
            out += [remote(src.at[:, NR - 1:NR, cols], b.at[t, 0:LEV, R0 - 1:R0, :], col, row + 1, has_n, has_s),
                    remote(src.at[:, 0:1, cols], b.at[t, 0:LEV, R0 + NR:R0 + NR + 1, :], col, row - 1, has_s, has_n)]
        return out

    def slot_of(b):
        return [remote(b.at[:, LEV, R0 + NR - 1:R0 + NR, :], b.at[:, LEV, R0 - 1:R0, :], col, row + 1, has_n, has_s),
                remote(b.at[:, LEV, R0:R0 + 1, :], b.at[:, LEV, R0 + NR:R0 + NR + 1, :], col, row - 1, has_s, has_n)]

    def wide_of(b, lanes_w, lanes_e, from_e, from_w):
        own = b.at[:, 0:NT, XO:XO + NR, :]
        return [remote(own, b.at[:, 0:NT, 8:XO, :], col, row + 1, has_n, has_s),
                remote(own, b.at[:, 0:NT, XO + NR:XO + 2 * NR, :], col, row - 1, has_s, has_n),
                remote(lanes_w, from_e.at[1], west, row, None, None),
                remote(lanes_e, from_w.at[1], east, row, None, None),
                remote(lanes_w, from_e.at[2], west, row - 1, has_s, has_n),
                remote(lanes_e, from_w.at[2], east, row - 1, has_s, has_n),
                remote(lanes_w, from_e.at[0], west, row + 1, has_n, has_s),
                remote(lanes_e, from_w.at[0], east, row + 1, has_n, has_s)]

    row_group = rows_of(u_h, bu) + rows_of(v_h, bv)
    late_group = rows_of(s_h, bs) + rows_of(t_h, bt)
    slot_group = slot_of(bu) + slot_of(bv)
    lane_group = [remote(pw, re.at[R0:R0 + NR, :], west, row, None, None),
                  remote(pe, rw.at[R0:R0 + NR, :], east, row, None, None),
                  remote(pe.at[0:1, :], rw.at[R0 + NR:R0 + NR + 1, :], east, row - 1, has_s, has_n),
                  remote(pw.at[NR - 1:NR, :], re.at[R0 - 1:R0, :], west, row + 1, has_n, has_s)]
    wide_group = wide_of(x, qw, qe, we, ww)
    force_group = wide_of(xf, fw, fe, fre, frw)

    edge = jnp.logical_or(row == 0, row == n_row - 1)

    @pl.when(edge)
    def _():
        pl.semaphore_wait(barrier, 5)

    @pl.when(jnp.logical_not(edge))
    def _():
        pl.semaphore_wait(barrier, 8)

    start(row_group)
    lane_p = lax.broadcasted_iota(jnp.int32, (PR, L), 1)
    lane = lane_p[:NR]

    for t in range(NT):
        bt[t, LEV, R0:R0 + NR, :] = zero((NR, L))
        bs[t, LEV, R0:R0 + NR, :] = zero((NR, L))
    for cp in flat_loads[3 * NT:]:
        cp.wait()
    for t in range(NT):
        count = cnt_i[t].astype(f32)
        bu[t, LEV, R0:R0 + NR, :] = count
        x[3, t, XO:XO + NR, :] = jnp.where(count > 0.0, bv[t, LEV, R0:R0 + NR, :], 0.0)

    start(slot_group)
    start(late_group)

    def roll(a, shift):
        return pltpu.roll(a, shift, 1) if not (isinstance(shift, int) and shift % L == 0) else a

    pair = lax.shift_right_logical(lane, 1)
    packed = [zero((NR, L))] * 2
    for f, b in enumerate(bufs):
        edge_loads[2 * f].wait()
        edge_loads[2 * f + 1].wait()
        for k in range(SLOT):
            p = SLOT * (f % 2) + k
            both = jnp.where(lane == 0, b[0, k, R0:R0 + NR, :], b[NT - 1, k, R0:R0 + NR, :])
            packed[f // 2] = jnp.where(pair == p, roll(both, (2 * p + 1) % L), packed[f // 2])
    even = lax.rem(lane_p, 2) == 0
    pw[...] = jnp.where(even[:NR], roll(packed[1], L - 1), packed[0])
    pe[...] = jnp.where(even[:NR], packed[0], roll(packed[1], 1))
    start(lane_group)

    def pack_wide(b, n_fields):
        first = last = zero((NR, L))
        for f in range(n_fields):
            mine = (lane >= 32 * f) & (lane < 32 * f + 32)
            first = jnp.where(mine, roll(b[f, 0, XO:XO + NR, :], 32 * f), first)
            last = jnp.where(mine, roll(b[f, NT - 1, XO:XO + NR, :], (32 * f + 32) % L), last)
        return first, last

    for cp in flat_loads[:3 * NT]:
        cp.wait()
    first, last = pack_wide(x, 4)
    qw[...] = first
    qe[...] = last
    start(wide_group)
    for cp in mid_loads:
        cp.wait()
    for cp in scalar_loads:
        cp.wait()

    for f in range(4):
        for t in range(NT + 1):
            x[f, t, 0:8, :] = zero((8, L))
            x[f, t, XR - 8:XR, :] = zero((8, L))
    for t in range(NT + 1):
        tt[t, XR - 8:XR, :] = zero((8, L))
    for t in range(NT):
        for a in (xu, xv, xt, xs):
            a[t, 0] = zero((NR, L))

    @pl.when(jnp.logical_not(has_s))
    def _():
        for b in bufs:
            b[:, :, R0 - 8:R0, :] = zero((NT, SLOT, 8, L))
        re[R0 - 8:R0, :] = zero((8, L))
        x[:, 0:NT, 8:XO, :] = zero((4, NT, NR, L))
        xf[:, 0:NT, 8:XO, :] = zero((2, NT, NR, L))
        for a in (we, ww, fre, frw):
            a[0] = zero((NR, L))

    @pl.when(jnp.logical_not(has_n))
    def _():
        for b in bufs:
            b[:, :, R0 + NR:PR, :] = zero((NT, SLOT, 8, L))
        rw[R0 + NR:PR, :] = zero((8, L))
        x[:, 0:NT, XO + NR:XO + 2 * NR, :] = zero((4, NT, NR, L))
        xf[:, 0:NT, XO + NR:XO + 2 * NR, :] = zero((2, NT, NR, L))
        for a in (we, ww, fre, frw):
            a[2] = zero((NR, L))


    row_pos = (row * NR + lax.broadcasted_iota(jnp.int32, (NR, L), 0)).astype(f32)
    total_rows = NR * n_row
    fu4[...] = 0.25 * (CORIO_F0 + CORIO_BETA * ((row_pos + 0.5) / total_rows - 0.5))
    fv4[...] = 0.25 * (CORIO_F0 + CORIO_BETA * ((row_pos + 1.0) / total_rows - 0.5))

    def to_east(tiles, halo, ts=range(NT)):
        last_lane = lane_p[:tiles[ts[0]].shape[0]] == L - 1
        rolled = {t: halo if t == NT else roll(tiles[t], L - 1) for t in sorted({t + d for t in ts for d in (0, 1)})}
        return {t: jnp.where(last_lane, rolled[t + 1], rolled[t]) for t in ts}

    def to_west(tiles, halo, ts=range(NT)):
        first_lane = lane_p[:tiles[ts[0]].shape[0]] == 0
        rolled = {t: halo if t < 0 else roll(tiles[t], 1) for t in sorted({t + d for t in ts for d in (-1, 0)})}
        return {t: jnp.where(first_lane, rolled[t - 1], rolled[t]) for t in ts}

    def side(f, k, lo=R0, n=NR):
        return pltpu.roll(ha[f // 2, lo:lo + n, :], lax.rem(L - 2 * (SLOT * (f % 2) + k), L), 1)

    def level(b, k, lo=R0, n=NR):
        return [b[t, k, lo:lo + n, :] for t in range(NT)]

    def each_level(fn, unroll):
        def some(i, _):
            base = i * unroll
            for j in range(unroll):
                fn(base + j, base + j - 1 if j else jnp.maximum(base - 1, 0), j % 2)
            return 0

        lax.fori_loop(0, -(-LEV // unroll), some, 0)

    p_scale = BC_GRAVITY / LEV

    def pressure(t, lo, n):
        total = zero((n, L))
        for k in range(LEV):
            density = CONTRACT_S * bs[t, k, lo:lo + n, :] - EXPAND_T * bt[t, k, lo:lo + n, :]
            total = total + density
            bp[t, k, lo:lo + n, :] = p_scale * (total - 0.5 * density)
        bp[t, LEV, lo:lo + n, :] = zero((n, L))

    def own_pressure(t, _):
        pressure(t, R0, NR)
        for k in range(LEV):
            bp[t, k, R0 + NR:PR, :] = zero((8, L))
        return 0

    lax.fori_loop(0, NT, own_pressure, 0)

    def momentum_down(ts, k, prev, slot):
        scale, carry = tab_s[k], tab_s[SLOT + k]
        u5, v5 = level(bu, k, R0, NR + 8), level(bv, k, R0 - 8, NR + 8)
        u_side = v_side = p_side = jnp.zeros((NR + 8, L), f32)
        if 0 in ts:
            u_side, v_side = side(0, k, R0, NR + 8), side(1, k, R0 - 8, NR + 8)
            p_side = pltpu.roll(rp[...], L - 1 - 2 * k, 1)
        uw, ve = to_west(u5, u_side, ts), to_east(v5, v_side, ts)
        um, vm = [a[:NR] for a in u5], [a[8:] for a in v5]
        ue, vw = to_east(um, u_side[:NR], ts), to_west(vm, v_side[8:], ts)
        pm, pn = level(bp, k), level(bp, k, R0 + 1)
        pe_ = to_east(pm, p_side, ts)
        for t in ts:
            u_sum, v_sum = u5[t] + uw[t], v5[t] + ve[t]
            s1[slot, t] = u_sum
            s2[slot, t] = v_sum
            ub4 = u_sum[:NR] + s1[slot, t, 1:NR + 1, :]
            vb4 = v_sum[8:] + s2[slot, t, 7:NR + 7, :]
            un, us = bu[t, k, R0 + 1:R0 + 1 + NR, :], bu[t, k, R0 - 1:R0 - 1 + NR, :]
            vn, vs = bv[t, k, R0 + 1:R0 + 1 + NR, :], bv[t, k, R0 - 1:R0 - 1 + NR, :]
            u_star = um[t] + vb4 * (fu4[...] - 0.125 * (un - us)) - um[t] * (0.5 * (ue[t] - uw[t][:NR])) + (pm[t] - pe_[t])
            v_star = vm[t] - ub4 * (fv4[...] + 0.125 * (ve[t][8:] - vw[t])) - vm[t] * (0.5 * (vn - vs)) + (pm[t] - pn[t])
            xu[t, k] = scale * u_star + carry * xu[t, prev]
            xv[t, k] = scale * v_star + carry * xv[t, prev]

    arrive(row_group)
    arrive(slot_group)
    each_level(functools.partial(momentum_down, tuple(range(1, NT - 1))), UNROLL_M)
    arrive(lane_group)
    ha[0] = jnp.where(even, rw[...], roll(re[...], L - 2))
    ha[1] = jnp.where(even, roll(rw[...], L - 1), roll(re[...], L - 1))
    east_ = roll(ha[1, R0:R0 + NR, :], 1)
    density = CONTRACT_S * roll(east_, L // 2) - EXPAND_T * east_
    total = density
    for step in (2, 4, 8, 16, 32):
        total = total + jnp.where(lane >= step, roll(total, step), 0.0)
    rp[...] = p_scale * (total - 0.5 * density)
    each_level(functools.partial(momentum_down, (0, NT - 1)), UNROLL_M)

    arrive(late_group)
    last_row = lax.broadcasted_iota(jnp.int32, (8, L), 0) == 7

    def north_pressure(t, _):
        pressure(t, R0 + NR, 8)
        sweep = zero((8, L))
        for k in range(LEV):
            sweep = tab_s[SLOT + k] * sweep - tab_s[k] * bp[t, k, R0 + NR - 7:R0 + NR + 1, :]
            xv[t, k, NR - 8:NR, :] += jnp.where(last_row, sweep, 0.0)
        return 0

    lax.fori_loop(0, NT, north_pressure, 0)

    c_mid, d_mid = level(bu, LEV), level(bv, LEV)
    c_east = to_east(c_mid, side(0, LEV))
    d_east = to_east(d_mid, side(1, LEV))
    c_north, c_south = level(bu, LEV, R0 + 1), level(bu, LEV, R0 - 1)
    d_north = level(bv, LEV, R0 + 1)
    for t in range(NT):
        cu[t] = jnp.minimum(c_mid[t], c_east[t])
        cv[t] = jnp.minimum(c_mid[t], c_north[t])
        hu[t] = 0.5 * (d_mid[t] + d_east[t])
        hv[t] = 0.5 * (d_mid[t] + d_north[t])
        cc_o[t] = c_mid[t]
    c_west0 = jnp.minimum(side(0, LEV), c_mid[0])

    def momentum_up(t, _):
        z = zero((NR, L))
        state = [[z, z, z], [z, z, z]]
        for k in range(LEV - 1, -1, -1):
            link, last_ = tab_s[2 * SLOT + k], tab_s[3 * SLOT + k]
            for q, (sweep, b, count) in enumerate(((xu, bu, cu), (xv, bv, cv))):
                below, sum_x, sum_0 = state[q]
                value = sweep[t, k]
                active = count[t] > float(k)
                solved = jnp.where(count[t] > float(k + 1), value + link * below, jnp.where(active, last_ * value, 0.0))
                sweep[t, k] = solved
                start_ = jnp.where(active, b[t, k, R0:R0 + NR, :], 0.0)
                b[t, k, R0:R0 + NR, :] = start_
                state[q] = [solved, sum_x + solved, sum_0 + start_]
        for q, (h, mean, count) in enumerate(((hu, su, cu), (hv, sv, cv))):
            _, total, start_ = state[q]
            n_active = jnp.maximum(count[t], 1.0)
            mean[t] = total / n_active
            xf[q, t, XO:XO + NR, :] = h[t] * (total - start_) / n_active / TIME_STEP
        c_south = jnp.minimum(bu[t, LEV, 0:8, :], pltpu.roll(bu[t, LEV, R0:R0 + 8, :], 7, 0))
        for k in range(LEV):
            bv[t, k, 0:8, :] = jnp.where(c_south > float(k), bv[t, k, 0:8, :], 0.0)
        return 0

    lax.fori_loop(0, NT, momentum_up, 0)

    first, last = pack_wide(xf, 2)
    fw[...] = first
    fe[...] = last
    start(force_group)

    def tracer_down(k, prev, slot):
        scale, carry = tab_s[4 * SLOT + k], tab_s[5 * SLOT + k]
        kf = lax.convert_element_type(k, f32)
        um, vm, vs = level(bu, k), level(bv, k), level(bv, k, R0 - 1)
        uw0 = jnp.where(c_west0 > kf, side(0, k), 0.0)
        for f, b, sweep in ((2, bt, xt), (3, bs, xs)):
            q = level(b, k)
            q_side = side(f, k)
            qe_ = to_east(q, q_side)
            f_east = [um[t] * (q[t] + qe_[t]) for t in range(NT)]
            f_west = to_west(f_east, uw0 * (q_side + q[0]))
            for t in range(NT):
                f_north = vm[t] * (q[t] + b[t, k, R0 + 1:R0 + 1 + NR, :])
                f_south = vs[t] * (b[t, k, R0 - 1:R0 - 1 + NR, :] + q[t])
                new = q[t] - 0.5 * TIME_STEP * (f_east[t] - f_west[t] + f_north - f_south)
                sweep[t, k] = jnp.where(bu[t, LEV, R0:R0 + NR, :] > kf, scale * new + carry * sweep[t, prev], new)

    each_level(tracer_down, UNROLL_T)

    arrive(wide_group)
    drain(wide_group)
    arrive(force_group)

    def unpack_wide(b, from_e, from_w, n_fields):
        for f in range(n_fields):
            for seg in range(3):
                b[f, NT, 8 + NR * seg:8 + NR * seg + NR, :] = jnp.where(lane < L // 2, roll(from_e[seg], (L - 32 * f) % L), roll(from_w[seg], (96 - 32 * f) % L))

    unpack_wide(x, we, ww, 4)
    unpack_wide(xf, fre, frw, 2)
    dt_fast = TIME_STEP / n_sub
    XT = NT + 1

    def ring_east(tiles, last_lane):
        rolled = [roll(a, L - 1) for a in tiles]
        return [jnp.where(last_lane, rolled[(t + 1) % XT], rolled[t]) for t in range(XT)]

    def ring_west(tiles, first_lane):
        rolled = [roll(a, 1) for a in tiles]
        return [jnp.where(first_lane, rolled[(t - 1) % XT], rolled[t]) for t in range(XT)]

    for seg in range(3):
        lo = 8 + NR * seg
        pos = (row * NR + NR * (seg - 1) + lax.broadcasted_iota(jnp.int32, (NR, L), 0)).astype(f32)
        f_u = CORIO_F0 + CORIO_BETA * ((pos + 0.5) / total_rows - 0.5)
        f_v = CORIO_F0 + CORIO_BETA * ((pos + 1.0) / total_rows - 0.5)
        d = [x[3, t, lo:lo + NR, :] for t in range(XT)]
        d_e = ring_east(d, lane == L - 1)
        for t in range(XT):
            d_n = x[3, t, lo + 1:lo + 1 + NR, :]
            wet = jnp.where((d[t] > 0.0) & (d_e[t] > 0.0), 1.0, 0.0)
            cm[t, lo:lo + NR, :] = wet
            ca[t, lo:lo + NR, :] = (0.25 * dt_fast) * f_u * wet
            cb[t, lo:lo + NR, :] = (dt_fast * GRAVITY * 0.5) * (d[t] + d_e[t]) * wet
            cc[t, lo:lo + NR, :] = dt_fast * xf[0, t, lo:lo + NR, :] * wet
            wet = jnp.where((d[t] > 0.0) & (d_n > 0.0), 1.0, 0.0)
            cn[t, lo:lo + NR, :] = wet
            cd[t, lo:lo + NR, :] = (0.25 * dt_fast) * f_v * wet
            cg[t, lo:lo + NR, :] = (dt_fast * GRAVITY * 0.5) * (d[t] + d_n) * wet
            ch[t, lo:lo + NR, :] = dt_fast * xf[1, t, lo:lo + NR, :] * wet

    for t in range(NT):
        au[t] = zero((NR, L))
        av[t] = zero((NR, L))

    def subcycle(side_rows, masked, n, _):
        weight = w_s[n]
        parts = ((XO - side_rows, side_rows), (XO, NR), (XO + NR, side_rows))
        for r, chunk in parts:
            first_lane = lane[:chunk] == 0
            u_t = [x[1, t, r:r + chunk, :] for t in range(XT)]
            u_w = ring_west(u_t, first_lane)
            for t in range(XT):
                v_t, v_s = x[2, t, r:r + chunk, :], x[2, t, r - 1:r - 1 + chunk, :]
                x[0, t, r:r + chunk, :] = x[0, t, r:r + chunk, :] - dt_fast * ((u_t[t] - u_w[t]) + (v_t - v_s))
                tt[t, r:r + chunk, :] = u_t[t] + u_w[t]
        for r, chunk in parts[::-1]:
            last_lane = lane[:chunk] == L - 1
            e_t = [x[0, t, r:r + chunk, :] for t in range(XT)]
            e_e = ring_east(e_t, last_lane)
            v_t = [x[2, t, r:r + chunk, :] for t in range(XT)]
            s_t = [v_t[t] + x[2, t, r - 1:r - 1 + chunk, :] for t in range(XT)]
            s_e = ring_east(s_t, last_lane)
            for t in range(XT):
                at = (t, slice(r, r + chunk))
                up = (t, slice(r + 1, r + 1 + chunk))
                e_n = x[0, t, r + 1:r + 1 + chunk, :]
                u_old = x[1, t, r:r + chunk, :] if masked else cm[at] * x[1, t, r:r + chunk, :]
                v_old = v_t[t] if masked else cn[at] * v_t[t]
                u_new = u_old + ca[at] * (s_t[t] + s_e[t]) + cc[at] - cb[at] * (e_e[t] - e_t[t])
                v_new = v_old - cd[at] * (tt[at] + tt[up]) + ch[at] - cg[at] * (e_n - e_t[t])
                x[1, t, r:r + chunk, :] = u_new
                x[2, t, r:r + chunk, :] = v_new
                if r == XO and t < NT:
                    au[t] += weight * u_new
                    av[t] += weight * v_new
        return 0

    done = 0
    for tiles in (4, 3, 2, 1):
        until = n_sub - 8 * (tiles - 1)
        stretch = functools.partial(subcycle, 8 * tiles)
        if done == 0:
            stretch(False, 0, 0)
            done = 1
        lax.fori_loop(done, until, functools.partial(stretch, True), 0)
        done = until

    for t in range(NT):
        eta_o[t] = x[0, t, XO:XO + NR, :]
        tu_o[t] = x[1, t, XO:XO + NR, :]
        tv_o[t] = x[2, t, XO:XO + NR, :]
        gu_o[t] = au[t] / hu[t] - su[t]
        gv_o[t] = av[t] / hv[t] - sv[t]

    for group in (row_group, late_group, slot_group, lane_group, force_group):
        drain(group)


def final_kernel(tab_s, xu, xv, xt, xs, gu, gv, cu, cv, cc, eta, tu, tv, eta_h, tu_h, tv_h, u_h, v_h, t_h, s_h, flat_b, u_b, v_b, t_b, s_b, sem):
    stores = []
    for i, (a, o) in enumerate(((eta, eta_h), (tu, tu_h), (tv, tv_h))):
        for t in range(NT):
            flat_b[i, :, L * t:L * t + L] = a[t]
        stores.append(pltpu.make_async_copy(flat_b.at[i], o, sem.at[4, i]))
        stores[-1].start()

    below = [[jnp.zeros((NR, L), f32)] * NT for _ in range(2)]
    top = LEV
    for k in range(LEV - 1, -1, -1):
        link, last = tab_s[6 * SLOT + k], tab_s[7 * SLOT + k]
        for t in range(NT):
            cols = slice(L * t, L * t + L)
            u_b[k, :, cols] = jnp.where(cu[t] > float(k), xu[t, k] + gu[t], 0.0)
            v_b[k, :, cols] = jnp.where(cv[t] > float(k), xv[t, k] + gv[t], 0.0)
            for q, (sweep, b) in enumerate(((xt, t_b), (xs, s_b))):
                value = sweep[t, k]
                solved = jnp.where(cc[t] > float(k + 1), value + link * below[q][t], jnp.where(cc[t] > float(k), last * value, value))
                below[q][t] = solved
                b[k, :, cols] = solved
        if k in GROUPS:
            for i, (b, o) in enumerate(((u_b, u_h), (v_b, v_h), (t_b, t_h), (s_b, s_h))):
                stores.append(pltpu.make_async_copy(b.at[k:top], o.at[k:top], sem.at[i, GROUPS.index(k)]))
                stores[-1].start()
            top = k
    for cp in stores:
        cp.wait()


def solution(mesh):
    n_col = mesh.shape['col']
    n_row = mesh.shape['row']

    def step(vel_u, vel_v, value_a11, salinity, surf_eta, trans_u, trans_v, bottom_depth, level_count, avg_weights):
        n_sub = avg_weights.shape[0]
        table = jnp.asarray(solve_table(LEV))
        hbm = pl.BlockSpec(memory_space=pltpu.HBM)
        vmem = pl.BlockSpec(memory_space=pltpu.VMEM)
        smem = pl.BlockSpec(memory_space=pltpu.SMEM)
        V = pltpu.VMEM
        tile = V((NT, NR, L), f32)
        sweep = V((NT, SLOT, NR, L), f32)
        wide = (NT + 1, XR, L)
        scratch = ([V((NT, SLOT, PR, L), f32)] * 5 + [V((NT, NR, L), jnp.int32), V((NR, L), f32)]
                   + [V((2, NT, NR + 8, L), f32)] * 2 + [V((NR, L), f32)] * 2 + [V((PR, L), f32)] * 2 + [V((2, PR, L), f32)]
                   + [V((4,) + wide, f32), V((2,) + wide, f32)] + [V((NR, L), f32)] * 2 + [V((3, NR, L), f32)] * 2
                   + [V((NR, L), f32)] * 2 + [V((3, NR, L), f32)] * 2
                   + [V((NR, L), f32)] * 2 + [V((NT, NR, L), f32)] * 4
                   + [V(wide, f32)] * 9 + [V((NT, NR, L), f32)] * 2
                   + [pltpu.SMEM((n_sub,), f32), pltpu.SMEM((8 * SLOT,), f32)]
                   + [pltpu.SemaphoreType.DMA((40,)), pltpu.SemaphoreType.DMA((64,)), pltpu.SemaphoreType.DMA((64,))])
        outs = pl.pallas_call(
            functools.partial(ocean_kernel, tuple(mesh.axis_names), n_col, n_row, n_sub),
            out_shape=[tile] * 8 + [sweep] * 4,
            in_specs=[hbm] * 11,
            out_specs=[vmem] * 12,
            scratch_shapes=scratch,
            compiler_params=pltpu.CompilerParams(collective_id=0, has_side_effects=True, vmem_limit_bytes=32 * 1024 * 1024),
        )(*[pltpu.with_memory_space_constraint(a, pltpu.HBM) for a in (vel_u, vel_v, value_a11, salinity, surf_eta, trans_u, trans_v, bottom_depth, level_count, avg_weights, table)])
        eta, tu, tv, gu, gv, cu, cv, cc, xu, xv, xt, xs = [pltpu.with_memory_space_constraint(o, pltpu.VMEM) for o in outs]

        cube = jax.ShapeDtypeStruct((LEV, NR, NC), f32)
        flat = jax.ShapeDtypeStruct((NR, NC), f32)
        return tuple(pl.pallas_call(
            final_kernel,
            out_shape=[flat] * 3 + [cube] * 4,
            in_specs=[smem] + [vmem] * 12,
            out_specs=[hbm] * 7,
            scratch_shapes=[V((3, NR, NC), f32)] + [V((LEV, NR, NC), f32)] * 4 + [pltpu.SemaphoreType.DMA((5, len(GROUPS)))],
            compiler_params=pltpu.CompilerParams(vmem_limit_bytes=24 * 1024 * 1024),
        )(table, xu, xv, xt, xs, gu, gv, cu, cv, cc, eta, tu, tv))

    cube = P(None, 'row', 'col')
    flat = P('row', 'col')
    return jax.shard_map(step, mesh=mesh, in_specs=(cube, cube, cube, cube, flat, flat, flat, flat, flat, P()), out_specs=(flat, flat, flat, cube, cube, cube, cube), check_vma=False)
```

```python
import functools

import jax
import jax.numpy as jnp
import numpy as np
from jax import lax
from jax.experimental import pallas as pl
from jax.experimental.pallas import tpu as pltpu
from jax.sharding import PartitionSpec as P

TIME_STEP = 1.0
GRAVITY = 16.0
BC_GRAVITY = 4.0
EXPAND_T = 0.2
CONTRACT_S = 0.6
CORIO_F0 = 0.4
CORIO_BETA = 0.4
VISC_R = 2.0
DIFF_R = 0.5

LEV = 31
SLOT = 32
NR = 32
NC = 512
NT = 4
L = 128
R0 = 8
PR = 48
XR = 112
XO = 40
MESH = pl.DeviceIdType.MESH
f32 = jnp.float32
UNROLL_M = 4
UNROLL_T = 1
GROUPS = (28, 24, 20, 16, 12, 8, 4, 2, 0)


def solve_table(n_levels):
    rows = []
    for s in (VISC_R, DIFF_R):
        scale, carry, link, last = np.zeros((4, SLOT))
        ratio = 0.0
        for k in range(n_levels):
            low = s if k else 0.0
            full = 1.0 + low + s - low * ratio
            end = 1.0 + low - low * ratio
            scale[k], carry[k], link[k], last[k] = 1.0 / full, low / full, s / full, full / end
            ratio = s / full
        rows += [scale, carry, link, last]
    return np.concatenate(rows).astype(np.float32)


def ocean_kernel(axes, n_col, n_row, n_sub, *refs):
    (u_h, v_h, t_h, s_h, eta_h, tu_h, tv_h, dep_h, cnt_h, w_h, tab_h,
     eta_o, tu_o, tv_o, gu_o, gv_o, cu, cv, cc_o, xu, xv, xt, xs,
     bu, bv, bt, bs, bp, cnt_i, rp, s1, s2,
     pn, ps, rn, rs, pw, pe, rw, re, ha, x, xf, qw, qe, we, ww, fw, fe, fre, frw,
     fu4, fv4, hu, hv, su, sv,
     ca, cb, cc, cd, cg, ch, cm, cn, tt, au, av,
     w_s, tab_s, lsem, ssem, rsem) = refs
    col = lax.axis_index('col')
    row = lax.axis_index('row')
    east = lax.rem(col + 1, n_col)
    west = lax.rem(col + n_col - 1, n_col)
    has_s = row > 0
    has_n = row < n_row - 1

    def dev(c, r):
        at = {'col': c, 'row': r}
        return tuple(at[name] for name in axes)

    bufs = (bu, bv, bt, bs)
    barrier = pltpu.get_barrier_semaphore()

    def signal(c, r):
        pl.semaphore_signal(barrier, inc=1, device_id=dev(c, r), device_id_type=MESH)

    signal(west, row)
    signal(east, row)

    @pl.when(has_s)
    def _():
        for c in (west, col, east):
            signal(c, row - 1)

    @pl.when(has_n)
    def _():
        for c in (west, col, east):
            signal(c, row + 1)

    zero = functools.partial(jnp.zeros, dtype=f32)

    loads = []
    for f, (src, dst) in enumerate(zip((u_h, v_h, t_h, s_h), bufs)):
        for t in range(NT):
            loads.append(pltpu.make_async_copy(src.at[:, :, L * t:L * t + L], dst.at[t, 0:LEV, R0:R0 + NR, :], lsem.at[len(loads)]))
    flat_loads = []
    for f, src in enumerate((eta_h, tu_h, tv_h)):
        for t in range(NT):
            flat_loads.append(pltpu.make_async_copy(src.at[:, L * t:L * t + L], x.at[f, t, XO:XO + NR, :], lsem.at[len(loads) + len(flat_loads)]))
    for t in range(NT):
        flat_loads.append(pltpu.make_async_copy(dep_h.at[:, L * t:L * t + L], bv.at[t, LEV, R0:R0 + NR, :], lsem.at[len(loads) + len(flat_loads)]))
    for t in range(NT):
        flat_loads.append(pltpu.make_async_copy(cnt_h.at[:, L * t:L * t + L], cnt_i.at[t], lsem.at[len(loads) + len(flat_loads)]))
    scalar_loads = [pltpu.make_async_copy(w_h, w_s, lsem.at[36]), pltpu.make_async_copy(tab_h, tab_s, lsem.at[37])]
    edge_loads = [loads[NT * f + t] for f in range(4) for t in (0, NT - 1)]
    mid_loads = [loads[NT * f + t] for f in range(4) for t in range(1, NT - 1)]
    for cp in flat_loads[3 * NT:] + edge_loads + mid_loads + flat_loads[:3 * NT] + scalar_loads:
        cp.start()

    n_copies = 0

    def remote(src, dst, c, r, sends, receives):
        nonlocal n_copies
        i = n_copies
        n_copies += 1
        return (pltpu.make_async_remote_copy(src, dst, ssem.at[i], rsem.at[i], device_id=dev(c, r), device_id_type=MESH), sends, receives)

    def maybe(cond, fn):
        if cond is None:
            fn()
        else:
            pl.when(cond)(fn)

    def start(group):
        for cp, sends, _ in group:
            maybe(sends, cp.start)

    def arrive(group):
        for cp, _, receives in group:
            maybe(receives, cp.wait_recv)

    def drain(group):
        for cp, sends, _ in group:
            maybe(sends, cp.wait_send)

    def rows_of(fields):
        return [remote(pn.at[fields], rs.at[fields], col, row + 1, has_n, has_s),
                remote(ps.at[fields], rn.at[fields], col, row - 1, has_s, has_n)]

    def level_rows(b, k, r):
        return b.reshape(NT, SLOT * PR, L), pl.ds(k * PR + r, 8, stride=PR)

    def pack_rows(fields):
        for f in fields:
            for t in range(NT):
                for k in range(0, SLOT, 8):
                    for to, r in ((pn, R0 + NR - 1), (ps, R0)):
                        flat, at = level_rows(bufs[f], k, r)
                        to[f, t, k:k + 8, :] = flat[t, at, :]

    def unpack_rows(fields):
        for f in fields:
            for t in range(NT):
                for k in range(0, SLOT, 8):
                    for to, r in ((rs, R0 - 1), (rn, R0 + NR)):
                        flat, at = level_rows(bufs[f], k, r)
                        flat[t, at, :] = to[f, t, k:k + 8, :]

    def wide_of(b, lanes_w, lanes_e, from_e, from_w):
        own = b.at[:, 0:NT, XO:XO + NR, :]
        return [remote(own, b.at[:, 0:NT, 8:XO, :], col, row + 1, has_n, has_s),
                remote(own, b.at[:, 0:NT, XO + NR:XO + 2 * NR, :], col, row - 1, has_s, has_n),
                remote(lanes_w, from_e.at[1], west, row, None, None),
                remote(lanes_e, from_w.at[1], east, row, None, None),
                remote(lanes_w, from_e.at[2], west, row - 1, has_s, has_n),
                remote(lanes_e, from_w.at[2], east, row - 1, has_s, has_n),
                remote(lanes_w, from_e.at[0], west, row + 1, has_n, has_s),
                remote(lanes_e, from_w.at[0], east, row + 1, has_n, has_s)]

    row_group, late_group = rows_of(slice(0, 2)), rows_of(slice(2, 4))
    lane_group = [remote(pw, re.at[R0:R0 + NR, :], west, row, None, None),
                  remote(pe, rw.at[R0:R0 + NR, :], east, row, None, None),
                  remote(pe.at[0:1, :], rw.at[R0 + NR:R0 + NR + 1, :], east, row - 1, has_s, has_n),
                  remote(pw.at[NR - 1:NR, :], re.at[R0 - 1:R0, :], west, row + 1, has_n, has_s)]
    wide_group = wide_of(x, qw, qe, we, ww)
    force_group = wide_of(xf, fw, fe, fre, frw)

    edge = jnp.logical_or(row == 0, row == n_row - 1)

    @pl.when(edge)
    def _():
        pl.semaphore_wait(barrier, 5)

    @pl.when(jnp.logical_not(edge))
    def _():
        pl.semaphore_wait(barrier, 8)

    lane_p = lax.broadcasted_iota(jnp.int32, (PR, L), 1)
    lane = lane_p[:NR]

    for t in range(NT):
        bt[t, LEV, R0:R0 + NR, :] = zero((NR, L))
        bs[t, LEV, R0:R0 + NR, :] = zero((NR, L))
    for cp in flat_loads[3 * NT:]:
        cp.wait()
    for t in range(NT):
        count = cnt_i[t].astype(f32)
        bu[t, LEV, R0:R0 + NR, :] = count
        x[3, t, XO:XO + NR, :] = jnp.where(count > 0.0, bv[t, LEV, R0:R0 + NR, :], 0.0)

    def roll(a, shift):
        return pltpu.roll(a, shift, 1) if not (isinstance(shift, int) and shift % L == 0) else a

    pair = lax.shift_right_logical(lane, 1)
    packed = [zero((NR, L))] * 2
    for f, b in enumerate(bufs):
        edge_loads[2 * f].wait()
        edge_loads[2 * f + 1].wait()
        for k in range(SLOT):
            p = SLOT * (f % 2) + k
            both = jnp.where(lane == 0, b[0, k, R0:R0 + NR, :], b[NT - 1, k, R0:R0 + NR, :])
            packed[f // 2] = jnp.where(pair == p, roll(both, (2 * p + 1) % L), packed[f // 2])
    even = lax.rem(lane_p, 2) == 0
    pw[...] = jnp.where(even[:NR], roll(packed[1], L - 1), packed[0])
    pe[...] = jnp.where(even[:NR], packed[0], roll(packed[1], 1))
    start(lane_group)
    for cp in mid_loads:
        cp.wait()
    pack_rows((0, 1))
    start(row_group)
    pack_rows((2, 3))
    start(late_group)

    def pack_wide(b, n_fields):
        first = last = zero((NR, L))
        for f in range(n_fields):
            mine = (lane >= 32 * f) & (lane < 32 * f + 32)
            first = jnp.where(mine, roll(b[f, 0, XO:XO + NR, :], 32 * f), first)
            last = jnp.where(mine, roll(b[f, NT - 1, XO:XO + NR, :], (32 * f + 32) % L), last)
        return first, last

    for cp in flat_loads[:3 * NT]:
        cp.wait()
    first, last = pack_wide(x, 4)
    qw[...] = first
    qe[...] = last
    start(wide_group)
    for cp in scalar_loads:
        cp.wait()

    for f in range(4):
        for t in range(NT + 1):
            x[f, t, 0:8, :] = zero((8, L))
            x[f, t, XR - 8:XR, :] = zero((8, L))
    for t in range(NT + 1):
        tt[t, XR - 8:XR, :] = zero((8, L))
    for t in range(NT):
        for a in (xu, xv, xt, xs):
            a[t, 0] = zero((NR, L))

    @pl.when(jnp.logical_not(has_s))
    def _():
        rs[...] = zero((4, NT, SLOT, L))
        re[R0 - 8:R0, :] = zero((8, L))
        x[:, 0:NT, 8:XO, :] = zero((4, NT, NR, L))
        xf[:, 0:NT, 8:XO, :] = zero((2, NT, NR, L))
        for a in (we, ww, fre, frw):
            a[0] = zero((NR, L))

    @pl.when(jnp.logical_not(has_n))
    def _():
        rn[...] = zero((4, NT, SLOT, L))
        rw[R0 + NR:PR, :] = zero((8, L))
        x[:, 0:NT, XO + NR:XO + 2 * NR, :] = zero((4, NT, NR, L))
        xf[:, 0:NT, XO + NR:XO + 2 * NR, :] = zero((2, NT, NR, L))
        for a in (we, ww, fre, frw):
            a[2] = zero((NR, L))


    row_pos = (row * NR + lax.broadcasted_iota(jnp.int32, (NR, L), 0)).astype(f32)
    total_rows = NR * n_row
    fu4[...] = 0.25 * (CORIO_F0 + CORIO_BETA * ((row_pos + 0.5) / total_rows - 0.5))
    fv4[...] = 0.25 * (CORIO_F0 + CORIO_BETA * ((row_pos + 1.0) / total_rows - 0.5))

    def to_east(tiles, halo, ts=range(NT)):
        last_lane = lane_p[:tiles[ts[0]].shape[0]] == L - 1
        rolled = {t: halo if t == NT else roll(tiles[t], L - 1) for t in sorted({t + d for t in ts for d in (0, 1)})}
        return {t: jnp.where(last_lane, rolled[t + 1], rolled[t]) for t in ts}

    def to_west(tiles, halo, ts=range(NT)):
        first_lane = lane_p[:tiles[ts[0]].shape[0]] == 0
        rolled = {t: halo if t < 0 else roll(tiles[t], 1) for t in sorted({t + d for t in ts for d in (-1, 0)})}
        return {t: jnp.where(first_lane, rolled[t - 1], rolled[t]) for t in ts}

    def side(f, k, lo=R0, n=NR):
        return pltpu.roll(ha[f // 2, lo:lo + n, :], lax.rem(L - 2 * (SLOT * (f % 2) + k), L), 1)

    def level(b, k, lo=R0, n=NR):
        return [b[t, k, lo:lo + n, :] for t in range(NT)]

    def each_level(fn, unroll):
        def some(i, _):
            base = i * unroll
            for j in range(unroll):
                fn(base + j, base + j - 1 if j else jnp.maximum(base - 1, 0), j % 2)
            return 0

        lax.fori_loop(0, -(-LEV // unroll), some, 0)

    p_scale = BC_GRAVITY / LEV

    def pressure(t, lo, n):
        total = zero((n, L))
        for k in range(LEV):
            density = CONTRACT_S * bs[t, k, lo:lo + n, :] - EXPAND_T * bt[t, k, lo:lo + n, :]
            total = total + density
            bp[t, k, lo:lo + n, :] = p_scale * (total - 0.5 * density)
        bp[t, LEV, lo:lo + n, :] = zero((n, L))

    def own_pressure(t, _):
        pressure(t, R0, NR)
        for k in range(LEV):
            bp[t, k, R0 + NR:PR, :] = zero((8, L))
        return 0

    lax.fori_loop(0, NT, own_pressure, 0)

    def momentum_down(ts, k, prev, slot):
        scale, carry = tab_s[k], tab_s[SLOT + k]
        u5, v5 = level(bu, k, R0, NR + 8), level(bv, k, R0 - 8, NR + 8)
        u_side = v_side = p_side = jnp.zeros((NR + 8, L), f32)
        if 0 in ts:
            u_side, v_side = side(0, k, R0, NR + 8), side(1, k, R0 - 8, NR + 8)
            p_side = pltpu.roll(rp[...], L - 1 - 2 * k, 1)
        uw, ve = to_west(u5, u_side, ts), to_east(v5, v_side, ts)
        um, vm = [a[:NR] for a in u5], [a[8:] for a in v5]
        ue, vw = to_east(um, u_side[:NR], ts), to_west(vm, v_side[8:], ts)
        pm, pn = level(bp, k), level(bp, k, R0 + 1)
        pe_ = to_east(pm, p_side, ts)
        for t in ts:
            u_sum, v_sum = u5[t] + uw[t], v5[t] + ve[t]
            s1[slot, t] = u_sum
            s2[slot, t] = v_sum
            ub4 = u_sum[:NR] + s1[slot, t, 1:NR + 1, :]
            vb4 = v_sum[8:] + s2[slot, t, 7:NR + 7, :]
            un, us = bu[t, k, R0 + 1:R0 + 1 + NR, :], bu[t, k, R0 - 1:R0 - 1 + NR, :]
            vn, vs = bv[t, k, R0 + 1:R0 + 1 + NR, :], bv[t, k, R0 - 1:R0 - 1 + NR, :]
            u_star = um[t] + vb4 * (fu4[...] - 0.125 * (un - us)) - um[t] * (0.5 * (ue[t] - uw[t][:NR])) + (pm[t] - pe_[t])
            v_star = vm[t] - ub4 * (fv4[...] + 0.125 * (ve[t][8:] - vw[t])) - vm[t] * (0.5 * (vn - vs)) + (pm[t] - pn[t])
            xu[t, k] = scale * u_star + carry * xu[t, prev]
            xv[t, k] = scale * v_star + carry * xv[t, prev]

    arrive(lane_group)
    ha[0] = jnp.where(even, rw[...], roll(re[...], L - 2))
    ha[1] = jnp.where(even, roll(rw[...], L - 1), roll(re[...], L - 1))
    east_ = roll(ha[1, R0:R0 + NR, :], 1)
    density = CONTRACT_S * roll(east_, L // 2) - EXPAND_T * east_
    total = density
    for step in (2, 4, 8, 16, 32):
        total = total + jnp.where(lane >= step, roll(total, step), 0.0)
    rp[...] = p_scale * (total - 0.5 * density)
    arrive(row_group)
    unpack_rows((0, 1))
    each_level(functools.partial(momentum_down, tuple(range(NT))), UNROLL_M)

    arrive(late_group)
    unpack_rows((2, 3))
    last_row = lax.broadcasted_iota(jnp.int32, (8, L), 0) == 7

    def north_pressure(t, _):
        pressure(t, R0 + NR, 8)
        sweep = zero((8, L))
        for k in range(LEV):
            sweep = tab_s[SLOT + k] * sweep - tab_s[k] * bp[t, k, R0 + NR - 7:R0 + NR + 1, :]
            xv[t, k, NR - 8:NR, :] += jnp.where(last_row, sweep, 0.0)
        return 0

    lax.fori_loop(0, NT, north_pressure, 0)

    c_mid, d_mid = level(bu, LEV), level(bv, LEV)
    c_east = to_east(c_mid, side(0, LEV))
    d_east = to_east(d_mid, side(1, LEV))
    c_north, c_south = level(bu, LEV, R0 + 1), level(bu, LEV, R0 - 1)
    d_north = level(bv, LEV, R0 + 1)
    for t in range(NT):
        cu[t] = jnp.minimum(c_mid[t], c_east[t])
        cv[t] = jnp.minimum(c_mid[t], c_north[t])
        hu[t] = 0.5 * (d_mid[t] + d_east[t])
        hv[t] = 0.5 * (d_mid[t] + d_north[t])
        cc_o[t] = c_mid[t]
    c_west0 = jnp.minimum(side(0, LEV), c_mid[0])

    def momentum_up(t, _):
        z = zero((NR, L))
        state = [[z, z, z], [z, z, z]]
        for k in range(LEV - 1, -1, -1):
            link, last_ = tab_s[2 * SLOT + k], tab_s[3 * SLOT + k]
            for q, (sweep, b, count) in enumerate(((xu, bu, cu), (xv, bv, cv))):
                below, sum_x, sum_0 = state[q]
                value = sweep[t, k]
                active = count[t] > float(k)
                solved = jnp.where(count[t] > float(k + 1), value + link * below, jnp.where(active, last_ * value, 0.0))
                sweep[t, k] = solved
                start_ = jnp.where(active, b[t, k, R0:R0 + NR, :], 0.0)
                b[t, k, R0:R0 + NR, :] = start_
                state[q] = [solved, sum_x + solved, sum_0 + start_]
        for q, (h, mean, count) in enumerate(((hu, su, cu), (hv, sv, cv))):
            _, total, start_ = state[q]
            n_active = jnp.maximum(count[t], 1.0)
            mean[t] = total / n_active
            xf[q, t, XO:XO + NR, :] = h[t] * (total - start_) / n_active / TIME_STEP
        c_south = jnp.minimum(bu[t, LEV, 0:8, :], pltpu.roll(bu[t, LEV, R0:R0 + 8, :], 7, 0))
        for k in range(LEV):
            bv[t, k, 0:8, :] = jnp.where(c_south > float(k), bv[t, k, 0:8, :], 0.0)
        return 0

    lax.fori_loop(0, NT, momentum_up, 0)

    first, last = pack_wide(xf, 2)
    fw[...] = first
    fe[...] = last
    start(force_group)

    def tracer_down(k, prev, slot):
        scale, carry = tab_s[4 * SLOT + k], tab_s[5 * SLOT + k]
        kf = lax.convert_element_type(k, f32)
        um, vm, vs = level(bu, k), level(bv, k), level(bv, k, R0 - 1)
        uw0 = jnp.where(c_west0 > kf, side(0, k), 0.0)
        for f, b, sweep in ((2, bt, xt), (3, bs, xs)):
            q = level(b, k)
            q_side = side(f, k)
            qe_ = to_east(q, q_side)
            f_east = [um[t] * (q[t] + qe_[t]) for t in range(NT)]
            f_west = to_west(f_east, uw0 * (q_side + q[0]))
            for t in range(NT):
                f_north = vm[t] * (q[t] + b[t, k, R0 + 1:R0 + 1 + NR, :])
                f_south = vs[t] * (b[t, k, R0 - 1:R0 - 1 + NR, :] + q[t])
                new = q[t] - 0.5 * TIME_STEP * (f_east[t] - f_west[t] + f_north - f_south)
                sweep[t, k] = jnp.where(bu[t, LEV, R0:R0 + NR, :] > kf, scale * new + carry * sweep[t, prev], new)

    each_level(tracer_down, UNROLL_T)

    arrive(wide_group)
    drain(wide_group)
    arrive(force_group)

    def unpack_wide(b, from_e, from_w, n_fields):
        for f in range(n_fields):
            for seg in range(3):
                b[f, NT, 8 + NR * seg:8 + NR * seg + NR, :] = jnp.where(lane < L // 2, roll(from_e[seg], (L - 32 * f) % L), roll(from_w[seg], (96 - 32 * f) % L))

    unpack_wide(x, we, ww, 4)
    unpack_wide(xf, fre, frw, 2)
    dt_fast = TIME_STEP / n_sub
    XT = NT + 1

    def ring_east(tiles, last_lane):
        rolled = [roll(a, L - 1) for a in tiles]
        return [jnp.where(last_lane, rolled[(t + 1) % XT], rolled[t]) for t in range(XT)]

    def ring_west(tiles, first_lane):
        rolled = [roll(a, 1) for a in tiles]
        return [jnp.where(first_lane, rolled[(t - 1) % XT], rolled[t]) for t in range(XT)]

    for seg in range(3):
        lo = 8 + NR * seg
        pos = (row * NR + NR * (seg - 1) + lax.broadcasted_iota(jnp.int32, (NR, L), 0)).astype(f32)
        f_u = CORIO_F0 + CORIO_BETA * ((pos + 0.5) / total_rows - 0.5)
        f_v = CORIO_F0 + CORIO_BETA * ((pos + 1.0) / total_rows - 0.5)
        d = [x[3, t, lo:lo + NR, :] for t in range(XT)]
        d_e = ring_east(d, lane == L - 1)
        for t in range(XT):
            d_n = x[3, t, lo + 1:lo + 1 + NR, :]
            wet = jnp.where((d[t] > 0.0) & (d_e[t] > 0.0), 1.0, 0.0)
            cm[t, lo:lo + NR, :] = wet
            ca[t, lo:lo + NR, :] = (0.25 * dt_fast) * f_u * wet
            cb[t, lo:lo + NR, :] = (dt_fast * GRAVITY * 0.5) * (d[t] + d_e[t]) * wet
            cc[t, lo:lo + NR, :] = dt_fast * xf[0, t, lo:lo + NR, :] * wet
            wet = jnp.where((d[t] > 0.0) & (d_n > 0.0), 1.0, 0.0)
            cn[t, lo:lo + NR, :] = wet
            cd[t, lo:lo + NR, :] = (0.25 * dt_fast) * f_v * wet
            cg[t, lo:lo + NR, :] = (dt_fast * GRAVITY * 0.5) * (d[t] + d_n) * wet
            ch[t, lo:lo + NR, :] = dt_fast * xf[1, t, lo:lo + NR, :] * wet

    for t in range(NT):
        au[t] = zero((NR, L))
        av[t] = zero((NR, L))

    def subcycle(side_rows, masked, n, _):
        weight = w_s[n]
        parts = ((XO - side_rows, side_rows), (XO, NR), (XO + NR, side_rows))
        for r, chunk in parts:
            first_lane = lane[:chunk] == 0
            u_t = [x[1, t, r:r + chunk, :] for t in range(XT)]
            u_w = ring_west(u_t, first_lane)
            for t in range(XT):
                v_t, v_s = x[2, t, r:r + chunk, :], x[2, t, r - 1:r - 1 + chunk, :]
                x[0, t, r:r + chunk, :] = x[0, t, r:r + chunk, :] - dt_fast * ((u_t[t] - u_w[t]) + (v_t - v_s))
                tt[t, r:r + chunk, :] = u_t[t] + u_w[t]
        for r, chunk in parts[::-1]:
            last_lane = lane[:chunk] == L - 1
            e_t = [x[0, t, r:r + chunk, :] for t in range(XT)]
            e_e = ring_east(e_t, last_lane)
            v_t = [x[2, t, r:r + chunk, :] for t in range(XT)]
            s_t = [v_t[t] + x[2, t, r - 1:r - 1 + chunk, :] for t in range(XT)]
            s_e = ring_east(s_t, last_lane)
            for t in range(XT):
                at = (t, slice(r, r + chunk))
                up = (t, slice(r + 1, r + 1 + chunk))
                e_n = x[0, t, r + 1:r + 1 + chunk, :]
                u_old = x[1, t, r:r + chunk, :] if masked else cm[at] * x[1, t, r:r + chunk, :]
                v_old = v_t[t] if masked else cn[at] * v_t[t]
                u_new = u_old + ca[at] * (s_t[t] + s_e[t]) + cc[at] - cb[at] * (e_e[t] - e_t[t])
                v_new = v_old - cd[at] * (tt[at] + tt[up]) + ch[at] - cg[at] * (e_n - e_t[t])
                x[1, t, r:r + chunk, :] = u_new
                x[2, t, r:r + chunk, :] = v_new
                if r == XO and t < NT:
                    au[t] += weight * u_new
                    av[t] += weight * v_new
        return 0

    done = 0
    for tiles in (4, 3, 2, 1):
        until = n_sub - 8 * (tiles - 1)
        stretch = functools.partial(subcycle, 8 * tiles)
        if done == 0:
            stretch(False, 0, 0)
            done = 1
        lax.fori_loop(done, until, functools.partial(stretch, True), 0)
        done = until

    for t in range(NT):
        eta_o[t] = x[0, t, XO:XO + NR, :]
        tu_o[t] = x[1, t, XO:XO + NR, :]
        tv_o[t] = x[2, t, XO:XO + NR, :]
        gu_o[t] = au[t] / hu[t] - su[t]
        gv_o[t] = av[t] / hv[t] - sv[t]

    for group in (row_group, late_group, lane_group, force_group):
        drain(group)


def final_kernel(tab_s, xu, xv, xt, xs, gu, gv, cu, cv, cc, eta, tu, tv, eta_h, tu_h, tv_h, u_h, v_h, t_h, s_h, flat_b, u_b, v_b, t_b, s_b, sem):
    stores = []
    for i, (a, o) in enumerate(((eta, eta_h), (tu, tu_h), (tv, tv_h))):
        for t in range(NT):
            flat_b[i, :, L * t:L * t + L] = a[t]
        stores.append(pltpu.make_async_copy(flat_b.at[i], o, sem.at[4, i]))
        stores[-1].start()

    below = [[jnp.zeros((NR, L), f32)] * NT for _ in range(2)]
    top = LEV
    for k in range(LEV - 1, -1, -1):
        link, last = tab_s[6 * SLOT + k], tab_s[7 * SLOT + k]
        for t in range(NT):
            cols = slice(L * t, L * t + L)
            u_b[k, :, cols] = jnp.where(cu[t] > float(k), xu[t, k] + gu[t], 0.0)
            v_b[k, :, cols] = jnp.where(cv[t] > float(k), xv[t, k] + gv[t], 0.0)
            for q, (sweep, b) in enumerate(((xt, t_b), (xs, s_b))):
                value = sweep[t, k]
                solved = jnp.where(cc[t] > float(k + 1), value + link * below[q][t], jnp.where(cc[t] > float(k), last * value, value))
                below[q][t] = solved
                b[k, :, cols] = solved
        if k in GROUPS:
            for i, (b, o) in enumerate(((u_b, u_h), (v_b, v_h), (t_b, t_h), (s_b, s_h))):
                stores.append(pltpu.make_async_copy(b.at[k:top], o.at[k:top], sem.at[i, GROUPS.index(k)]))
                stores[-1].start()
            top = k
    for cp in stores:
        cp.wait()


def solution(mesh):
    n_col = mesh.shape['col']
    n_row = mesh.shape['row']

    def step(vel_u, vel_v, value_a11, salinity, surf_eta, trans_u, trans_v, bottom_depth, level_count, avg_weights):
        n_sub = avg_weights.shape[0]
        table = jnp.asarray(solve_table(LEV))
        hbm = pl.BlockSpec(memory_space=pltpu.HBM)
        vmem = pl.BlockSpec(memory_space=pltpu.VMEM)
        smem = pl.BlockSpec(memory_space=pltpu.SMEM)
        V = pltpu.VMEM
        tile = V((NT, NR, L), f32)
        sweep = V((NT, SLOT, NR, L), f32)
        wide = (NT + 1, XR, L)
        scratch = ([V((NT, SLOT, PR, L), f32)] * 5 + [V((NT, NR, L), jnp.int32), V((NR, L), f32)]
                   + [V((2, NT, NR + 8, L), f32)] * 2 + [V((4, NT, SLOT, L), f32)] * 4 + [V((NR, L), f32)] * 2 + [V((PR, L), f32)] * 2 + [V((2, PR, L), f32)]
                   + [V((4,) + wide, f32), V((2,) + wide, f32)] + [V((NR, L), f32)] * 2 + [V((3, NR, L), f32)] * 2
                   + [V((NR, L), f32)] * 2 + [V((3, NR, L), f32)] * 2
                   + [V((NR, L), f32)] * 2 + [V((NT, NR, L), f32)] * 4
                   + [V(wide, f32)] * 9 + [V((NT, NR, L), f32)] * 2
                   + [pltpu.SMEM((n_sub,), f32), pltpu.SMEM((8 * SLOT,), f32)]
                   + [pltpu.SemaphoreType.DMA((40,)), pltpu.SemaphoreType.DMA((64,)), pltpu.SemaphoreType.DMA((64,))])
        outs = pl.pallas_call(
            functools.partial(ocean_kernel, tuple(mesh.axis_names), n_col, n_row, n_sub),
            out_shape=[tile] * 8 + [sweep] * 4,
            in_specs=[hbm] * 11,
            out_specs=[vmem] * 12,
            scratch_shapes=scratch,
            compiler_params=pltpu.CompilerParams(collective_id=0, has_side_effects=True, vmem_limit_bytes=32 * 1024 * 1024),
        )(*[pltpu.with_memory_space_constraint(a, pltpu.HBM) for a in (vel_u, vel_v, value_a11, salinity, surf_eta, trans_u, trans_v, bottom_depth, level_count, avg_weights, table)])
        eta, tu, tv, gu, gv, cu, cv, cc, xu, xv, xt, xs = [pltpu.with_memory_space_constraint(o, pltpu.VMEM) for o in outs]

        cube = jax.ShapeDtypeStruct((LEV, NR, NC), f32)
        flat = jax.ShapeDtypeStruct((NR, NC), f32)
        return tuple(pl.pallas_call(
            final_kernel,
            out_shape=[flat] * 3 + [cube] * 4,
            in_specs=[smem] + [vmem] * 12,
            out_specs=[hbm] * 7,
            scratch_shapes=[V((3, NR, NC), f32)] + [V((LEV, NR, NC), f32)] * 4 + [pltpu.SemaphoreType.DMA((5, len(GROUPS)))],
            compiler_params=pltpu.CompilerParams(vmem_limit_bytes=24 * 1024 * 1024),
        )(table, xu, xv, xt, xs, gu, gv, cu, cv, cc, eta, tu, tv))

    cube = P(None, 'row', 'col')
    flat = P('row', 'col')
    return jax.shard_map(step, mesh=mesh, in_specs=(cube, cube, cube, cube, flat, flat, flat, flat, flat, P()), out_specs=(flat, flat, flat, cube, cube, cube, cube), check_vma=False)
```

```python
import functools

import jax
import jax.numpy as jnp
import numpy as np
from jax import lax
from jax.experimental import pallas as pl
from jax.experimental.pallas import tpu as pltpu
from jax.sharding import PartitionSpec as P

TIME_STEP = 1.0
GRAVITY = 16.0
BC_GRAVITY = 4.0
EXPAND_T = 0.2
CONTRACT_S = 0.6
CORIO_F0 = 0.4
CORIO_BETA = 0.4
VISC_R = 2.0
DIFF_R = 0.5

LEV = 31
SLOT = 32
NR = 32
NC = 512
NT = 4
L = 128
R0 = 8
PR = 56
KA = SLOT + 1
RA = NR + 8
XR = 120
XO = 40
MESH = pl.DeviceIdType.MESH
f32 = jnp.float32
UNROLL_M = 4
UNROLL_T = 1
GROUPS = (28, 24, 20, 16, 12, 8, 4, 2, 0)


def solve_table(n_levels):
    rows = []
    for s in (VISC_R, DIFF_R):
        scale, carry, link, last = np.zeros((4, SLOT))
        ratio = 0.0
        for k in range(n_levels):
            low = s if k else 0.0
            full = 1.0 + low + s - low * ratio
            end = 1.0 + low - low * ratio
            scale[k], carry[k], link[k], last[k] = 1.0 / full, low / full, s / full, full / end
            ratio = s / full
        rows += [scale, carry, link, last]
    return np.concatenate(rows).astype(np.float32)


def ocean_kernel(axes, n_col, n_row, n_sub, *refs):
    (u_h, v_h, t_h, s_h, eta_h, tu_h, tv_h, dep_h, cnt_h, w_h, tab_h,
     eta_o, tu_o, tv_o, gu_o, gv_o, cu, cv, cc_o, xu, xv, xt, xs,
     bu, bv, bt, bs, bp, cnt_i, rp, s1, s2,
     pn, ps, rn, rs, pw, pe, rw, re, ha, x, xf, qw, qe, we, ww, fw, fe, fre, frw,
     fu4, fv4, hu, hv, su, sv,
     ca, cb, cc, cd, cg, ch, cm, cn, tt, au, av,
     w_s, tab_s, lsem, ssem, rsem) = refs
    xu, xv, xt, xs = [a.at[:, 0:SLOT, 0:NR, :] for a in (xu, xv, xt, xs)]
    eta_o, tu_o, tv_o, gu_o, gv_o, cu, cv, cc_o, hu, hv, su, sv, au, av = [a.at[:, 0:NR, :] for a in (eta_o, tu_o, tv_o, gu_o, gv_o, cu, cv, cc_o, hu, hv, su, sv, au, av)]
    col = lax.axis_index('col')
    row = lax.axis_index('row')
    east = lax.rem(col + 1, n_col)
    west = lax.rem(col + n_col - 1, n_col)
    has_s = row > 0
    has_n = row < n_row - 1

    def dev(c, r):
        at = {'col': c, 'row': r}
        return tuple(at[name] for name in axes)

    bufs = (bu, bv, bt, bs)
    barrier = pltpu.get_barrier_semaphore()

    def signal(c, r):
        pl.semaphore_signal(barrier, inc=1, device_id=dev(c, r), device_id_type=MESH)

    signal(west, row)
    signal(east, row)

    @pl.when(has_s)
    def _():
        for c in (west, col, east):
            signal(c, row - 1)

    @pl.when(has_n)
    def _():
        for c in (west, col, east):
            signal(c, row + 1)

    zero = functools.partial(jnp.zeros, dtype=f32)

    loads = []
    for f, (src, dst) in enumerate(zip((u_h, v_h, t_h, s_h), bufs)):
        for t in range(NT):
            loads.append(pltpu.make_async_copy(src.at[:, :, L * t:L * t + L], dst.at[t, 0:LEV, R0:R0 + NR, :], lsem.at[len(loads)]))
    flat_loads = []
    for f, src in enumerate((eta_h, tu_h, tv_h)):
        for t in range(NT):
            flat_loads.append(pltpu.make_async_copy(src.at[:, L * t:L * t + L], x.at[f, t, XO:XO + NR, :], lsem.at[len(loads) + len(flat_loads)]))
    for t in range(NT):
        flat_loads.append(pltpu.make_async_copy(dep_h.at[:, L * t:L * t + L], bv.at[t, LEV, R0:R0 + NR, :], lsem.at[len(loads) + len(flat_loads)]))
    for t in range(NT):
        flat_loads.append(pltpu.make_async_copy(cnt_h.at[:, L * t:L * t + L], cnt_i.at[t], lsem.at[len(loads) + len(flat_loads)]))
    scalar_loads = [pltpu.make_async_copy(w_h, w_s, lsem.at[36]), pltpu.make_async_copy(tab_h, tab_s, lsem.at[37])]
    edge_loads = [loads[NT * f + t] for f in range(4) for t in (0, NT - 1)]
    mid_loads = [loads[NT * f + t] for f in range(4) for t in range(1, NT - 1)]
    for cp in flat_loads[3 * NT:] + edge_loads + mid_loads + flat_loads[:3 * NT] + scalar_loads:
        cp.start()

    n_copies = 0

    def remote(src, dst, c, r, sends, receives):
        nonlocal n_copies
        i = n_copies
        n_copies += 1
        return (pltpu.make_async_remote_copy(src, dst, ssem.at[i], rsem.at[i], device_id=dev(c, r), device_id_type=MESH), sends, receives)

    def maybe(cond, fn):
        if cond is None:
            fn()
        else:
            pl.when(cond)(fn)

    def start(group):
        for cp, sends, _ in group:
            maybe(sends, cp.start)

    def arrive(group):
        for cp, _, receives in group:
            maybe(receives, cp.wait_recv)

    def drain(group):
        for cp, sends, _ in group:
            maybe(sends, cp.wait_send)

    def rows_of(fields):
        return [remote(pn.at[fields], rs.at[fields], col, row + 1, has_n, has_s),
                remote(ps.at[fields], rn.at[fields], col, row - 1, has_s, has_n)]

    def level_rows(b, k, r):
        return b.reshape(NT, KA * PR, L), pl.ds(k * PR + r, 8, stride=PR)

    def pack_rows(fields):
        for f in fields:
            for t in range(NT):
                for k in range(0, SLOT, 8):
                    for to, r in ((pn, R0 + NR - 1), (ps, R0)):
                        flat, at = level_rows(bufs[f], k, r)
                        to[f, t, k:k + 8, :] = flat[t, at, :]

    def unpack_rows(fields):
        for f in fields:
            for t in range(NT):
                for k in range(0, SLOT, 8):
                    for to, r in ((rs, R0 - 1), (rn, R0 + NR)):
                        flat, at = level_rows(bufs[f], k, r)
                        flat[t, at, :] = to[f, t, k:k + 8, :]

    def wide_of(b, lanes_w, lanes_e, from_e, from_w):
        own = b.at[:, 0:NT, XO:XO + NR, :]
        return [remote(own, b.at[:, 0:NT, 8:XO, :], col, row + 1, has_n, has_s),
                remote(own, b.at[:, 0:NT, XO + NR:XO + 2 * NR, :], col, row - 1, has_s, has_n),
                remote(lanes_w, from_e.at[1], west, row, None, None),
                remote(lanes_e, from_w.at[1], east, row, None, None),
                remote(lanes_w, from_e.at[2], west, row - 1, has_s, has_n),
                remote(lanes_e, from_w.at[2], east, row - 1, has_s, has_n),
                remote(lanes_w, from_e.at[0], west, row + 1, has_n, has_s),
                remote(lanes_e, from_w.at[0], east, row + 1, has_n, has_s)]

    row_group, late_group = rows_of(slice(0, 2)), rows_of(slice(2, 4))
    lane_group = [remote(pw, re.at[R0:R0 + NR, :], west, row, None, None),
                  remote(pe, rw.at[R0:R0 + NR, :], east, row, None, None),
                  remote(pe.at[0:1, :], rw.at[R0 + NR:R0 + NR + 1, :], east, row - 1, has_s, has_n),
                  remote(pw.at[NR - 1:NR, :], re.at[R0 - 1:R0, :], west, row + 1, has_n, has_s)]
    wide_group = wide_of(x, qw, qe, we, ww)
    force_group = wide_of(xf, fw, fe, fre, frw)

    edge = jnp.logical_or(row == 0, row == n_row - 1)

    @pl.when(edge)
    def _():
        pl.semaphore_wait(barrier, 5)

    @pl.when(jnp.logical_not(edge))
    def _():
        pl.semaphore_wait(barrier, 8)

    lane_p = lax.broadcasted_iota(jnp.int32, (PR, L), 1)
    lane = lane_p[:NR]

    for t in range(NT):
        bt[t, LEV, R0:R0 + NR, :] = zero((NR, L))
        bs[t, LEV, R0:R0 + NR, :] = zero((NR, L))
    for cp in flat_loads[3 * NT:]:
        cp.wait()
    for t in range(NT):
        count = cnt_i[t].astype(f32)
        bu[t, LEV, R0:R0 + NR, :] = count
        x[3, t, XO:XO + NR, :] = jnp.where(count > 0.0, bv[t, LEV, R0:R0 + NR, :], 0.0)

    def roll(a, shift):
        return pltpu.roll(a, shift, 1) if not (isinstance(shift, int) and shift % L == 0) else a

    pair = lax.shift_right_logical(lane, 1)
    packed = [zero((NR, L))] * 2
    for f, b in enumerate(bufs):
        edge_loads[2 * f].wait()
        edge_loads[2 * f + 1].wait()
        for k in range(SLOT):
            p = SLOT * (f % 2) + k
            both = jnp.where(lane == 0, b[0, k, R0:R0 + NR, :], b[NT - 1, k, R0:R0 + NR, :])
            packed[f // 2] = jnp.where(pair == p, roll(both, (2 * p + 1) % L), packed[f // 2])
    even = lax.rem(lane_p, 2) == 0
    pw[...] = jnp.where(even[:NR], roll(packed[1], L - 1), packed[0])
    pe[...] = jnp.where(even[:NR], packed[0], roll(packed[1], 1))
    start(lane_group)
    for cp in mid_loads:
        cp.wait()
    pack_rows((0, 1))
    start(row_group)
    pack_rows((2, 3))
    start(late_group)

    def pack_wide(b, n_fields):
        first = last = zero((NR, L))
        for f in range(n_fields):
            mine = (lane >= 32 * f) & (lane < 32 * f + 32)
            first = jnp.where(mine, roll(b[f, 0, XO:XO + NR, :], 32 * f), first)
            last = jnp.where(mine, roll(b[f, NT - 1, XO:XO + NR, :], (32 * f + 32) % L), last)
        return first, last

    for cp in flat_loads[:3 * NT]:
        cp.wait()
    first, last = pack_wide(x, 4)
    qw[...] = first
    qe[...] = last
    start(wide_group)
    for cp in scalar_loads:
        cp.wait()

    for f in range(4):
        for t in range(NT + 1):
            x[f, t, 0:8, :] = zero((8, L))
            x[f, t, XR - 16:XR, :] = zero((16, L))
    for t in range(NT + 1):
        tt[t, XR - 16:XR, :] = zero((16, L))
    for t in range(NT):
        for a in (xu, xv, xt, xs):
            a[t, 0] = zero((NR, L))

    @pl.when(jnp.logical_not(has_s))
    def _():
        rs[...] = zero((4, NT, SLOT, L))
        re[R0 - 8:R0, :] = zero((8, L))
        x[:, 0:NT, 8:XO, :] = zero((4, NT, NR, L))
        xf[:, 0:NT, 8:XO, :] = zero((2, NT, NR, L))
        for a in (we, ww, fre, frw):
            a[0] = zero((NR, L))

    @pl.when(jnp.logical_not(has_n))
    def _():
        rn[...] = zero((4, NT, SLOT, L))
        rw[R0 + NR:R0 + NR + 8, :] = zero((8, L))
        x[:, 0:NT, XO + NR:XO + 2 * NR, :] = zero((4, NT, NR, L))
        xf[:, 0:NT, XO + NR:XO + 2 * NR, :] = zero((2, NT, NR, L))
        for a in (we, ww, fre, frw):
            a[2] = zero((NR, L))


    row_pos = (row * NR + lax.broadcasted_iota(jnp.int32, (NR, L), 0)).astype(f32)
    total_rows = NR * n_row
    fu4[...] = 0.25 * (CORIO_F0 + CORIO_BETA * ((row_pos + 0.5) / total_rows - 0.5))
    fv4[...] = 0.25 * (CORIO_F0 + CORIO_BETA * ((row_pos + 1.0) / total_rows - 0.5))

    def to_east(tiles, halo, ts=range(NT)):
        last_lane = lane_p[:tiles[ts[0]].shape[0]] == L - 1
        rolled = {t: halo if t == NT else roll(tiles[t], L - 1) for t in sorted({t + d for t in ts for d in (0, 1)})}
        return {t: jnp.where(last_lane, rolled[t + 1], rolled[t]) for t in ts}

    def to_west(tiles, halo, ts=range(NT)):
        first_lane = lane_p[:tiles[ts[0]].shape[0]] == 0
        rolled = {t: halo if t < 0 else roll(tiles[t], 1) for t in sorted({t + d for t in ts for d in (-1, 0)})}
        return {t: jnp.where(first_lane, rolled[t - 1], rolled[t]) for t in ts}

    def side(f, k, lo=R0, n=NR):
        return pltpu.roll(ha[f // 2, lo:lo + n, :], lax.rem(L - 2 * (SLOT * (f % 2) + k), L), 1)

    def level(b, k, lo=R0, n=NR):
        return [b[t, k, lo:lo + n, :] for t in range(NT)]

    def each_level(fn, unroll):
        def some(i, _):
            base = i * unroll
            for j in range(unroll):
                fn(base + j, base + j - 1 if j else jnp.maximum(base - 1, 0), j % 2)
            return 0

        lax.fori_loop(0, -(-LEV // unroll), some, 0)

    p_scale = BC_GRAVITY / LEV

    def pressure(t, lo, n):
        total = zero((n, L))
        for k in range(LEV):
            density = CONTRACT_S * bs[t, k, lo:lo + n, :] - EXPAND_T * bt[t, k, lo:lo + n, :]
            total = total + density
            bp[t, k, lo:lo + n, :] = p_scale * (total - 0.5 * density)
        bp[t, LEV, lo:lo + n, :] = zero((n, L))

    def own_pressure(t, _):
        pressure(t, R0, NR)
        for k in range(LEV):
            bp[t, k, R0 + NR:R0 + NR + 8, :] = zero((8, L))
        return 0

    lax.fori_loop(0, NT, own_pressure, 0)

    def momentum_down(ts, k, prev, slot):
        scale, carry = tab_s[k], tab_s[SLOT + k]
        u5, v5 = level(bu, k, R0, NR + 8), level(bv, k, R0 - 8, NR + 8)
        u_side = v_side = p_side = jnp.zeros((NR + 8, L), f32)
        if 0 in ts:
            u_side, v_side = side(0, k, R0, NR + 8), side(1, k, R0 - 8, NR + 8)
            p_side = pltpu.roll(rp[...], L - 1 - 2 * k, 1)
        uw, ve = to_west(u5, u_side, ts), to_east(v5, v_side, ts)
        um, vm = [a[:NR] for a in u5], [a[8:] for a in v5]
        ue, vw = to_east(um, u_side[:NR], ts), to_west(vm, v_side[8:], ts)
        pm, pn = level(bp, k), level(bp, k, R0 + 1)
        pe_ = to_east(pm, p_side, ts)
        for t in ts:
            u_sum, v_sum = u5[t] + uw[t], v5[t] + ve[t]
            s1[slot, t] = u_sum
            s2[slot, t] = v_sum
            ub4 = u_sum[:NR] + s1[slot, t, 1:NR + 1, :]
            vb4 = v_sum[8:] + s2[slot, t, 7:NR + 7, :]
            un, us = bu[t, k, R0 + 1:R0 + 1 + NR, :], bu[t, k, R0 - 1:R0 - 1 + NR, :]
            vn, vs = bv[t, k, R0 + 1:R0 + 1 + NR, :], bv[t, k, R0 - 1:R0 - 1 + NR, :]
            u_star = um[t] + vb4 * (fu4[...] - 0.125 * (un - us)) - um[t] * (0.5 * (ue[t] - uw[t][:NR])) + (pm[t] - pe_[t])
            v_star = vm[t] - ub4 * (fv4[...] + 0.125 * (ve[t][8:] - vw[t])) - vm[t] * (0.5 * (vn - vs)) + (pm[t] - pn[t])
            xu[t, k] = scale * u_star + carry * xu[t, prev]
            xv[t, k] = scale * v_star + carry * xv[t, prev]

    arrive(lane_group)
    ha[0] = jnp.where(even, rw[...], roll(re[...], L - 2))
    ha[1] = jnp.where(even, roll(rw[...], L - 1), roll(re[...], L - 1))
    east_ = roll(ha[1, R0:R0 + NR, :], 1)
    density = CONTRACT_S * roll(east_, L // 2) - EXPAND_T * east_
    total = density
    for step in (2, 4, 8, 16, 32):
        total = total + jnp.where(lane >= step, roll(total, step), 0.0)
    rp[...] = p_scale * (total - 0.5 * density)
    arrive(row_group)
    unpack_rows((0, 1))
    each_level(functools.partial(momentum_down, tuple(range(NT))), UNROLL_M)

    arrive(late_group)
    unpack_rows((2, 3))
    last_row = lax.broadcasted_iota(jnp.int32, (8, L), 0) == 7

    def north_pressure(t, _):
        pressure(t, R0 + NR, 8)
        sweep = zero((8, L))
        for k in range(LEV):
            sweep = tab_s[SLOT + k] * sweep - tab_s[k] * bp[t, k, R0 + NR - 7:R0 + NR + 1, :]
            xv[t, k, NR - 8:NR, :] += jnp.where(last_row, sweep, 0.0)
        return 0

    lax.fori_loop(0, NT, north_pressure, 0)

    c_mid, d_mid = level(bu, LEV), level(bv, LEV)
    c_east = to_east(c_mid, side(0, LEV))
    d_east = to_east(d_mid, side(1, LEV))
    c_north, c_south = level(bu, LEV, R0 + 1), level(bu, LEV, R0 - 1)
    d_north = level(bv, LEV, R0 + 1)
    for t in range(NT):
        cu[t] = jnp.minimum(c_mid[t], c_east[t])
        cv[t] = jnp.minimum(c_mid[t], c_north[t])
        hu[t] = 0.5 * (d_mid[t] + d_east[t])
        hv[t] = 0.5 * (d_mid[t] + d_north[t])
        cc_o[t] = c_mid[t]
    c_west0 = jnp.minimum(side(0, LEV), c_mid[0])

    def momentum_up(t, _):
        z = zero((NR, L))
        state = [[z, z, z], [z, z, z]]
        for k in range(LEV - 1, -1, -1):
            link, last_ = tab_s[2 * SLOT + k], tab_s[3 * SLOT + k]
            for q, (sweep, b, count) in enumerate(((xu, bu, cu), (xv, bv, cv))):
                below, sum_x, sum_0 = state[q]
                value = sweep[t, k]
                active = count[t] > float(k)
                solved = jnp.where(count[t] > float(k + 1), value + link * below, jnp.where(active, last_ * value, 0.0))
                sweep[t, k] = solved
                start_ = jnp.where(active, b[t, k, R0:R0 + NR, :], 0.0)
                b[t, k, R0:R0 + NR, :] = start_
                state[q] = [solved, sum_x + solved, sum_0 + start_]
        for q, (h, mean, count) in enumerate(((hu, su, cu), (hv, sv, cv))):
            _, total, start_ = state[q]
            n_active = jnp.maximum(count[t], 1.0)
            mean[t] = total / n_active
            xf[q, t, XO:XO + NR, :] = h[t] * (total - start_) / n_active / TIME_STEP
        c_south = jnp.minimum(bu[t, LEV, 0:8, :], pltpu.roll(bu[t, LEV, R0:R0 + 8, :], 7, 0))
        for k in range(LEV):
            bv[t, k, 0:8, :] = jnp.where(c_south > float(k), bv[t, k, 0:8, :], 0.0)
        return 0

    lax.fori_loop(0, NT, momentum_up, 0)

    first, last = pack_wide(xf, 2)
    fw[...] = first
    fe[...] = last
    start(force_group)

    def tracer_down(k, prev, slot):
        scale, carry = tab_s[4 * SLOT + k], tab_s[5 * SLOT + k]
        kf = lax.convert_element_type(k, f32)
        um, vm, vs = level(bu, k), level(bv, k), level(bv, k, R0 - 1)
        uw0 = jnp.where(c_west0 > kf, side(0, k), 0.0)
        for f, b, sweep in ((2, bt, xt), (3, bs, xs)):
            q = level(b, k)
            q_side = side(f, k)
            qe_ = to_east(q, q_side)
            f_east = [um[t] * (q[t] + qe_[t]) for t in range(NT)]
            f_west = to_west(f_east, uw0 * (q_side + q[0]))
            for t in range(NT):
                f_north = vm[t] * (q[t] + b[t, k, R0 + 1:R0 + 1 + NR, :])
                f_south = vs[t] * (b[t, k, R0 - 1:R0 - 1 + NR, :] + q[t])
                new = q[t] - 0.5 * TIME_STEP * (f_east[t] - f_west[t] + f_north - f_south)
                sweep[t, k] = jnp.where(bu[t, LEV, R0:R0 + NR, :] > kf, scale * new + carry * sweep[t, prev], new)

    each_level(tracer_down, UNROLL_T)

    arrive(wide_group)
    drain(wide_group)
    arrive(force_group)

    def unpack_wide(b, from_e, from_w, n_fields):
        for f in range(n_fields):
            for seg in range(3):
                b[f, NT, 8 + NR * seg:8 + NR * seg + NR, :] = jnp.where(lane < L // 2, roll(from_e[seg], (L - 32 * f) % L), roll(from_w[seg], (96 - 32 * f) % L))

    unpack_wide(x, we, ww, 4)
    unpack_wide(xf, fre, frw, 2)
    dt_fast = TIME_STEP / n_sub
    XT = NT + 1

    def ring_east(tiles, last_lane):
        rolled = [roll(a, L - 1) for a in tiles]
        return [jnp.where(last_lane, rolled[(t + 1) % XT], rolled[t]) for t in range(XT)]

    def ring_west(tiles, first_lane):
        rolled = [roll(a, 1) for a in tiles]
        return [jnp.where(first_lane, rolled[(t - 1) % XT], rolled[t]) for t in range(XT)]

    for seg in range(3):
        lo = 8 + NR * seg
        pos = (row * NR + NR * (seg - 1) + lax.broadcasted_iota(jnp.int32, (NR, L), 0)).astype(f32)
        f_u = CORIO_F0 + CORIO_BETA * ((pos + 0.5) / total_rows - 0.5)
        f_v = CORIO_F0 + CORIO_BETA * ((pos + 1.0) / total_rows - 0.5)
        d = [x[3, t, lo:lo + NR, :] for t in range(XT)]
        d_e = ring_east(d, lane == L - 1)
        for t in range(XT):
            d_n = x[3, t, lo + 1:lo + 1 + NR, :]
            wet = jnp.where((d[t] > 0.0) & (d_e[t] > 0.0), 1.0, 0.0)
            cm[t, lo:lo + NR, :] = wet
            ca[t, lo:lo + NR, :] = (0.25 * dt_fast) * f_u * wet
            cb[t, lo:lo + NR, :] = (dt_fast * GRAVITY * 0.5) * (d[t] + d_e[t]) * wet
            cc[t, lo:lo + NR, :] = dt_fast * xf[0, t, lo:lo + NR, :] * wet
            wet = jnp.where((d[t] > 0.0) & (d_n > 0.0), 1.0, 0.0)
            cn[t, lo:lo + NR, :] = wet
            cd[t, lo:lo + NR, :] = (0.25 * dt_fast) * f_v * wet
            cg[t, lo:lo + NR, :] = (dt_fast * GRAVITY * 0.5) * (d[t] + d_n) * wet
            ch[t, lo:lo + NR, :] = dt_fast * xf[1, t, lo:lo + NR, :] * wet

    for t in range(NT):
        au[t] = zero((NR, L))
        av[t] = zero((NR, L))

    def subcycle(side_rows, masked, n, _):
        weight = w_s[n]
        parts = ((XO - side_rows, side_rows), (XO, NR), (XO + NR, side_rows))
        for r, chunk in parts:
            first_lane = lane[:chunk] == 0
            u_t = [x[1, t, r:r + chunk, :] for t in range(XT)]
            u_w = ring_west(u_t, first_lane)
            for t in range(XT):
                v_t, v_s = x[2, t, r:r + chunk, :], x[2, t, r - 1:r - 1 + chunk, :]
                x[0, t, r:r + chunk, :] = x[0, t, r:r + chunk, :] - dt_fast * ((u_t[t] - u_w[t]) + (v_t - v_s))
                tt[t, r:r + chunk, :] = u_t[t] + u_w[t]
        for r, chunk in parts[::-1]:
            last_lane = lane[:chunk] == L - 1
            e_t = [x[0, t, r:r + chunk, :] for t in range(XT)]
            e_e = ring_east(e_t, last_lane)
            v_t = [x[2, t, r:r + chunk, :] for t in range(XT)]
            s_t = [v_t[t] + x[2, t, r - 1:r - 1 + chunk, :] for t in range(XT)]
            s_e = ring_east(s_t, last_lane)
            for t in range(XT):
                at = (t, slice(r, r + chunk))
                up = (t, slice(r + 1, r + 1 + chunk))
                e_n = x[0, t, r + 1:r + 1 + chunk, :]
                u_old = x[1, t, r:r + chunk, :] if masked else cm[at] * x[1, t, r:r + chunk, :]
                v_old = v_t[t] if masked else cn[at] * v_t[t]
                u_new = u_old + ca[at] * (s_t[t] + s_e[t]) + cc[at] - cb[at] * (e_e[t] - e_t[t])
                v_new = v_old - cd[at] * (tt[at] + tt[up]) + ch[at] - cg[at] * (e_n - e_t[t])
                x[1, t, r:r + chunk, :] = u_new
                x[2, t, r:r + chunk, :] = v_new
                if r == XO and t < NT:
                    au[t] += weight * u_new
                    av[t] += weight * v_new
        return 0

    done = 0
    for tiles in (4, 3, 2, 1):
        until = n_sub - 8 * (tiles - 1)
        stretch = functools.partial(subcycle, 8 * tiles)
        if done == 0:
            stretch(False, 0, 0)
            done = 1
        lax.fori_loop(done, until, functools.partial(stretch, True), 0)
        done = until

    for t in range(NT):
        eta_o[t] = x[0, t, XO:XO + NR, :]
        tu_o[t] = x[1, t, XO:XO + NR, :]
        tv_o[t] = x[2, t, XO:XO + NR, :]
        gu_o[t] = au[t] / hu[t] - su[t]
        gv_o[t] = av[t] / hv[t] - sv[t]

    for group in (row_group, late_group, lane_group, force_group):
        drain(group)


def final_kernel(tab_s, xu, xv, xt, xs, gu, gv, cu, cv, cc, eta, tu, tv, eta_h, tu_h, tv_h, u_h, v_h, t_h, s_h, flat_b, u_b, v_b, t_b, s_b, sem):
    xu, xv, xt, xs = [a.at[:, 0:SLOT, 0:NR, :] for a in (xu, xv, xt, xs)]
    gu, gv, cu, cv, cc, eta, tu, tv = [a.at[:, 0:NR, :] for a in (gu, gv, cu, cv, cc, eta, tu, tv)]
    stores = []
    for i, (a, o) in enumerate(((eta, eta_h), (tu, tu_h), (tv, tv_h))):
        for t in range(NT):
            flat_b[i, :, L * t:L * t + L] = a[t]
        stores.append(pltpu.make_async_copy(flat_b.at[i], o, sem.at[4, i]))
        stores[-1].start()

    below = [[jnp.zeros((NR, L), f32)] * NT for _ in range(2)]
    top = LEV
    for k in range(LEV - 1, -1, -1):
        link, last = tab_s[6 * SLOT + k], tab_s[7 * SLOT + k]
        for t in range(NT):
            cols = slice(L * t, L * t + L)
            u_b[k, :, cols] = jnp.where(cu[t] > float(k), xu[t, k] + gu[t], 0.0)
            v_b[k, :, cols] = jnp.where(cv[t] > float(k), xv[t, k] + gv[t], 0.0)
            for q, (sweep, b) in enumerate(((xt, t_b), (xs, s_b))):
                value = sweep[t, k]
                solved = jnp.where(cc[t] > float(k + 1), value + link * below[q][t], jnp.where(cc[t] > float(k), last * value, value))
                below[q][t] = solved
                b[k, :, cols] = solved
        if k in GROUPS:
            for i, (b, o) in enumerate(((u_b, u_h), (v_b, v_h), (t_b, t_h), (s_b, s_h))):
                stores.append(pltpu.make_async_copy(b.at[k:top], o.at[k:top], sem.at[i, GROUPS.index(k)]))
                stores[-1].start()
            top = k
    for cp in stores:
        cp.wait()


def solution(mesh):
    n_col = mesh.shape['col']
    n_row = mesh.shape['row']

    def step(vel_u, vel_v, value_a11, salinity, surf_eta, trans_u, trans_v, bottom_depth, level_count, avg_weights):
        n_sub = avg_weights.shape[0]
        table = jnp.asarray(solve_table(LEV))
        hbm = pl.BlockSpec(memory_space=pltpu.HBM)
        vmem = pl.BlockSpec(memory_space=pltpu.VMEM)
        smem = pl.BlockSpec(memory_space=pltpu.SMEM)
        V = pltpu.VMEM
        tile = V((NT, RA, L), f32)
        sweep = V((NT, KA, RA, L), f32)
        wide = (NT + 1, XR, L)
        scratch = ([V((NT, KA, PR, L), f32)] * 5 + [V((NT, NR, L), jnp.int32), V((NR, L), f32)]
                   + [V((2, NT, NR + 8, L), f32)] * 2 + [V((4, NT, SLOT, L), f32)] * 4 + [V((NR, L), f32)] * 2 + [V((PR, L), f32)] * 2 + [V((2, PR, L), f32)]
                   + [V((4,) + wide, f32), V((2,) + wide, f32)] + [V((NR, L), f32)] * 2 + [V((3, NR, L), f32)] * 2
                   + [V((NR, L), f32)] * 2 + [V((3, NR, L), f32)] * 2
                   + [V((NR, L), f32)] * 2 + [tile] * 4
                   + [V(wide, f32)] * 9 + [tile] * 2
                   + [pltpu.SMEM((n_sub,), f32), pltpu.SMEM((8 * SLOT,), f32)]
                   + [pltpu.SemaphoreType.DMA((40,)), pltpu.SemaphoreType.DMA((64,)), pltpu.SemaphoreType.DMA((64,))])
        outs = pl.pallas_call(
            functools.partial(ocean_kernel, tuple(mesh.axis_names), n_col, n_row, n_sub),
            out_shape=[tile] * 8 + [sweep] * 4,
            in_specs=[hbm] * 11,
            out_specs=[vmem] * 12,
            scratch_shapes=scratch,
            compiler_params=pltpu.CompilerParams(collective_id=0, has_side_effects=True, vmem_limit_bytes=40 * 1024 * 1024),
        )(*[pltpu.with_memory_space_constraint(a, pltpu.HBM) for a in (vel_u, vel_v, value_a11, salinity, surf_eta, trans_u, trans_v, bottom_depth, level_count, avg_weights, table)])
        eta, tu, tv, gu, gv, cu, cv, cc, xu, xv, xt, xs = [pltpu.with_memory_space_constraint(o, pltpu.VMEM) for o in outs]

        cube = jax.ShapeDtypeStruct((LEV, NR, NC), f32)
        flat = jax.ShapeDtypeStruct((NR, NC), f32)
        return tuple(pl.pallas_call(
            final_kernel,
            out_shape=[flat] * 3 + [cube] * 4,
            in_specs=[smem] + [vmem] * 12,
            out_specs=[hbm] * 7,
            scratch_shapes=[V((3, NR, NC), f32)] + [V((LEV, NR, NC), f32)] * 4 + [pltpu.SemaphoreType.DMA((5, len(GROUPS)))],
            compiler_params=pltpu.CompilerParams(vmem_limit_bytes=24 * 1024 * 1024),
        )(table, xu, xv, xt, xs, gu, gv, cu, cv, cc, eta, tu, tv))

    cube = P(None, 'row', 'col')
    flat = P('row', 'col')
    return jax.shard_map(step, mesh=mesh, in_specs=(cube, cube, cube, cube, flat, flat, flat, flat, flat, P()), out_specs=(flat, flat, flat, cube, cube, cube, cube), check_vma=False)
```

```python
import functools

import jax
import jax.numpy as jnp
import numpy as np
from jax import lax
from jax.experimental import pallas as pl
from jax.experimental.pallas import tpu as pltpu
from jax.sharding import PartitionSpec as P

TIME_STEP = 1.0
GRAVITY = 16.0
BC_GRAVITY = 4.0
EXPAND_T = 0.2
CONTRACT_S = 0.6
CORIO_F0 = 0.4
CORIO_BETA = 0.4
VISC_R = 2.0
DIFF_R = 0.5

LEV = 31
SLOT = 32
NR = 32
NC = 512
NT = 4
L = 128
R0 = 8
PR = 56
KA = SLOT + 1
RA = NR + 8
XR = 120
XO = 40
MESH = pl.DeviceIdType.MESH
f32 = jnp.float32
UNROLL_M = 8
UNROLL_T = 4
GROUPS = (28, 24, 20, 16, 12, 8, 4, 2, 0)


def solve_table(n_levels):
    rows = []
    for s in (VISC_R, DIFF_R):
        scale, carry, link, last = np.zeros((4, SLOT))
        ratio = 0.0
        for k in range(n_levels):
            low = s if k else 0.0
            full = 1.0 + low + s - low * ratio
            end = 1.0 + low - low * ratio
            scale[k], carry[k], link[k], last[k] = 1.0 / full, low / full, s / full, full / end
            ratio = s / full
        rows += [scale, carry, link, last]
    return np.concatenate(rows).astype(np.float32)


def ocean_kernel(axes, n_col, n_row, n_sub, *refs):
    (u_h, v_h, t_h, s_h, eta_h, tu_h, tv_h, dep_h, cnt_h, w_h, tab_h,
     eta_o, tu_o, tv_o, gu_o, gv_o, cu, cv, cc_o, xu, xv, xt, xs,
     bu, bv, bt, bs, bp, cnt_i, rp, s1, s2,
     pn, ps, rn, rs, pw, pe, rw, re, ha, x, xf, qw, qe, we, ww, fw, fe, fre, frw,
     fu4, fv4, hu, hv, su, sv,
     ca, cb, cc, cd, cg, ch, cm, cn, tt, au, av,
     w_s, tab_s, lsem, ssem, rsem) = refs
    xu, xv, xt, xs = [a.at[:, 0:SLOT, 0:NR, :] for a in (xu, xv, xt, xs)]
    eta_o, tu_o, tv_o, gu_o, gv_o, cu, cv, cc_o, hu, hv, su, sv, au, av = [a.at[:, 0:NR, :] for a in (eta_o, tu_o, tv_o, gu_o, gv_o, cu, cv, cc_o, hu, hv, su, sv, au, av)]
    col = lax.axis_index('col')
    row = lax.axis_index('row')
    east = lax.rem(col + 1, n_col)
    west = lax.rem(col + n_col - 1, n_col)
    has_s = row > 0
    has_n = row < n_row - 1

    def dev(c, r):
        at = {'col': c, 'row': r}
        return tuple(at[name] for name in axes)

    bufs = (bu, bv, bt, bs)
    barrier = pltpu.get_barrier_semaphore()

    def signal(c, r):
        pl.semaphore_signal(barrier, inc=1, device_id=dev(c, r), device_id_type=MESH)

    signal(west, row)
    signal(east, row)

    @pl.when(has_s)
    def _():
        for c in (west, col, east):
            signal(c, row - 1)

    @pl.when(has_n)
    def _():
        for c in (west, col, east):
            signal(c, row + 1)

    zero = functools.partial(jnp.zeros, dtype=f32)

    loads = []
    for f, (src, dst) in enumerate(zip((u_h, v_h, t_h, s_h), bufs)):
        for t in range(NT):
            loads.append(pltpu.make_async_copy(src.at[:, :, L * t:L * t + L], dst.at[t, 0:LEV, R0:R0 + NR, :], lsem.at[len(loads)]))
    flat_loads = []
    for f, src in enumerate((eta_h, tu_h, tv_h)):
        for t in range(NT):
            flat_loads.append(pltpu.make_async_copy(src.at[:, L * t:L * t + L], x.at[f, t, XO:XO + NR, :], lsem.at[len(loads) + len(flat_loads)]))
    for t in range(NT):
        flat_loads.append(pltpu.make_async_copy(dep_h.at[:, L * t:L * t + L], bv.at[t, LEV, R0:R0 + NR, :], lsem.at[len(loads) + len(flat_loads)]))
    for t in range(NT):
        flat_loads.append(pltpu.make_async_copy(cnt_h.at[:, L * t:L * t + L], cnt_i.at[t], lsem.at[len(loads) + len(flat_loads)]))
    scalar_loads = [pltpu.make_async_copy(w_h, w_s, lsem.at[36]), pltpu.make_async_copy(tab_h, tab_s, lsem.at[37])]
    edge_loads = [loads[NT * f + t] for f in range(4) for t in (0, NT - 1)]
    mid_loads = [loads[NT * f + t] for f in range(4) for t in range(1, NT - 1)]
    for cp in flat_loads[3 * NT:] + edge_loads + mid_loads + flat_loads[:3 * NT] + scalar_loads:
        cp.start()

    n_copies = 0

    def remote(src, dst, c, r, sends, receives):
        nonlocal n_copies
        i = n_copies
        n_copies += 1
        return (pltpu.make_async_remote_copy(src, dst, ssem.at[i], rsem.at[i], device_id=dev(c, r), device_id_type=MESH), sends, receives)

    def maybe(cond, fn):
        if cond is None:
            fn()
        else:
            pl.when(cond)(fn)

    def start(group):
        for cp, sends, _ in group:
            maybe(sends, cp.start)

    def arrive(group):
        for cp, _, receives in group:
            maybe(receives, cp.wait_recv)

    def drain(group):
        for cp, sends, _ in group:
            maybe(sends, cp.wait_send)

    def rows_of(fields):
        return [remote(pn.at[fields], rs.at[fields], col, row + 1, has_n, has_s),
                remote(ps.at[fields], rn.at[fields], col, row - 1, has_s, has_n)]

    def level_rows(b, k, r):
        return b.reshape(NT, KA * PR, L), pl.ds(k * PR + r, 8, stride=PR)

    def pack_rows(fields):
        for f in fields:
            for t in range(NT):
                for k in range(0, SLOT, 8):
                    for to, r in ((pn, R0 + NR - 1), (ps, R0)):
                        flat, at = level_rows(bufs[f], k, r)
                        to[f, t, k:k + 8, :] = flat[t, at, :]

    def unpack_rows(fields):
        for f in fields:
            for t in range(NT):
                for k in range(0, SLOT, 8):
                    for to, r in ((rs, R0 - 1), (rn, R0 + NR)):
                        flat, at = level_rows(bufs[f], k, r)
                        flat[t, at, :] = to[f, t, k:k + 8, :]

    def wide_of(b, lanes_w, lanes_e, from_e, from_w):
        own = b.at[:, 0:NT, XO:XO + NR, :]
        return [remote(own, b.at[:, 0:NT, 8:XO, :], col, row + 1, has_n, has_s),
                remote(own, b.at[:, 0:NT, XO + NR:XO + 2 * NR, :], col, row - 1, has_s, has_n),
                remote(lanes_w, from_e.at[1], west, row, None, None),
                remote(lanes_e, from_w.at[1], east, row, None, None),
                remote(lanes_w, from_e.at[2], west, row - 1, has_s, has_n),
                remote(lanes_e, from_w.at[2], east, row - 1, has_s, has_n),
                remote(lanes_w, from_e.at[0], west, row + 1, has_n, has_s),
                remote(lanes_e, from_w.at[0], east, row + 1, has_n, has_s)]

    row_group, late_group = rows_of(slice(0, 2)), rows_of(slice(2, 4))
    lane_group = [remote(pw, re.at[R0:R0 + NR, :], west, row, None, None),
                  remote(pe, rw.at[R0:R0 + NR, :], east, row, None, None),
                  remote(pe.at[0:1, :], rw.at[R0 + NR:R0 + NR + 1, :], east, row - 1, has_s, has_n),
                  remote(pw.at[NR - 1:NR, :], re.at[R0 - 1:R0, :], west, row + 1, has_n, has_s)]
    wide_group = wide_of(x, qw, qe, we, ww)
    force_group = wide_of(xf, fw, fe, fre, frw)

    edge = jnp.logical_or(row == 0, row == n_row - 1)

    @pl.when(edge)
    def _():
        pl.semaphore_wait(barrier, 5)

    @pl.when(jnp.logical_not(edge))
    def _():
        pl.semaphore_wait(barrier, 8)

    lane_p = lax.broadcasted_iota(jnp.int32, (PR, L), 1)
    lane = lane_p[:NR]

    for t in range(NT):
        bt[t, LEV, R0:R0 + NR, :] = zero((NR, L))
        bs[t, LEV, R0:R0 + NR, :] = zero((NR, L))
    for cp in flat_loads[3 * NT:]:
        cp.wait()
    for t in range(NT):
        count = cnt_i[t].astype(f32)
        bu[t, LEV, R0:R0 + NR, :] = count
        x[3, t, XO:XO + NR, :] = jnp.where(count > 0.0, bv[t, LEV, R0:R0 + NR, :], 0.0)

    def roll(a, shift):
        return pltpu.roll(a, shift, 1) if not (isinstance(shift, int) and shift % L == 0) else a

    pair = lax.shift_right_logical(lane, 1)
    packed = [zero((NR, L))] * 2
    for f, b in enumerate(bufs):
        edge_loads[2 * f].wait()
        edge_loads[2 * f + 1].wait()
        for k in range(SLOT):
            p = SLOT * (f % 2) + k
            both = jnp.where(lane == 0, b[0, k, R0:R0 + NR, :], b[NT - 1, k, R0:R0 + NR, :])
            packed[f // 2] = jnp.where(pair == p, roll(both, (2 * p + 1) % L), packed[f // 2])
    even = lax.rem(lane_p, 2) == 0
    pw[...] = jnp.where(even[:NR], roll(packed[1], L - 1), packed[0])
    pe[...] = jnp.where(even[:NR], packed[0], roll(packed[1], 1))
    start(lane_group)
    for cp in mid_loads:
        cp.wait()
    pack_rows((0, 1))
    start(row_group)
    pack_rows((2, 3))
    start(late_group)

    def pack_wide(b, n_fields):
        first = last = zero((NR, L))
        for f in range(n_fields):
            mine = (lane >= 32 * f) & (lane < 32 * f + 32)
            first = jnp.where(mine, roll(b[f, 0, XO:XO + NR, :], 32 * f), first)
            last = jnp.where(mine, roll(b[f, NT - 1, XO:XO + NR, :], (32 * f + 32) % L), last)
        return first, last

    for cp in flat_loads[:3 * NT]:
        cp.wait()
    first, last = pack_wide(x, 4)
    qw[...] = first
    qe[...] = last
    start(wide_group)
    for cp in scalar_loads:
        cp.wait()

    for f in range(4):
        for t in range(NT + 1):
            x[f, t, 0:8, :] = zero((8, L))
            x[f, t, XR - 16:XR, :] = zero((16, L))
    for t in range(NT + 1):
        tt[t, XR - 16:XR, :] = zero((16, L))
    for t in range(NT):
        for a in (xu, xv, xt, xs):
            a[t, 0] = zero((NR, L))

    @pl.when(jnp.logical_not(has_s))
    def _():
        rs[...] = zero((4, NT, SLOT, L))
        re[R0 - 8:R0, :] = zero((8, L))
        x[:, 0:NT, 8:XO, :] = zero((4, NT, NR, L))
        xf[:, 0:NT, 8:XO, :] = zero((2, NT, NR, L))
        for a in (we, ww, fre, frw):
            a[0] = zero((NR, L))

    @pl.when(jnp.logical_not(has_n))
    def _():
        rn[...] = zero((4, NT, SLOT, L))
        rw[R0 + NR:R0 + NR + 8, :] = zero((8, L))
        x[:, 0:NT, XO + NR:XO + 2 * NR, :] = zero((4, NT, NR, L))
        xf[:, 0:NT, XO + NR:XO + 2 * NR, :] = zero((2, NT, NR, L))
        for a in (we, ww, fre, frw):
            a[2] = zero((NR, L))


    row_pos = (row * NR + lax.broadcasted_iota(jnp.int32, (NR, L), 0)).astype(f32)
    total_rows = NR * n_row
    fu4[...] = 0.25 * (CORIO_F0 + CORIO_BETA * ((row_pos + 0.5) / total_rows - 0.5))
    fv4[...] = 0.25 * (CORIO_F0 + CORIO_BETA * ((row_pos + 1.0) / total_rows - 0.5))

    def to_east(tiles, halo, ts=range(NT)):
        last_lane = lane_p[:tiles[ts[0]].shape[0]] == L - 1
        rolled = {t: halo if t == NT else roll(tiles[t], L - 1) for t in sorted({t + d for t in ts for d in (0, 1)})}
        return {t: jnp.where(last_lane, rolled[t + 1], rolled[t]) for t in ts}

    def to_west(tiles, halo, ts=range(NT)):
        first_lane = lane_p[:tiles[ts[0]].shape[0]] == 0
        rolled = {t: halo if t < 0 else roll(tiles[t], 1) for t in sorted({t + d for t in ts for d in (-1, 0)})}
        return {t: jnp.where(first_lane, rolled[t - 1], rolled[t]) for t in ts}

    def side(f, k, lo=R0, n=NR):
        return pltpu.roll(ha[f // 2, lo:lo + n, :], lax.rem(L - 2 * (SLOT * (f % 2) + k), L), 1)

    def level(b, k, lo=R0, n=NR):
        return [b[t, k, lo:lo + n, :] for t in range(NT)]

    def each_level(fn, unroll):
        def some(i, _):
            base = i * unroll
            for j in range(unroll):
                fn(base + j, base + j - 1 if j else jnp.maximum(base - 1, 0), j % 2)
            return 0

        lax.fori_loop(0, -(-LEV // unroll), some, 0)

    p_scale = BC_GRAVITY / LEV

    def pressure(t, lo, n):
        total = zero((n, L))
        for k in range(LEV):
            density = CONTRACT_S * bs[t, k, lo:lo + n, :] - EXPAND_T * bt[t, k, lo:lo + n, :]
            total = total + density
            bp[t, k, lo:lo + n, :] = p_scale * (total - 0.5 * density)
        bp[t, LEV, lo:lo + n, :] = zero((n, L))

    def own_pressure(t, _):
        pressure(t, R0, NR)
        for k in range(LEV):
            bp[t, k, R0 + NR:R0 + NR + 8, :] = zero((8, L))
        return 0

    lax.fori_loop(0, NT, own_pressure, 0)

    def momentum_down(ts, k, prev, slot):
        scale, carry = tab_s[k], tab_s[SLOT + k]
        u5, v5 = level(bu, k, R0, NR + 8), level(bv, k, R0 - 8, NR + 8)
        u_side = v_side = p_side = jnp.zeros((NR + 8, L), f32)
        if 0 in ts:
            u_side, v_side = side(0, k, R0, NR + 8), side(1, k, R0 - 8, NR + 8)
            p_side = pltpu.roll(rp[...], L - 1 - 2 * k, 1)
        uw, ve = to_west(u5, u_side, ts), to_east(v5, v_side, ts)
        um, vm = [a[:NR] for a in u5], [a[8:] for a in v5]
        ue, vw = to_east(um, u_side[:NR], ts), to_west(vm, v_side[8:], ts)
        pm, pn = level(bp, k), level(bp, k, R0 + 1)
        pe_ = to_east(pm, p_side, ts)
        for t in ts:
            u_sum, v_sum = u5[t] + uw[t], v5[t] + ve[t]
            s1[slot, t] = u_sum
            s2[slot, t] = v_sum
            ub4 = u_sum[:NR] + s1[slot, t, 1:NR + 1, :]
            vb4 = v_sum[8:] + s2[slot, t, 7:NR + 7, :]
            un, us = bu[t, k, R0 + 1:R0 + 1 + NR, :], bu[t, k, R0 - 1:R0 - 1 + NR, :]
            vn, vs = bv[t, k, R0 + 1:R0 + 1 + NR, :], bv[t, k, R0 - 1:R0 - 1 + NR, :]
            u_star = um[t] + vb4 * (fu4[...] - 0.125 * (un - us)) - um[t] * (0.5 * (ue[t] - uw[t][:NR])) + (pm[t] - pe_[t])
            v_star = vm[t] - ub4 * (fv4[...] + 0.125 * (ve[t][8:] - vw[t])) - vm[t] * (0.5 * (vn - vs)) + (pm[t] - pn[t])
            xu[t, k] = scale * u_star + carry * xu[t, prev]
            xv[t, k] = scale * v_star + carry * xv[t, prev]

    arrive(lane_group)
    ha[0] = jnp.where(even, rw[...], roll(re[...], L - 2))
    ha[1] = jnp.where(even, roll(rw[...], L - 1), roll(re[...], L - 1))
    east_ = roll(ha[1, R0:R0 + NR, :], 1)
    density = CONTRACT_S * roll(east_, L // 2) - EXPAND_T * east_
    total = density
    for step in (2, 4, 8, 16, 32):
        total = total + jnp.where(lane >= step, roll(total, step), 0.0)
    rp[...] = p_scale * (total - 0.5 * density)
    arrive(row_group)
    unpack_rows((0, 1))
    each_level(functools.partial(momentum_down, tuple(range(NT))), UNROLL_M)

    arrive(late_group)
    unpack_rows((2, 3))
    last_row = lax.broadcasted_iota(jnp.int32, (8, L), 0) == 7

    def north_pressure(t, _):
        pressure(t, R0 + NR, 8)
        sweep = zero((8, L))
        for k in range(LEV):
            sweep = tab_s[SLOT + k] * sweep - tab_s[k] * bp[t, k, R0 + NR - 7:R0 + NR + 1, :]
            xv[t, k, NR - 8:NR, :] += jnp.where(last_row, sweep, 0.0)
        return 0

    lax.fori_loop(0, NT, north_pressure, 0)

    c_mid, d_mid = level(bu, LEV), level(bv, LEV)
    c_east = to_east(c_mid, side(0, LEV))
    d_east = to_east(d_mid, side(1, LEV))
    c_north, c_south = level(bu, LEV, R0 + 1), level(bu, LEV, R0 - 1)
    d_north = level(bv, LEV, R0 + 1)
    for t in range(NT):
        cu[t] = jnp.minimum(c_mid[t], c_east[t])
        cv[t] = jnp.minimum(c_mid[t], c_north[t])
        hu[t] = 0.5 * (d_mid[t] + d_east[t])
        hv[t] = 0.5 * (d_mid[t] + d_north[t])
        cc_o[t] = c_mid[t]
    c_west0 = jnp.minimum(side(0, LEV), c_mid[0])

    def momentum_up(t, _):
        z = zero((NR, L))
        state = [[z, z, z], [z, z, z]]
        for k in range(LEV - 1, -1, -1):
            link, last_ = tab_s[2 * SLOT + k], tab_s[3 * SLOT + k]
            for q, (sweep, b, count) in enumerate(((xu, bu, cu), (xv, bv, cv))):
                below, sum_x, sum_0 = state[q]
                value = sweep[t, k]
                active = count[t] > float(k)
                solved = jnp.where(count[t] > float(k + 1), value + link * below, jnp.where(active, last_ * value, 0.0))
                sweep[t, k] = solved
                start_ = jnp.where(active, b[t, k, R0:R0 + NR, :], 0.0)
                b[t, k, R0:R0 + NR, :] = start_
                state[q] = [solved, sum_x + solved, sum_0 + start_]
        for q, (h, mean, count) in enumerate(((hu, su, cu), (hv, sv, cv))):
            _, total, start_ = state[q]
            n_active = jnp.maximum(count[t], 1.0)
            mean[t] = total / n_active
            xf[q, t, XO:XO + NR, :] = h[t] * (total - start_) / n_active / TIME_STEP
        c_south = jnp.minimum(bu[t, LEV, 0:8, :], pltpu.roll(bu[t, LEV, R0:R0 + 8, :], 7, 0))
        for k in range(LEV):
            bv[t, k, 0:8, :] = jnp.where(c_south > float(k), bv[t, k, 0:8, :], 0.0)
        return 0

    lax.fori_loop(0, NT, momentum_up, 0)

    first, last = pack_wide(xf, 2)
    fw[...] = first
    fe[...] = last
    start(force_group)

    def tracer_down(k, prev, slot):
        scale, carry = tab_s[4 * SLOT + k], tab_s[5 * SLOT + k]
        kf = lax.convert_element_type(k, f32)
        um, vm, vs = level(bu, k), level(bv, k), level(bv, k, R0 - 1)
        uw0 = jnp.where(c_west0 > kf, side(0, k), 0.0)
        for f, b, sweep in ((2, bt, xt), (3, bs, xs)):
            q = level(b, k)
            q_side = side(f, k)
            qe_ = to_east(q, q_side)
            f_east = [um[t] * (q[t] + qe_[t]) for t in range(NT)]
            f_west = to_west(f_east, uw0 * (q_side + q[0]))
            for t in range(NT):
                f_north = vm[t] * (q[t] + b[t, k, R0 + 1:R0 + 1 + NR, :])
                f_south = vs[t] * (b[t, k, R0 - 1:R0 - 1 + NR, :] + q[t])
                new = q[t] - 0.5 * TIME_STEP * (f_east[t] - f_west[t] + f_north - f_south)
                sweep[t, k] = jnp.where(bu[t, LEV, R0:R0 + NR, :] > kf, scale * new + carry * sweep[t, prev], new)

    each_level(tracer_down, UNROLL_T)

    arrive(wide_group)
    drain(wide_group)
    arrive(force_group)

    def unpack_wide(b, from_e, from_w, n_fields):
        for f in range(n_fields):
            for seg in range(3):
                b[f, NT, 8 + NR * seg:8 + NR * seg + NR, :] = jnp.where(lane < L // 2, roll(from_e[seg], (L - 32 * f) % L), roll(from_w[seg], (96 - 32 * f) % L))

    unpack_wide(x, we, ww, 4)
    unpack_wide(xf, fre, frw, 2)
    dt_fast = TIME_STEP / n_sub
    XT = NT + 1

    def ring_east(tiles, last_lane):
        rolled = [roll(a, L - 1) for a in tiles]
        return [jnp.where(last_lane, rolled[(t + 1) % XT], rolled[t]) for t in range(XT)]

    def ring_west(tiles, first_lane):
        rolled = [roll(a, 1) for a in tiles]
        return [jnp.where(first_lane, rolled[(t - 1) % XT], rolled[t]) for t in range(XT)]

    for seg in range(3):
        lo = 8 + NR * seg
        pos = (row * NR + NR * (seg - 1) + lax.broadcasted_iota(jnp.int32, (NR, L), 0)).astype(f32)
        f_u = CORIO_F0 + CORIO_BETA * ((pos + 0.5) / total_rows - 0.5)
        f_v = CORIO_F0 + CORIO_BETA * ((pos + 1.0) / total_rows - 0.5)
        d = [x[3, t, lo:lo + NR, :] for t in range(XT)]
        d_e = ring_east(d, lane == L - 1)
        for t in range(XT):
            d_n = x[3, t, lo + 1:lo + 1 + NR, :]
            wet = jnp.where((d[t] > 0.0) & (d_e[t] > 0.0), 1.0, 0.0)
            cm[t, lo:lo + NR, :] = wet
            ca[t, lo:lo + NR, :] = (0.25 * dt_fast) * f_u * wet
            cb[t, lo:lo + NR, :] = (dt_fast * GRAVITY * 0.5) * (d[t] + d_e[t]) * wet
            cc[t, lo:lo + NR, :] = dt_fast * xf[0, t, lo:lo + NR, :] * wet
            wet = jnp.where((d[t] > 0.0) & (d_n > 0.0), 1.0, 0.0)
            cn[t, lo:lo + NR, :] = wet
            cd[t, lo:lo + NR, :] = (0.25 * dt_fast) * f_v * wet
            cg[t, lo:lo + NR, :] = (dt_fast * GRAVITY * 0.5) * (d[t] + d_n) * wet
            ch[t, lo:lo + NR, :] = dt_fast * xf[1, t, lo:lo + NR, :] * wet

    for t in range(NT):
        au[t] = zero((NR, L))
        av[t] = zero((NR, L))

    def subcycle(side_rows, masked, n, _):
        weight = w_s[n]
        parts = ((XO - side_rows, side_rows), (XO, NR), (XO + NR, side_rows))
        for r, chunk in parts:
            first_lane = lane[:chunk] == 0
            u_t = [x[1, t, r:r + chunk, :] for t in range(XT)]
            u_w = ring_west(u_t, first_lane)
            for t in range(XT):
                v_t, v_s = x[2, t, r:r + chunk, :], x[2, t, r - 1:r - 1 + chunk, :]
                x[0, t, r:r + chunk, :] = x[0, t, r:r + chunk, :] - dt_fast * ((u_t[t] - u_w[t]) + (v_t - v_s))
                tt[t, r:r + chunk, :] = u_t[t] + u_w[t]
        for r, chunk in parts[::-1]:
            last_lane = lane[:chunk] == L - 1
            e_t = [x[0, t, r:r + chunk, :] for t in range(XT)]
            e_e = ring_east(e_t, last_lane)
            v_t = [x[2, t, r:r + chunk, :] for t in range(XT)]
            s_t = [v_t[t] + x[2, t, r - 1:r - 1 + chunk, :] for t in range(XT)]
            s_e = ring_east(s_t, last_lane)
            for t in range(XT):
                at = (t, slice(r, r + chunk))
                up = (t, slice(r + 1, r + 1 + chunk))
                e_n = x[0, t, r + 1:r + 1 + chunk, :]
                u_old = x[1, t, r:r + chunk, :] if masked else cm[at] * x[1, t, r:r + chunk, :]
                v_old = v_t[t] if masked else cn[at] * v_t[t]
                u_new = u_old + ca[at] * (s_t[t] + s_e[t]) + cc[at] - cb[at] * (e_e[t] - e_t[t])
                v_new = v_old - cd[at] * (tt[at] + tt[up]) + ch[at] - cg[at] * (e_n - e_t[t])
                x[1, t, r:r + chunk, :] = u_new
                x[2, t, r:r + chunk, :] = v_new
                if r == XO and t < NT:
                    au[t] += weight * u_new
                    av[t] += weight * v_new
        return 0

    done = 0
    for tiles in (4, 3, 2, 1):
        until = n_sub - 8 * (tiles - 1)
        stretch = functools.partial(subcycle, 8 * tiles)
        if done == 0:
            stretch(False, 0, 0)
            stretch(True, 1, 0)
            done = 2

        def two(i, _, stretch=stretch, done=done):
            stretch(True, done + 2 * i, 0)
            stretch(True, done + 2 * i + 1, 0)
            return 0

        lax.fori_loop(0, (until - done) // 2, two, 0)
        for n in range(done + (until - done) // 2 * 2, until):
            stretch(True, n, 0)
        done = until

    for t in range(NT):
        eta_o[t] = x[0, t, XO:XO + NR, :]
        tu_o[t] = x[1, t, XO:XO + NR, :]
        tv_o[t] = x[2, t, XO:XO + NR, :]
        gu_o[t] = au[t] / hu[t] - su[t]
        gv_o[t] = av[t] / hv[t] - sv[t]

    for group in (row_group, late_group, lane_group, force_group):
        drain(group)


def final_kernel(tab_s, xu, xv, xt, xs, gu, gv, cu, cv, cc, eta, tu, tv, eta_h, tu_h, tv_h, u_h, v_h, t_h, s_h, flat_b, u_b, v_b, t_b, s_b, sem):
    xu, xv, xt, xs = [a.at[:, 0:SLOT, 0:NR, :] for a in (xu, xv, xt, xs)]
    gu, gv, cu, cv, cc, eta, tu, tv = [a.at[:, 0:NR, :] for a in (gu, gv, cu, cv, cc, eta, tu, tv)]
    stores = []
    for i, (a, o) in enumerate(((eta, eta_h), (tu, tu_h), (tv, tv_h))):
        for t in range(NT):
            flat_b[i, :, L * t:L * t + L] = a[t]
        stores.append(pltpu.make_async_copy(flat_b.at[i], o, sem.at[4, i]))
        stores[-1].start()

    below = [[jnp.zeros((NR, L), f32)] * NT for _ in range(2)]
    top = LEV
    for k in range(LEV - 1, -1, -1):
        link, last = tab_s[6 * SLOT + k], tab_s[7 * SLOT + k]
        for t in range(NT):
            cols = slice(L * t, L * t + L)
            u_b[k, :, cols] = jnp.where(cu[t] > float(k), xu[t, k] + gu[t], 0.0)
            v_b[k, :, cols] = jnp.where(cv[t] > float(k), xv[t, k] + gv[t], 0.0)
            for q, (sweep, b) in enumerate(((xt, t_b), (xs, s_b))):
                value = sweep[t, k]
                solved = jnp.where(cc[t] > float(k + 1), value + link * below[q][t], jnp.where(cc[t] > float(k), last * value, value))
                below[q][t] = solved
                b[k, :, cols] = solved
        if k in GROUPS:
            for i, (b, o) in enumerate(((u_b, u_h), (v_b, v_h), (t_b, t_h), (s_b, s_h))):
                stores.append(pltpu.make_async_copy(b.at[k:top], o.at[k:top], sem.at[i, GROUPS.index(k)]))
                stores[-1].start()
            top = k
    for cp in stores:
        cp.wait()


def solution(mesh):
    n_col = mesh.shape['col']
    n_row = mesh.shape['row']

    def step(vel_u, vel_v, value_a11, salinity, surf_eta, trans_u, trans_v, bottom_depth, level_count, avg_weights):
        n_sub = avg_weights.shape[0]
        table = jnp.asarray(solve_table(LEV))
        hbm = pl.BlockSpec(memory_space=pltpu.HBM)
        vmem = pl.BlockSpec(memory_space=pltpu.VMEM)
        smem = pl.BlockSpec(memory_space=pltpu.SMEM)
        V = pltpu.VMEM
        tile = V((NT, RA, L), f32)
        sweep = V((NT, KA, RA, L), f32)
        wide = (NT + 1, XR, L)
        scratch = ([V((NT, KA, PR, L), f32)] * 5 + [V((NT, NR, L), jnp.int32), V((NR, L), f32)]
                   + [V((2, NT, NR + 8, L), f32)] * 2 + [V((4, NT, SLOT, L), f32)] * 4 + [V((NR, L), f32)] * 2 + [V((PR, L), f32)] * 2 + [V((2, PR, L), f32)]
                   + [V((4,) + wide, f32), V((2,) + wide, f32)] + [V((NR, L), f32)] * 2 + [V((3, NR, L), f32)] * 2
                   + [V((NR, L), f32)] * 2 + [V((3, NR, L), f32)] * 2
                   + [V((NR, L), f32)] * 2 + [tile] * 4
                   + [V(wide, f32)] * 9 + [tile] * 2
                   + [pltpu.SMEM((n_sub,), f32), pltpu.SMEM((8 * SLOT,), f32)]
                   + [pltpu.SemaphoreType.DMA((40,)), pltpu.SemaphoreType.DMA((64,)), pltpu.SemaphoreType.DMA((64,))])
        outs = pl.pallas_call(
            functools.partial(ocean_kernel, tuple(mesh.axis_names), n_col, n_row, n_sub),
            out_shape=[tile] * 8 + [sweep] * 4,
            in_specs=[hbm] * 11,
            out_specs=[vmem] * 12,
            scratch_shapes=scratch,
            compiler_params=pltpu.CompilerParams(collective_id=0, has_side_effects=True, vmem_limit_bytes=40 * 1024 * 1024),
        )(*[pltpu.with_memory_space_constraint(a, pltpu.HBM) for a in (vel_u, vel_v, value_a11, salinity, surf_eta, trans_u, trans_v, bottom_depth, level_count, avg_weights, table)])
        eta, tu, tv, gu, gv, cu, cv, cc, xu, xv, xt, xs = [pltpu.with_memory_space_constraint(o, pltpu.VMEM) for o in outs]

        cube = jax.ShapeDtypeStruct((LEV, NR, NC), f32)
        flat = jax.ShapeDtypeStruct((NR, NC), f32)
        return tuple(pl.pallas_call(
            final_kernel,
            out_shape=[flat] * 3 + [cube] * 4,
            in_specs=[smem] + [vmem] * 12,
            out_specs=[hbm] * 7,
            scratch_shapes=[V((3, NR, NC), f32)] + [V((LEV, NR, NC), f32)] * 4 + [pltpu.SemaphoreType.DMA((5, len(GROUPS)))],
            compiler_params=pltpu.CompilerParams(vmem_limit_bytes=24 * 1024 * 1024),
        )(table, xu, xv, xt, xs, gu, gv, cu, cv, cc, eta, tu, tv))

    cube = P(None, 'row', 'col')
    flat = P('row', 'col')
    return jax.shard_map(step, mesh=mesh, in_specs=(cube, cube, cube, cube, flat, flat, flat, flat, flat, P()), out_specs=(flat, flat, flat, cube, cube, cube, cube), check_vma=False)
```

```python
import functools

import jax
import jax.numpy as jnp
import numpy as np
from jax import lax
from jax.experimental import pallas as pl
from jax.experimental.pallas import tpu as pltpu
from jax.sharding import PartitionSpec as P

TIME_STEP = 1.0
GRAVITY = 16.0
BC_GRAVITY = 4.0
EXPAND_T = 0.2
CONTRACT_S = 0.6
CORIO_F0 = 0.4
CORIO_BETA = 0.4
VISC_R = 2.0
DIFF_R = 0.5

LEV = 31
SLOT = 32
NR = 32
NC = 512
NT = 4
L = 128
R0 = 8
PR = 56
KA = SLOT + 1
RA = NR + 8
XR = 120
XO = 40
MESH = pl.DeviceIdType.MESH
f32 = jnp.float32
UNROLL_M = 8
UNROLL_T = 4
GROUPS = (28, 24, 20, 16, 12, 8, 4, 2, 0)


def solve_table(n_levels):
    rows = []
    for s in (VISC_R, DIFF_R):
        scale, carry, link, last = np.zeros((4, SLOT))
        ratio = 0.0
        for k in range(n_levels):
            low = s if k else 0.0
            full = 1.0 + low + s - low * ratio
            end = 1.0 + low - low * ratio
            scale[k], carry[k], link[k], last[k] = 1.0 / full, low / full, s / full, full / end
            ratio = s / full
        rows += [scale, carry, link, last]
    return np.concatenate(rows).astype(np.float32)


def ocean_kernel(axes, n_col, n_row, n_sub, *refs):
    (u_h, v_h, t_h, s_h, eta_h, tu_h, tv_h, dep_h, cnt_h, w_h, tab_h,
     eta_o, tu_o, tv_o, gu_o, gv_o, cu, cv, cc_o, xu, xv, xt, xs,
     bu, bv, bt, bs, bp, cnt_i, rp, s1, s2,
     pn, ps, rn, rs, pw, pe, rw, re, ha, x, xf, qw, qe, we, ww, fw, fe, fre, frw,
     fu4, fv4, hu, hv, su, sv,
     ca, cb, cc, cd, cg, ch, cm, cn, tt, au, av,
     w_s, tab_s, lsem, ssem, rsem) = refs
    xu, xv, xt, xs = [a.at[:, 0:SLOT, 0:NR, :] for a in (xu, xv, xt, xs)]
    eta_o, tu_o, tv_o, gu_o, gv_o, cu, cv, cc_o, hu, hv, su, sv, au, av = [a.at[:, 0:NR, :] for a in (eta_o, tu_o, tv_o, gu_o, gv_o, cu, cv, cc_o, hu, hv, su, sv, au, av)]
    col = lax.axis_index('col')
    row = lax.axis_index('row')
    east = lax.rem(col + 1, n_col)
    west = lax.rem(col + n_col - 1, n_col)
    has_s = row > 0
    has_n = row < n_row - 1

    def dev(c, r):
        at = {'col': c, 'row': r}
        return tuple(at[name] for name in axes)

    bufs = (bu, bv, bt, bs)
    barrier = pltpu.get_barrier_semaphore()

    def signal(c, r):
        pl.semaphore_signal(barrier, inc=1, device_id=dev(c, r), device_id_type=MESH)

    signal(west, row)
    signal(east, row)

    @pl.when(has_s)
    def _():
        for c in (west, col, east):
            signal(c, row - 1)

    @pl.when(has_n)
    def _():
        for c in (west, col, east):
            signal(c, row + 1)

    zero = functools.partial(jnp.zeros, dtype=f32)

    loads = []
    for f, (src, dst) in enumerate(zip((u_h, v_h, t_h, s_h), bufs)):
        for t in range(NT):
            loads.append(pltpu.make_async_copy(src.at[:, :, L * t:L * t + L], dst.at[t, 0:LEV, R0:R0 + NR, :], lsem.at[len(loads)]))
    flat_loads = []
    for f, src in enumerate((eta_h, tu_h, tv_h)):
        for t in range(NT):
            flat_loads.append(pltpu.make_async_copy(src.at[:, L * t:L * t + L], x.at[f, t, XO:XO + NR, :], lsem.at[len(loads) + len(flat_loads)]))
    for t in range(NT):
        flat_loads.append(pltpu.make_async_copy(dep_h.at[:, L * t:L * t + L], bv.at[t, LEV, R0:R0 + NR, :], lsem.at[len(loads) + len(flat_loads)]))
    for t in range(NT):
        flat_loads.append(pltpu.make_async_copy(cnt_h.at[:, L * t:L * t + L], cnt_i.at[t], lsem.at[len(loads) + len(flat_loads)]))
    scalar_loads = [pltpu.make_async_copy(w_h, w_s, lsem.at[36]), pltpu.make_async_copy(tab_h, tab_s, lsem.at[37])]
    edge_loads = [loads[NT * f + t] for f in range(4) for t in (0, NT - 1)]
    mid_loads = [loads[NT * f + t] for f in range(4) for t in range(1, NT - 1)]
    for cp in flat_loads[3 * NT:] + edge_loads + mid_loads + flat_loads[:3 * NT] + scalar_loads:
        cp.start()

    n_copies = 0

    def remote(src, dst, c, r, sends, receives):
        nonlocal n_copies
        i = n_copies
        n_copies += 1
        return (pltpu.make_async_remote_copy(src, dst, ssem.at[i], rsem.at[i], device_id=dev(c, r), device_id_type=MESH), sends, receives)

    def maybe(cond, fn):
        if cond is None:
            fn()
        else:
            pl.when(cond)(fn)

    def start(group):
        for cp, sends, _ in group:
            maybe(sends, cp.start)

    def arrive(group):
        for cp, _, receives in group:
            maybe(receives, cp.wait_recv)

    def drain(group):
        for cp, sends, _ in group:
            maybe(sends, cp.wait_send)

    def rows_of(fields):
        return [remote(pn.at[fields], rs.at[fields], col, row + 1, has_n, has_s),
                remote(ps.at[fields], rn.at[fields], col, row - 1, has_s, has_n)]

    def level_rows(b, k, r):
        return b.reshape(NT, KA * PR, L), pl.ds(k * PR + r, 8, stride=PR)

    def pack_rows(fields):
        for f in fields:
            for t in range(NT):
                for k in range(0, SLOT, 8):
                    for to, r in ((pn, R0 + NR - 1), (ps, R0)):
                        flat, at = level_rows(bufs[f], k, r)
                        to[f, t, k:k + 8, :] = flat[t, at, :]

    def unpack_rows(fields):
        for f in fields:
            for t in range(NT):
                for k in range(0, SLOT, 8):
                    for to, r in ((rs, R0 - 1), (rn, R0 + NR)):
                        flat, at = level_rows(bufs[f], k, r)
                        flat[t, at, :] = to[f, t, k:k + 8, :]

    def wide_of(b, lanes_w, lanes_e, from_e, from_w):
        own = b.at[:, 0:NT, XO:XO + NR, :]
        return [remote(own, b.at[:, 0:NT, 8:XO, :], col, row + 1, has_n, has_s),
                remote(own, b.at[:, 0:NT, XO + NR:XO + 2 * NR, :], col, row - 1, has_s, has_n),
                remote(lanes_w, from_e.at[1], west, row, None, None),
                remote(lanes_e, from_w.at[1], east, row, None, None),
                remote(lanes_w, from_e.at[2], west, row - 1, has_s, has_n),
                remote(lanes_e, from_w.at[2], east, row - 1, has_s, has_n),
                remote(lanes_w, from_e.at[0], west, row + 1, has_n, has_s),
                remote(lanes_e, from_w.at[0], east, row + 1, has_n, has_s)]

    row_group, late_group = rows_of(slice(0, 2)), rows_of(slice(2, 4))
    lane_group = [remote(pw, re.at[R0:R0 + NR, :], west, row, None, None),
                  remote(pe, rw.at[R0:R0 + NR, :], east, row, None, None),
                  remote(pe.at[0:1, :], rw.at[R0 + NR:R0 + NR + 1, :], east, row - 1, has_s, has_n),
                  remote(pw.at[NR - 1:NR, :], re.at[R0 - 1:R0, :], west, row + 1, has_n, has_s)]
    wide_group = wide_of(x, qw, qe, we, ww)
    force_group = wide_of(xf, fw, fe, fre, frw)

    edge = jnp.logical_or(row == 0, row == n_row - 1)

    @pl.when(edge)
    def _():
        pl.semaphore_wait(barrier, 5)

    @pl.when(jnp.logical_not(edge))
    def _():
        pl.semaphore_wait(barrier, 8)

    lane_p = lax.broadcasted_iota(jnp.int32, (PR, L), 1)
    lane = lane_p[:NR]

    for t in range(NT):
        bt[t, LEV, R0:R0 + NR, :] = zero((NR, L))
        bs[t, LEV, R0:R0 + NR, :] = zero((NR, L))
    for cp in flat_loads[3 * NT:]:
        cp.wait()
    for t in range(NT):
        count = cnt_i[t].astype(f32)
        bu[t, LEV, R0:R0 + NR, :] = count
        x[3, t, XO:XO + NR, :] = jnp.where(count > 0.0, bv[t, LEV, R0:R0 + NR, :], 0.0)

    def roll(a, shift):
        return pltpu.roll(a, shift, 1) if not (isinstance(shift, int) and shift % L == 0) else a

    pair = lax.shift_right_logical(lane, 1)
    packed = [zero((NR, L))] * 2
    for f, b in enumerate(bufs):
        edge_loads[2 * f].wait()
        edge_loads[2 * f + 1].wait()
        for k in range(SLOT):
            p = SLOT * (f % 2) + k
            both = jnp.where(lane == 0, b[0, k, R0:R0 + NR, :], b[NT - 1, k, R0:R0 + NR, :])
            packed[f // 2] = jnp.where(pair == p, roll(both, (2 * p + 1) % L), packed[f // 2])
    even = lax.rem(lane_p, 2) == 0
    pw[...] = jnp.where(even[:NR], roll(packed[1], L - 1), packed[0])
    pe[...] = jnp.where(even[:NR], packed[0], roll(packed[1], 1))
    start(lane_group)
    for cp in mid_loads:
        cp.wait()
    pack_rows((0, 1))
    start(row_group)
    pack_rows((2, 3))
    start(late_group)

    def pack_wide(b, n_fields):
        first = last = zero((NR, L))
        for f in range(n_fields):
            mine = (lane >= 32 * f) & (lane < 32 * f + 32)
            first = jnp.where(mine, roll(b[f, 0, XO:XO + NR, :], 32 * f), first)
            last = jnp.where(mine, roll(b[f, NT - 1, XO:XO + NR, :], (32 * f + 32) % L), last)
        return first, last

    for cp in flat_loads[:3 * NT]:
        cp.wait()
    first, last = pack_wide(x, 4)
    qw[...] = first
    qe[...] = last
    start(wide_group)
    for cp in scalar_loads:
        cp.wait()

    for f in range(4):
        for t in range(NT + 1):
            x[f, t, 0:8, :] = zero((8, L))
            x[f, t, XR - 16:XR, :] = zero((16, L))
    for t in range(NT + 1):
        tt[t, XR - 16:XR, :] = zero((16, L))
    for t in range(NT):
        for a in (xu, xv, xt, xs):
            a[t, 0] = zero((NR, L))

    @pl.when(jnp.logical_not(has_s))
    def _():
        rs[...] = zero((4, NT, SLOT, L))
        re[R0 - 8:R0, :] = zero((8, L))
        x[:, 0:NT, 8:XO, :] = zero((4, NT, NR, L))
        xf[:, 0:NT, 8:XO, :] = zero((2, NT, NR, L))
        for a in (we, ww, fre, frw):
            a[0] = zero((NR, L))

    @pl.when(jnp.logical_not(has_n))
    def _():
        rn[...] = zero((4, NT, SLOT, L))
        rw[R0 + NR:R0 + NR + 8, :] = zero((8, L))
        x[:, 0:NT, XO + NR:XO + 2 * NR, :] = zero((4, NT, NR, L))
        xf[:, 0:NT, XO + NR:XO + 2 * NR, :] = zero((2, NT, NR, L))
        for a in (we, ww, fre, frw):
            a[2] = zero((NR, L))


    row_pos = (row * NR + lax.broadcasted_iota(jnp.int32, (NR, L), 0)).astype(f32)
    total_rows = NR * n_row
    fu4[...] = 0.25 * (CORIO_F0 + CORIO_BETA * ((row_pos + 0.5) / total_rows - 0.5))
    fv4[...] = 0.25 * (CORIO_F0 + CORIO_BETA * ((row_pos + 1.0) / total_rows - 0.5))

    def to_east(tiles, halo, ts=range(NT)):
        last_lane = lane_p[:tiles[ts[0]].shape[0]] == L - 1
        rolled = {t: halo if t == NT else roll(tiles[t], L - 1) for t in sorted({t + d for t in ts for d in (0, 1)})}
        return {t: jnp.where(last_lane, rolled[t + 1], rolled[t]) for t in ts}

    def to_west(tiles, halo, ts=range(NT)):
        first_lane = lane_p[:tiles[ts[0]].shape[0]] == 0
        rolled = {t: halo if t < 0 else roll(tiles[t], 1) for t in sorted({t + d for t in ts for d in (-1, 0)})}
        return {t: jnp.where(first_lane, rolled[t - 1], rolled[t]) for t in ts}

    def side(f, k, lo=R0, n=NR):
        return pltpu.roll(ha[f // 2, lo:lo + n, :], lax.rem(L - 2 * (SLOT * (f % 2) + k), L), 1)

    def level(b, k, lo=R0, n=NR):
        return [b[t, k, lo:lo + n, :] for t in range(NT)]

    def each_level(fn, unroll):
        def some(i, _):
            base = i * unroll
            for j in range(unroll):
                fn(base + j, base + j - 1 if j else jnp.maximum(base - 1, 0), j % 2)
            return 0

        lax.fori_loop(0, -(-LEV // unroll), some, 0)

    p_scale = BC_GRAVITY / LEV

    def pressure(lo, n):
        total = zero((NT, n, L))
        for k in range(LEV):
            density = CONTRACT_S * bs[:, k, lo:lo + n, :] - EXPAND_T * bt[:, k, lo:lo + n, :]
            total = total + density
            bp[:, k, lo:lo + n, :] = p_scale * (total - 0.5 * density)
        bp[:, LEV, lo:lo + n, :] = zero((NT, n, L))

    pressure(R0, NR)
    for k in range(LEV):
        bp[:, k, R0 + NR:R0 + NR + 8, :] = zero((NT, 8, L))

    def momentum_down(ts, k, prev, slot):
        scale, carry = tab_s[k], tab_s[SLOT + k]
        u5, v5 = level(bu, k, R0, NR + 8), level(bv, k, R0 - 8, NR + 8)
        u_side = v_side = p_side = jnp.zeros((NR + 8, L), f32)
        if 0 in ts:
            u_side, v_side = side(0, k, R0, NR + 8), side(1, k, R0 - 8, NR + 8)
            p_side = pltpu.roll(rp[...], L - 1 - 2 * k, 1)
        uw, ve = to_west(u5, u_side, ts), to_east(v5, v_side, ts)
        um, vm = [a[:NR] for a in u5], [a[8:] for a in v5]
        ue, vw = to_east(um, u_side[:NR], ts), to_west(vm, v_side[8:], ts)
        pm, pn = level(bp, k), level(bp, k, R0 + 1)
        pe_ = to_east(pm, p_side, ts)
        for t in ts:
            u_sum, v_sum = u5[t] + uw[t], v5[t] + ve[t]
            s1[slot, t] = u_sum
            s2[slot, t] = v_sum
            ub4 = u_sum[:NR] + s1[slot, t, 1:NR + 1, :]
            vb4 = v_sum[8:] + s2[slot, t, 7:NR + 7, :]
            un, us = bu[t, k, R0 + 1:R0 + 1 + NR, :], bu[t, k, R0 - 1:R0 - 1 + NR, :]
            vn, vs = bv[t, k, R0 + 1:R0 + 1 + NR, :], bv[t, k, R0 - 1:R0 - 1 + NR, :]
            u_star = um[t] + vb4 * (fu4[...] - 0.125 * (un - us)) - um[t] * (0.5 * (ue[t] - uw[t][:NR])) + (pm[t] - pe_[t])
            v_star = vm[t] - ub4 * (fv4[...] + 0.125 * (ve[t][8:] - vw[t])) - vm[t] * (0.5 * (vn - vs)) + (pm[t] - pn[t])
            xu[t, k] = scale * u_star + carry * xu[t, prev]
            xv[t, k] = scale * v_star + carry * xv[t, prev]

    arrive(lane_group)
    ha[0] = jnp.where(even, rw[...], roll(re[...], L - 2))
    ha[1] = jnp.where(even, roll(rw[...], L - 1), roll(re[...], L - 1))
    east_ = roll(ha[1, R0:R0 + NR, :], 1)
    density = CONTRACT_S * roll(east_, L // 2) - EXPAND_T * east_
    total = density
    for step in (2, 4, 8, 16, 32):
        total = total + jnp.where(lane >= step, roll(total, step), 0.0)
    rp[...] = p_scale * (total - 0.5 * density)
    arrive(row_group)
    unpack_rows((0, 1))
    each_level(functools.partial(momentum_down, tuple(range(NT))), UNROLL_M)

    arrive(late_group)
    unpack_rows((2, 3))
    last_row = lax.broadcasted_iota(jnp.int32, (NT, 8, L), 1) == 7
    pressure(R0 + NR, 8)
    sweep = zero((NT, 8, L))
    for k in range(LEV):
        sweep = tab_s[SLOT + k] * sweep - tab_s[k] * bp[:, k, R0 + NR - 7:R0 + NR + 1, :]
        xv[:, k, NR - 8:NR, :] += jnp.where(last_row, sweep, 0.0)

    c_mid, d_mid = level(bu, LEV), level(bv, LEV)
    c_east = to_east(c_mid, side(0, LEV))
    d_east = to_east(d_mid, side(1, LEV))
    c_north, c_south = level(bu, LEV, R0 + 1), level(bu, LEV, R0 - 1)
    d_north = level(bv, LEV, R0 + 1)
    for t in range(NT):
        cu[t] = jnp.minimum(c_mid[t], c_east[t])
        cv[t] = jnp.minimum(c_mid[t], c_north[t])
        hu[t] = 0.5 * (d_mid[t] + d_east[t])
        hv[t] = 0.5 * (d_mid[t] + d_north[t])
        cc_o[t] = c_mid[t]
    c_west0 = jnp.minimum(side(0, LEV), c_mid[0])

    def momentum_up(t, _):
        z = zero((NR, L))
        state = [[z, z, z], [z, z, z]]
        for k in range(LEV - 1, -1, -1):
            link, last_ = tab_s[2 * SLOT + k], tab_s[3 * SLOT + k]
            for q, (sweep, b, count) in enumerate(((xu, bu, cu), (xv, bv, cv))):
                below, sum_x, sum_0 = state[q]
                value = sweep[t, k]
                active = count[t] > float(k)
                solved = jnp.where(count[t] > float(k + 1), value + link * below, jnp.where(active, last_ * value, 0.0))
                sweep[t, k] = solved
                start_ = jnp.where(active, b[t, k, R0:R0 + NR, :], 0.0)
                b[t, k, R0:R0 + NR, :] = start_
                state[q] = [solved, sum_x + solved, sum_0 + start_]
        for q, (h, mean, count) in enumerate(((hu, su, cu), (hv, sv, cv))):
            _, total, start_ = state[q]
            n_active = jnp.maximum(count[t], 1.0)
            mean[t] = total / n_active
            xf[q, t, XO:XO + NR, :] = h[t] * (total - start_) / n_active / TIME_STEP
        c_south = jnp.minimum(bu[t, LEV, 0:8, :], pltpu.roll(bu[t, LEV, R0:R0 + 8, :], 7, 0))
        for k in range(LEV):
            bv[t, k, 0:8, :] = jnp.where(c_south > float(k), bv[t, k, 0:8, :], 0.0)
        return 0

    lax.fori_loop(0, NT, momentum_up, 0)

    first, last = pack_wide(xf, 2)
    fw[...] = first
    fe[...] = last
    start(force_group)

    def tracer_down(k, prev, slot):
        scale, carry = tab_s[4 * SLOT + k], tab_s[5 * SLOT + k]
        kf = lax.convert_element_type(k, f32)
        um, vm, vs = level(bu, k), level(bv, k), level(bv, k, R0 - 1)
        uw0 = jnp.where(c_west0 > kf, side(0, k), 0.0)
        for f, b, sweep in ((2, bt, xt), (3, bs, xs)):
            q = level(b, k)
            q_side = side(f, k)
            qe_ = to_east(q, q_side)
            f_east = [um[t] * (q[t] + qe_[t]) for t in range(NT)]
            f_west = to_west(f_east, uw0 * (q_side + q[0]))
            for t in range(NT):
                f_north = vm[t] * (q[t] + b[t, k, R0 + 1:R0 + 1 + NR, :])
                f_south = vs[t] * (b[t, k, R0 - 1:R0 - 1 + NR, :] + q[t])
                new = q[t] - 0.5 * TIME_STEP * (f_east[t] - f_west[t] + f_north - f_south)
                sweep[t, k] = jnp.where(bu[t, LEV, R0:R0 + NR, :] > kf, scale * new + carry * sweep[t, prev], new)

    each_level(tracer_down, UNROLL_T)

    arrive(wide_group)
    drain(wide_group)
    arrive(force_group)

    def unpack_wide(b, from_e, from_w, n_fields):
        for f in range(n_fields):
            for seg in range(3):
                b[f, NT, 8 + NR * seg:8 + NR * seg + NR, :] = jnp.where(lane < L // 2, roll(from_e[seg], (L - 32 * f) % L), roll(from_w[seg], (96 - 32 * f) % L))

    unpack_wide(x, we, ww, 4)
    unpack_wide(xf, fre, frw, 2)
    dt_fast = TIME_STEP / n_sub
    XT = NT + 1

    def ring_east(tiles, last_lane):
        rolled = [roll(a, L - 1) for a in tiles]
        return [jnp.where(last_lane, rolled[(t + 1) % XT], rolled[t]) for t in range(XT)]

    def ring_west(tiles, first_lane):
        rolled = [roll(a, 1) for a in tiles]
        return [jnp.where(first_lane, rolled[(t - 1) % XT], rolled[t]) for t in range(XT)]

    for seg in range(3):
        lo = 8 + NR * seg
        pos = (row * NR + NR * (seg - 1) + lax.broadcasted_iota(jnp.int32, (NR, L), 0)).astype(f32)
        f_u = CORIO_F0 + CORIO_BETA * ((pos + 0.5) / total_rows - 0.5)
        f_v = CORIO_F0 + CORIO_BETA * ((pos + 1.0) / total_rows - 0.5)
        d = [x[3, t, lo:lo + NR, :] for t in range(XT)]
        d_e = ring_east(d, lane == L - 1)
        for t in range(XT):
            d_n = x[3, t, lo + 1:lo + 1 + NR, :]
            wet = jnp.where((d[t] > 0.0) & (d_e[t] > 0.0), 1.0, 0.0)
            cm[t, lo:lo + NR, :] = wet
            ca[t, lo:lo + NR, :] = (0.25 * dt_fast) * f_u * wet
            cb[t, lo:lo + NR, :] = (dt_fast * GRAVITY * 0.5) * (d[t] + d_e[t]) * wet
            cc[t, lo:lo + NR, :] = dt_fast * xf[0, t, lo:lo + NR, :] * wet
            wet = jnp.where((d[t] > 0.0) & (d_n > 0.0), 1.0, 0.0)
            cn[t, lo:lo + NR, :] = wet
            cd[t, lo:lo + NR, :] = (0.25 * dt_fast) * f_v * wet
            cg[t, lo:lo + NR, :] = (dt_fast * GRAVITY * 0.5) * (d[t] + d_n) * wet
            ch[t, lo:lo + NR, :] = dt_fast * xf[1, t, lo:lo + NR, :] * wet

    for t in range(NT):
        au[t] = zero((NR, L))
        av[t] = zero((NR, L))

    def subcycle(side_rows, masked, n, _):
        weight = w_s[n]
        parts = ((XO - side_rows, side_rows), (XO, NR), (XO + NR, side_rows))
        for r, chunk in parts:
            first_lane = lane[:chunk] == 0
            u_t = [x[1, t, r:r + chunk, :] for t in range(XT)]
            u_w = ring_west(u_t, first_lane)
            for t in range(XT):
                v_t, v_s = x[2, t, r:r + chunk, :], x[2, t, r - 1:r - 1 + chunk, :]
                x[0, t, r:r + chunk, :] = x[0, t, r:r + chunk, :] - dt_fast * ((u_t[t] - u_w[t]) + (v_t - v_s))
                tt[t, r:r + chunk, :] = u_t[t] + u_w[t]
        for r, chunk in parts[::-1]:
            last_lane = lane[:chunk] == L - 1
            e_t = [x[0, t, r:r + chunk, :] for t in range(XT)]
            e_e = ring_east(e_t, last_lane)
            v_t = [x[2, t, r:r + chunk, :] for t in range(XT)]
            s_t = [v_t[t] + x[2, t, r - 1:r - 1 + chunk, :] for t in range(XT)]
            s_e = ring_east(s_t, last_lane)
            for t in range(XT):
                at = (t, slice(r, r + chunk))
                up = (t, slice(r + 1, r + 1 + chunk))
                e_n = x[0, t, r + 1:r + 1 + chunk, :]
                u_old = x[1, t, r:r + chunk, :] if masked else cm[at] * x[1, t, r:r + chunk, :]
                v_old = v_t[t] if masked else cn[at] * v_t[t]
                u_new = u_old + ca[at] * (s_t[t] + s_e[t]) + cc[at] - cb[at] * (e_e[t] - e_t[t])
                v_new = v_old - cd[at] * (tt[at] + tt[up]) + ch[at] - cg[at] * (e_n - e_t[t])
                x[1, t, r:r + chunk, :] = u_new
                x[2, t, r:r + chunk, :] = v_new
                if r == XO and t < NT:
                    au[t] += weight * u_new
                    av[t] += weight * v_new
        return 0

    done = 0
    for tiles in (4, 3, 2, 1):
        until = n_sub - 8 * (tiles - 1)
        stretch = functools.partial(subcycle, 8 * tiles)
        if done == 0:
            stretch(False, 0, 0)
            stretch(True, 1, 0)
            done = 2

        def two(i, _, stretch=stretch, done=done):
            stretch(True, done + 2 * i, 0)
            stretch(True, done + 2 * i + 1, 0)
            return 0

        lax.fori_loop(0, (until - done) // 2, two, 0)
        for n in range(done + (until - done) // 2 * 2, until):
            stretch(True, n, 0)
        done = until

    for t in range(NT):
        eta_o[t] = x[0, t, XO:XO + NR, :]
        tu_o[t] = x[1, t, XO:XO + NR, :]
        tv_o[t] = x[2, t, XO:XO + NR, :]
        gu_o[t] = au[t] / hu[t] - su[t]
        gv_o[t] = av[t] / hv[t] - sv[t]

    for group in (row_group, late_group, lane_group, force_group):
        drain(group)


def final_kernel(tab_s, xu, xv, xt, xs, gu, gv, cu, cv, cc, eta, tu, tv, eta_h, tu_h, tv_h, u_h, v_h, t_h, s_h, flat_b, u_b, v_b, t_b, s_b, sem):
    xu, xv, xt, xs = [a.at[:, 0:SLOT, 0:NR, :] for a in (xu, xv, xt, xs)]
    gu, gv, cu, cv, cc, eta, tu, tv = [a.at[:, 0:NR, :] for a in (gu, gv, cu, cv, cc, eta, tu, tv)]
    stores = []
    for i, (a, o) in enumerate(((eta, eta_h), (tu, tu_h), (tv, tv_h))):
        for t in range(NT):
            flat_b[i, :, L * t:L * t + L] = a[t]
        stores.append(pltpu.make_async_copy(flat_b.at[i], o, sem.at[4, i]))
        stores[-1].start()

    below = [[jnp.zeros((NR, L), f32)] * NT for _ in range(2)]
    top = LEV
    for k in range(LEV - 1, -1, -1):
        link, last = tab_s[6 * SLOT + k], tab_s[7 * SLOT + k]
        for t in range(NT):
            cols = slice(L * t, L * t + L)
            u_b[k, :, cols] = jnp.where(cu[t] > float(k), xu[t, k] + gu[t], 0.0)
            v_b[k, :, cols] = jnp.where(cv[t] > float(k), xv[t, k] + gv[t], 0.0)
            for q, (sweep, b) in enumerate(((xt, t_b), (xs, s_b))):
                value = sweep[t, k]
                solved = jnp.where(cc[t] > float(k + 1), value + link * below[q][t], jnp.where(cc[t] > float(k), last * value, value))
                below[q][t] = solved
                b[k, :, cols] = solved
        if k in GROUPS:
            for i, (b, o) in enumerate(((u_b, u_h), (v_b, v_h), (t_b, t_h), (s_b, s_h))):
                stores.append(pltpu.make_async_copy(b.at[k:top], o.at[k:top], sem.at[i, GROUPS.index(k)]))
                stores[-1].start()
            top = k
    for cp in stores:
        cp.wait()


def solution(mesh):
    n_col = mesh.shape['col']
    n_row = mesh.shape['row']

    def step(vel_u, vel_v, value_a11, salinity, surf_eta, trans_u, trans_v, bottom_depth, level_count, avg_weights):
        n_sub = avg_weights.shape[0]
        table = jnp.asarray(solve_table(LEV))
        hbm = pl.BlockSpec(memory_space=pltpu.HBM)
        vmem = pl.BlockSpec(memory_space=pltpu.VMEM)
        smem = pl.BlockSpec(memory_space=pltpu.SMEM)
        V = pltpu.VMEM
        tile = V((NT, RA, L), f32)
        sweep = V((NT, KA, RA, L), f32)
        wide = (NT + 1, XR, L)
        scratch = ([V((NT, KA, PR, L), f32)] * 5 + [V((NT, NR, L), jnp.int32), V((NR, L), f32)]
                   + [V((2, NT, NR + 8, L), f32)] * 2 + [V((4, NT, SLOT, L), f32)] * 4 + [V((NR, L), f32)] * 2 + [V((PR, L), f32)] * 2 + [V((2, PR, L), f32)]
                   + [V((4,) + wide, f32), V((2,) + wide, f32)] + [V((NR, L), f32)] * 2 + [V((3, NR, L), f32)] * 2
                   + [V((NR, L), f32)] * 2 + [V((3, NR, L), f32)] * 2
                   + [V((NR, L), f32)] * 2 + [tile] * 4
                   + [V(wide, f32)] * 9 + [tile] * 2
                   + [pltpu.SMEM((n_sub,), f32), pltpu.SMEM((8 * SLOT,), f32)]
                   + [pltpu.SemaphoreType.DMA((40,)), pltpu.SemaphoreType.DMA((64,)), pltpu.SemaphoreType.DMA((64,))])
        outs = pl.pallas_call(
            functools.partial(ocean_kernel, tuple(mesh.axis_names), n_col, n_row, n_sub),
            out_shape=[tile] * 8 + [sweep] * 4,
            in_specs=[hbm] * 11,
            out_specs=[vmem] * 12,
            scratch_shapes=scratch,
            compiler_params=pltpu.CompilerParams(collective_id=0, has_side_effects=True, vmem_limit_bytes=40 * 1024 * 1024),
        )(*[pltpu.with_memory_space_constraint(a, pltpu.HBM) for a in (vel_u, vel_v, value_a11, salinity, surf_eta, trans_u, trans_v, bottom_depth, level_count, avg_weights, table)])
        eta, tu, tv, gu, gv, cu, cv, cc, xu, xv, xt, xs = [pltpu.with_memory_space_constraint(o, pltpu.VMEM) for o in outs]

        cube = jax.ShapeDtypeStruct((LEV, NR, NC), f32)
        flat = jax.ShapeDtypeStruct((NR, NC), f32)
        return tuple(pl.pallas_call(
            final_kernel,
            out_shape=[flat] * 3 + [cube] * 4,
            in_specs=[smem] + [vmem] * 12,
            out_specs=[hbm] * 7,
            scratch_shapes=[V((3, NR, NC), f32)] + [V((LEV, NR, NC), f32)] * 4 + [pltpu.SemaphoreType.DMA((5, len(GROUPS)))],
            compiler_params=pltpu.CompilerParams(vmem_limit_bytes=24 * 1024 * 1024),
        )(table, xu, xv, xt, xs, gu, gv, cu, cv, cc, eta, tu, tv))

    cube = P(None, 'row', 'col')
    flat = P('row', 'col')
    return jax.shard_map(step, mesh=mesh, in_specs=(cube, cube, cube, cube, flat, flat, flat, flat, flat, P()), out_specs=(flat, flat, flat, cube, cube, cube, cube), check_vma=False)
```

```python
import functools

import jax
import jax.numpy as jnp
import numpy as np
from jax import lax
from jax.experimental import pallas as pl
from jax.experimental.pallas import tpu as pltpu
from jax.sharding import PartitionSpec as P

TIME_STEP = 1.0
GRAVITY = 16.0
BC_GRAVITY = 4.0
EXPAND_T = 0.2
CONTRACT_S = 0.6
CORIO_F0 = 0.4
CORIO_BETA = 0.4
VISC_R = 2.0
DIFF_R = 0.5

LEV = 31
SLOT = 32
NR = 32
NC = 512
NT = 4
L = 128
R0 = 8
PR = 56
KA = SLOT + 1
RA = NR + 8
XR = 120
XO = 40
MESH = pl.DeviceIdType.MESH
f32 = jnp.float32
UNROLL_M = 8
UNROLL_T = 4
GROUPS = (28, 24, 20, 16, 12, 8, 4, 2, 0)


def solve_table(n_levels):
    rows = []
    for s in (VISC_R, DIFF_R):
        scale, carry, link, last = np.zeros((4, SLOT))
        ratio = 0.0
        for k in range(n_levels):
            low = s if k else 0.0
            full = 1.0 + low + s - low * ratio
            end = 1.0 + low - low * ratio
            scale[k], carry[k], link[k], last[k] = 1.0 / full, low / full, s / full, full / end
            ratio = s / full
        rows += [scale, carry, link, last]
    return np.concatenate(rows).astype(np.float32)


def ocean_kernel(axes, n_col, n_row, n_sub, *refs):
    (u_h, v_h, t_h, s_h, eta_h, tu_h, tv_h, dep_h, cnt_h, w_h, tab_h,
     eta_o, tu_o, tv_o, gu_o, gv_o, cu, cv, cc_o, xu, xv, xt, xs,
     bu, bv, bt, bs, bp, cnt_i, rp, s1, s2,
     pn, ps, rn, rs, pw, pe, rw, re, ha, x, xf, qw, qe, we, ww, fw, fe, fre, frw,
     fu4, fv4, hu, hv, su, sv,
     ca, cb, cc, cd, cg, ch, cm, cn, tt, au, av,
     w_s, tab_s, lsem, ssem, rsem) = refs
    xu, xv, xt, xs = [a.at[:, 0:SLOT, 0:NR, :] for a in (xu, xv, xt, xs)]
    eta_o, tu_o, tv_o, gu_o, gv_o, cu, cv, cc_o, hu, hv, su, sv, au, av = [a.at[:, 0:NR, :] for a in (eta_o, tu_o, tv_o, gu_o, gv_o, cu, cv, cc_o, hu, hv, su, sv, au, av)]
    col = lax.axis_index('col')
    row = lax.axis_index('row')
    east = lax.rem(col + 1, n_col)
    west = lax.rem(col + n_col - 1, n_col)
    has_s = row > 0
    has_n = row < n_row - 1

    def dev(c, r):
        at = {'col': c, 'row': r}
        return tuple(at[name] for name in axes)

    bufs = (bu, bv, bt, bs)
    barrier = pltpu.get_barrier_semaphore()

    def signal(c, r):
        pl.semaphore_signal(barrier, inc=1, device_id=dev(c, r), device_id_type=MESH)

    signal(west, row)
    signal(east, row)

    @pl.when(has_s)
    def _():
        for c in (west, col, east):
            signal(c, row - 1)

    @pl.when(has_n)
    def _():
        for c in (west, col, east):
            signal(c, row + 1)

    zero = functools.partial(jnp.zeros, dtype=f32)

    loads = []
    for f, (src, dst) in enumerate(zip((u_h, v_h, t_h, s_h), bufs)):
        for t in range(NT):
            loads.append(pltpu.make_async_copy(src.at[:, :, L * t:L * t + L], dst.at[t, 0:LEV, R0:R0 + NR, :], lsem.at[len(loads)]))
    flat_loads = []
    for f, src in enumerate((eta_h, tu_h, tv_h)):
        for t in range(NT):
            flat_loads.append(pltpu.make_async_copy(src.at[:, L * t:L * t + L], x.at[f, t, XO:XO + NR, :], lsem.at[len(loads) + len(flat_loads)]))
    for t in range(NT):
        flat_loads.append(pltpu.make_async_copy(dep_h.at[:, L * t:L * t + L], bv.at[t, LEV, R0:R0 + NR, :], lsem.at[len(loads) + len(flat_loads)]))
    for t in range(NT):
        flat_loads.append(pltpu.make_async_copy(cnt_h.at[:, L * t:L * t + L], cnt_i.at[t], lsem.at[len(loads) + len(flat_loads)]))
    scalar_loads = [pltpu.make_async_copy(w_h, w_s, lsem.at[36]), pltpu.make_async_copy(tab_h, tab_s, lsem.at[37])]
    edge_loads = [loads[NT * f + t] for f in range(4) for t in (0, NT - 1)]
    mid_loads = [loads[NT * f + t] for f in range(4) for t in range(1, NT - 1)]
    for cp in flat_loads[3 * NT:] + edge_loads + mid_loads + flat_loads[:3 * NT] + scalar_loads:
        cp.start()

    n_copies = 0

    def remote(src, dst, c, r, sends, receives):
        nonlocal n_copies
        i = n_copies
        n_copies += 1
        return (pltpu.make_async_remote_copy(src, dst, ssem.at[i], rsem.at[i], device_id=dev(c, r), device_id_type=MESH), sends, receives)

    def maybe(cond, fn):
        if cond is None:
            fn()
        else:
            pl.when(cond)(fn)

    def start(group):
        for cp, sends, _ in group:
            maybe(sends, cp.start)

    def arrive(group):
        for cp, _, receives in group:
            maybe(receives, cp.wait_recv)

    def drain(group):
        for cp, sends, _ in group:
            maybe(sends, cp.wait_send)

    def rows_of(fields):
        return [remote(pn.at[fields], rs.at[fields], col, row + 1, has_n, has_s),
                remote(ps.at[fields], rn.at[fields], col, row - 1, has_s, has_n)]

    def level_rows(b, k, r):
        return b.reshape(NT, KA * PR, L), pl.ds(k * PR + r, 8, stride=PR)

    def pack_rows(fields):
        for f in fields:
            for t in range(NT):
                for k in range(0, SLOT, 8):
                    for to, r in ((pn, R0 + NR - 1), (ps, R0)):
                        flat, at = level_rows(bufs[f], k, r)
                        to[f, t, k:k + 8, :] = flat[t, at, :]

    def unpack_rows(fields):
        for f in fields:
            for t in range(NT):
                for k in range(0, SLOT, 8):
                    for to, r in ((rs, R0 - 1), (rn, R0 + NR)):
                        flat, at = level_rows(bufs[f], k, r)
                        flat[t, at, :] = to[f, t, k:k + 8, :]

    def wide_of(b, lanes_w, lanes_e, from_e, from_w):
        own = b.at[:, 0:NT, XO:XO + NR, :]
        return [remote(own, b.at[:, 0:NT, 8:XO, :], col, row + 1, has_n, has_s),
                remote(own, b.at[:, 0:NT, XO + NR:XO + 2 * NR, :], col, row - 1, has_s, has_n),
                remote(lanes_w, from_e.at[1], west, row, None, None),
                remote(lanes_e, from_w.at[1], east, row, None, None),
                remote(lanes_w, from_e.at[2], west, row - 1, has_s, has_n),
                remote(lanes_e, from_w.at[2], east, row - 1, has_s, has_n),
                remote(lanes_w, from_e.at[0], west, row + 1, has_n, has_s),
                remote(lanes_e, from_w.at[0], east, row + 1, has_n, has_s)]

    row_group, late_group = rows_of(slice(0, 2)), rows_of(slice(2, 4))
    lane_group = [remote(pw, re.at[R0:R0 + NR, :], west, row, None, None),
                  remote(pe, rw.at[R0:R0 + NR, :], east, row, None, None),
                  remote(pe.at[0:1, :], rw.at[R0 + NR:R0 + NR + 1, :], east, row - 1, has_s, has_n),
                  remote(pw.at[NR - 1:NR, :], re.at[R0 - 1:R0, :], west, row + 1, has_n, has_s)]
    wide_group = wide_of(x, qw, qe, we, ww)
    force_group = wide_of(xf, fw, fe, fre, frw)

    edge = jnp.logical_or(row == 0, row == n_row - 1)

    @pl.when(edge)
    def _():
        pl.semaphore_wait(barrier, 5)

    @pl.when(jnp.logical_not(edge))
    def _():
        pl.semaphore_wait(barrier, 8)

    lane_p = lax.broadcasted_iota(jnp.int32, (PR, L), 1)
    lane = lane_p[:NR]

    for t in range(NT):
        bt[t, LEV, R0:R0 + NR, :] = zero((NR, L))
        bs[t, LEV, R0:R0 + NR, :] = zero((NR, L))
    for cp in flat_loads[3 * NT:]:
        cp.wait()
    for t in range(NT):
        count = cnt_i[t].astype(f32)
        bu[t, LEV, R0:R0 + NR, :] = count
        x[3, t, XO:XO + NR, :] = jnp.where(count > 0.0, bv[t, LEV, R0:R0 + NR, :], 0.0)

    def roll(a, shift):
        return pltpu.roll(a, shift, 1) if not (isinstance(shift, int) and shift % L == 0) else a

    pair = lax.shift_right_logical(lane, 1)
    packed = [zero((NR, L))] * 2
    for f, b in enumerate(bufs):
        edge_loads[2 * f].wait()
        edge_loads[2 * f + 1].wait()
        for k in range(SLOT):
            p = SLOT * (f % 2) + k
            both = jnp.where(lane == 0, b[0, k, R0:R0 + NR, :], b[NT - 1, k, R0:R0 + NR, :])
            packed[f // 2] = jnp.where(pair == p, roll(both, (2 * p + 1) % L), packed[f // 2])
    even = lax.rem(lane_p, 2) == 0
    pw[...] = jnp.where(even[:NR], roll(packed[1], L - 1), packed[0])
    pe[...] = jnp.where(even[:NR], packed[0], roll(packed[1], 1))
    start(lane_group)
    for cp in mid_loads:
        cp.wait()
    pack_rows((0, 1))
    start(row_group)
    pack_rows((2, 3))
    start(late_group)

    def pack_wide(b, n_fields):
        first = last = zero((NR, L))
        for f in range(n_fields):
            mine = (lane >= 32 * f) & (lane < 32 * f + 32)
            first = jnp.where(mine, roll(b[f, 0, XO:XO + NR, :], 32 * f), first)
            last = jnp.where(mine, roll(b[f, NT - 1, XO:XO + NR, :], (32 * f + 32) % L), last)
        return first, last

    for cp in flat_loads[:3 * NT]:
        cp.wait()
    first, last = pack_wide(x, 4)
    qw[...] = first
    qe[...] = last
    start(wide_group)
    for cp in scalar_loads:
        cp.wait()

    for f in range(4):
        for t in range(NT + 1):
            x[f, t, 0:8, :] = zero((8, L))
            x[f, t, XR - 16:XR, :] = zero((16, L))
    for t in range(NT + 1):
        tt[t, XR - 16:XR, :] = zero((16, L))
    for t in range(NT):
        for a in (xu, xv, xt, xs):
            a[t, 0] = zero((NR, L))

    @pl.when(jnp.logical_not(has_s))
    def _():
        rs[...] = zero((4, NT, SLOT, L))
        re[R0 - 8:R0, :] = zero((8, L))
        x[:, 0:NT, 8:XO, :] = zero((4, NT, NR, L))
        xf[:, 0:NT, 8:XO, :] = zero((2, NT, NR, L))
        for a in (we, ww, fre, frw):
            a[0] = zero((NR, L))

    @pl.when(jnp.logical_not(has_n))
    def _():
        rn[...] = zero((4, NT, SLOT, L))
        rw[R0 + NR:R0 + NR + 8, :] = zero((8, L))
        x[:, 0:NT, XO + NR:XO + 2 * NR, :] = zero((4, NT, NR, L))
        xf[:, 0:NT, XO + NR:XO + 2 * NR, :] = zero((2, NT, NR, L))
        for a in (we, ww, fre, frw):
            a[2] = zero((NR, L))


    row_pos = (row * NR + lax.broadcasted_iota(jnp.int32, (NR, L), 0)).astype(f32)
    total_rows = NR * n_row
    fu4[...] = 0.25 * (CORIO_F0 + CORIO_BETA * ((row_pos + 0.5) / total_rows - 0.5))
    fv4[...] = 0.25 * (CORIO_F0 + CORIO_BETA * ((row_pos + 1.0) / total_rows - 0.5))

    def to_east(tiles, halo, ts=range(NT)):
        last_lane = lane_p[:tiles[ts[0]].shape[0]] == L - 1
        rolled = {t: halo if t == NT else roll(tiles[t], L - 1) for t in sorted({t + d for t in ts for d in (0, 1)})}
        return {t: jnp.where(last_lane, rolled[t + 1], rolled[t]) for t in ts}

    def to_west(tiles, halo, ts=range(NT)):
        first_lane = lane_p[:tiles[ts[0]].shape[0]] == 0
        rolled = {t: halo if t < 0 else roll(tiles[t], 1) for t in sorted({t + d for t in ts for d in (-1, 0)})}
        return {t: jnp.where(first_lane, rolled[t - 1], rolled[t]) for t in ts}

    def side(f, k, lo=R0, n=NR):
        return pltpu.roll(ha[f // 2, lo:lo + n, :], lax.rem(L - 2 * (SLOT * (f % 2) + k), L), 1)

    def level(b, k, lo=R0, n=NR):
        return [b[t, k, lo:lo + n, :] for t in range(NT)]

    def each_level(fn, unroll):
        def some(i, _):
            base = i * unroll
            for j in range(unroll):
                fn(base + j, base + j - 1 if j else jnp.maximum(base - 1, 0), j % 2)
            return 0

        lax.fori_loop(0, -(-LEV // unroll), some, 0)

    p_scale = BC_GRAVITY / LEV

    def pressure(lo, n):
        total = zero((NT, n, L))
        for k in range(LEV):
            density = CONTRACT_S * bs[:, k, lo:lo + n, :] - EXPAND_T * bt[:, k, lo:lo + n, :]
            total = total + density
            bp[:, k, lo:lo + n, :] = p_scale * (total - 0.5 * density)
        bp[:, LEV, lo:lo + n, :] = zero((NT, n, L))

    pressure(R0, NR)
    for k in range(LEV):
        bp[:, k, R0 + NR:R0 + NR + 8, :] = zero((NT, 8, L))

    def momentum_down(ts, k, prev, slot):
        scale, carry = tab_s[k], tab_s[SLOT + k]
        u5, v5 = level(bu, k, R0, NR + 8), level(bv, k, R0 - 8, NR + 8)
        u_side = v_side = p_side = jnp.zeros((NR + 8, L), f32)
        if 0 in ts:
            u_side, v_side = side(0, k, R0, NR + 8), side(1, k, R0 - 8, NR + 8)
            p_side = pltpu.roll(rp[...], L - 1 - 2 * k, 1)
        uw, ve = to_west(u5, u_side, ts), to_east(v5, v_side, ts)
        um, vm = [a[:NR] for a in u5], [a[8:] for a in v5]
        ue, vw = to_east(um, u_side[:NR], ts), to_west(vm, v_side[8:], ts)
        pm, pn = level(bp, k), level(bp, k, R0 + 1)
        pe_ = to_east(pm, p_side, ts)
        for t in ts:
            u_sum, v_sum = u5[t] + uw[t], v5[t] + ve[t]
            s1[slot, t] = u_sum
            s2[slot, t] = v_sum
            ub4 = u_sum[:NR] + s1[slot, t, 1:NR + 1, :]
            vb4 = v_sum[8:] + s2[slot, t, 7:NR + 7, :]
            un, us = bu[t, k, R0 + 1:R0 + 1 + NR, :], bu[t, k, R0 - 1:R0 - 1 + NR, :]
            vn, vs = bv[t, k, R0 + 1:R0 + 1 + NR, :], bv[t, k, R0 - 1:R0 - 1 + NR, :]
            u_star = um[t] + vb4 * (fu4[...] - 0.125 * (un - us)) - um[t] * (0.5 * (ue[t] - uw[t][:NR])) + (pm[t] - pe_[t])
            v_star = vm[t] - ub4 * (fv4[...] + 0.125 * (ve[t][8:] - vw[t])) - vm[t] * (0.5 * (vn - vs)) + (pm[t] - pn[t])
            xu[t, k] = scale * u_star + carry * xu[t, prev]
            xv[t, k] = scale * v_star + carry * xv[t, prev]

    arrive(lane_group)
    ha[0] = jnp.where(even, rw[...], roll(re[...], L - 2))
    ha[1] = jnp.where(even, roll(rw[...], L - 1), roll(re[...], L - 1))
    east_ = roll(ha[1, R0:R0 + NR, :], 1)
    density = CONTRACT_S * roll(east_, L // 2) - EXPAND_T * east_
    total = density
    for step in (2, 4, 8, 16, 32):
        total = total + jnp.where(lane >= step, roll(total, step), 0.0)
    rp[...] = p_scale * (total - 0.5 * density)
    arrive(row_group)
    unpack_rows((0, 1))
    each_level(functools.partial(momentum_down, tuple(range(NT))), UNROLL_M)

    arrive(late_group)
    unpack_rows((2, 3))
    last_row = lax.broadcasted_iota(jnp.int32, (NT, 8, L), 1) == 7
    pressure(R0 + NR, 8)
    sweep = zero((NT, 8, L))
    for k in range(LEV):
        sweep = tab_s[SLOT + k] * sweep - tab_s[k] * bp[:, k, R0 + NR - 7:R0 + NR + 1, :]
        xv[:, k, NR - 8:NR, :] += jnp.where(last_row, sweep, 0.0)

    c_mid, d_mid = level(bu, LEV), level(bv, LEV)
    c_east = to_east(c_mid, side(0, LEV))
    d_east = to_east(d_mid, side(1, LEV))
    c_north, c_south = level(bu, LEV, R0 + 1), level(bu, LEV, R0 - 1)
    d_north = level(bv, LEV, R0 + 1)
    for t in range(NT):
        cu[t] = jnp.minimum(c_mid[t], c_east[t])
        cv[t] = jnp.minimum(c_mid[t], c_north[t])
        hu[t] = 0.5 * (d_mid[t] + d_east[t])
        hv[t] = 0.5 * (d_mid[t] + d_north[t])
        cc_o[t] = c_mid[t]
    c_west0 = jnp.minimum(side(0, LEV), c_mid[0])

    def momentum_up(i, _):
        t = pl.ds(2 * i, 2)
        z = zero((2, NR, L))
        state = [[z, z, z], [z, z, z]]
        for k in range(LEV - 1, -1, -1):
            link, last_ = tab_s[2 * SLOT + k], tab_s[3 * SLOT + k]
            for q, (sweep, b, count) in enumerate(((xu, bu, cu), (xv, bv, cv))):
                below, sum_x, sum_0 = state[q]
                value = sweep[t, k]
                active = count[t] > float(k)
                solved = jnp.where(count[t] > float(k + 1), value + link * below, jnp.where(active, last_ * value, 0.0))
                sweep[t, k] = solved
                start_ = jnp.where(active, b[t, k, R0:R0 + NR, :], 0.0)
                b[t, k, R0:R0 + NR, :] = start_
                state[q] = [solved, sum_x + solved, sum_0 + start_]
        for q, (h, mean, count) in enumerate(((hu, su, cu), (hv, sv, cv))):
            _, total, start_ = state[q]
            n_active = jnp.maximum(count[t], 1.0)
            mean[t] = total / n_active
            xf[q, t, XO:XO + NR, :] = h[t] * (total - start_) / n_active / TIME_STEP
        c_south = jnp.minimum(bu[t, LEV, 0:8, :], bu[t, LEV, 1:9, :])
        for k in range(LEV):
            bv[t, k, 0:8, :] = jnp.where(c_south > float(k), bv[t, k, 0:8, :], 0.0)
        return 0

    lax.fori_loop(0, NT // 2, momentum_up, 0)

    first, last = pack_wide(xf, 2)
    fw[...] = first
    fe[...] = last
    start(force_group)

    def tracer_down(k, prev, slot):
        scale, carry = tab_s[4 * SLOT + k], tab_s[5 * SLOT + k]
        kf = lax.convert_element_type(k, f32)
        um, vm, vs = level(bu, k), level(bv, k), level(bv, k, R0 - 1)
        uw0 = jnp.where(c_west0 > kf, side(0, k), 0.0)
        for f, b, sweep in ((2, bt, xt), (3, bs, xs)):
            q = level(b, k)
            q_side = side(f, k)
            qe_ = to_east(q, q_side)
            f_east = [um[t] * (q[t] + qe_[t]) for t in range(NT)]
            f_west = to_west(f_east, uw0 * (q_side + q[0]))
            for t in range(NT):
                f_north = vm[t] * (q[t] + b[t, k, R0 + 1:R0 + 1 + NR, :])
                f_south = vs[t] * (b[t, k, R0 - 1:R0 - 1 + NR, :] + q[t])
                new = q[t] - 0.5 * TIME_STEP * (f_east[t] - f_west[t] + f_north - f_south)
                sweep[t, k] = jnp.where(bu[t, LEV, R0:R0 + NR, :] > kf, scale * new + carry * sweep[t, prev], new)

    each_level(tracer_down, UNROLL_T)

    arrive(wide_group)
    drain(wide_group)
    arrive(force_group)

    def unpack_wide(b, from_e, from_w, n_fields):
        for f in range(n_fields):
            for seg in range(3):
                b[f, NT, 8 + NR * seg:8 + NR * seg + NR, :] = jnp.where(lane < L // 2, roll(from_e[seg], (L - 32 * f) % L), roll(from_w[seg], (96 - 32 * f) % L))

    unpack_wide(x, we, ww, 4)
    unpack_wide(xf, fre, frw, 2)
    dt_fast = TIME_STEP / n_sub
    XT = NT + 1

    def ring_east(tiles, last_lane):
        rolled = [roll(a, L - 1) for a in tiles]
        return [jnp.where(last_lane, rolled[(t + 1) % XT], rolled[t]) for t in range(XT)]

    def ring_west(tiles, first_lane):
        rolled = [roll(a, 1) for a in tiles]
        return [jnp.where(first_lane, rolled[(t - 1) % XT], rolled[t]) for t in range(XT)]

    for seg in range(3):
        lo = 8 + NR * seg
        pos = (row * NR + NR * (seg - 1) + lax.broadcasted_iota(jnp.int32, (NR, L), 0)).astype(f32)
        f_u = CORIO_F0 + CORIO_BETA * ((pos + 0.5) / total_rows - 0.5)
        f_v = CORIO_F0 + CORIO_BETA * ((pos + 1.0) / total_rows - 0.5)
        d = [x[3, t, lo:lo + NR, :] for t in range(XT)]
        d_e = ring_east(d, lane == L - 1)
        for t in range(XT):
            d_n = x[3, t, lo + 1:lo + 1 + NR, :]
            wet = jnp.where((d[t] > 0.0) & (d_e[t] > 0.0), 1.0, 0.0)
            cm[t, lo:lo + NR, :] = wet
            ca[t, lo:lo + NR, :] = (0.25 * dt_fast) * f_u * wet
            cb[t, lo:lo + NR, :] = (dt_fast * GRAVITY * 0.5) * (d[t] + d_e[t]) * wet
            cc[t, lo:lo + NR, :] = dt_fast * xf[0, t, lo:lo + NR, :] * wet
            wet = jnp.where((d[t] > 0.0) & (d_n > 0.0), 1.0, 0.0)
            cn[t, lo:lo + NR, :] = wet
            cd[t, lo:lo + NR, :] = (0.25 * dt_fast) * f_v * wet
            cg[t, lo:lo + NR, :] = (dt_fast * GRAVITY * 0.5) * (d[t] + d_n) * wet
            ch[t, lo:lo + NR, :] = dt_fast * xf[1, t, lo:lo + NR, :] * wet

    for t in range(NT):
        au[t] = zero((NR, L))
        av[t] = zero((NR, L))

    def subcycle(side_rows, masked, n, _):
        weight = w_s[n]
        parts = ((XO - side_rows, side_rows), (XO, NR), (XO + NR, side_rows))
        for r, chunk in parts:
            first_lane = lane[:chunk] == 0
            u_t = [x[1, t, r:r + chunk, :] for t in range(XT)]
            u_w = ring_west(u_t, first_lane)
            for t in range(XT):
                v_t, v_s = x[2, t, r:r + chunk, :], x[2, t, r - 1:r - 1 + chunk, :]
                x[0, t, r:r + chunk, :] = x[0, t, r:r + chunk, :] - dt_fast * ((u_t[t] - u_w[t]) + (v_t - v_s))
                tt[t, r:r + chunk, :] = u_t[t] + u_w[t]
        for r, chunk in parts[::-1]:
            last_lane = lane[:chunk] == L - 1
            e_t = [x[0, t, r:r + chunk, :] for t in range(XT)]
            e_e = ring_east(e_t, last_lane)
            v_t = [x[2, t, r:r + chunk, :] for t in range(XT)]
            s_t = [v_t[t] + x[2, t, r - 1:r - 1 + chunk, :] for t in range(XT)]
            s_e = ring_east(s_t, last_lane)
            for t in range(XT):
                at = (t, slice(r, r + chunk))
                up = (t, slice(r + 1, r + 1 + chunk))
                e_n = x[0, t, r + 1:r + 1 + chunk, :]
                u_old = x[1, t, r:r + chunk, :] if masked else cm[at] * x[1, t, r:r + chunk, :]
                v_old = v_t[t] if masked else cn[at] * v_t[t]
                u_new = u_old + ca[at] * (s_t[t] + s_e[t]) + cc[at] - cb[at] * (e_e[t] - e_t[t])
                v_new = v_old - cd[at] * (tt[at] + tt[up]) + ch[at] - cg[at] * (e_n - e_t[t])
                x[1, t, r:r + chunk, :] = u_new
                x[2, t, r:r + chunk, :] = v_new
                if r == XO and t < NT:
                    au[t] += weight * u_new
                    av[t] += weight * v_new
        return 0

    done = 0
    for tiles in (4, 3, 2, 1):
        until = n_sub - 8 * (tiles - 1)
        stretch = functools.partial(subcycle, 8 * tiles)
        if done == 0:
            stretch(False, 0, 0)
            stretch(True, 1, 0)
            done = 2

        def two(i, _, stretch=stretch, done=done):
            stretch(True, done + 2 * i, 0)
            stretch(True, done + 2 * i + 1, 0)
            return 0

        lax.fori_loop(0, (until - done) // 2, two, 0)
        for n in range(done + (until - done) // 2 * 2, until):
            stretch(True, n, 0)
        done = until

    for t in range(NT):
        eta_o[t] = x[0, t, XO:XO + NR, :]
        tu_o[t] = x[1, t, XO:XO + NR, :]
        tv_o[t] = x[2, t, XO:XO + NR, :]
        gu_o[t] = au[t] / hu[t] - su[t]
        gv_o[t] = av[t] / hv[t] - sv[t]

    for group in (row_group, late_group, lane_group, force_group):
        drain(group)


def final_kernel(tab_s, xu, xv, xt, xs, gu, gv, cu, cv, cc, eta, tu, tv, eta_h, tu_h, tv_h, u_h, v_h, t_h, s_h, flat_b, u_b, v_b, t_b, s_b, sem):
    xu, xv, xt, xs = [a.at[:, 0:SLOT, 0:NR, :] for a in (xu, xv, xt, xs)]
    gu, gv, cu, cv, cc, eta, tu, tv = [a.at[:, 0:NR, :] for a in (gu, gv, cu, cv, cc, eta, tu, tv)]
    stores = []
    for i, (a, o) in enumerate(((eta, eta_h), (tu, tu_h), (tv, tv_h))):
        for t in range(NT):
            flat_b[i, :, L * t:L * t + L] = a[t]
        stores.append(pltpu.make_async_copy(flat_b.at[i], o, sem.at[4, i]))
        stores[-1].start()

    below = [[jnp.zeros((NR, L), f32)] * NT for _ in range(2)]
    top = LEV
    for k in range(LEV - 1, -1, -1):
        link, last = tab_s[6 * SLOT + k], tab_s[7 * SLOT + k]
        for t in range(NT):
            cols = slice(L * t, L * t + L)
            u_b[k, :, cols] = jnp.where(cu[t] > float(k), xu[t, k] + gu[t], 0.0)
            v_b[k, :, cols] = jnp.where(cv[t] > float(k), xv[t, k] + gv[t], 0.0)
            for q, (sweep, b) in enumerate(((xt, t_b), (xs, s_b))):
                value = sweep[t, k]
                solved = jnp.where(cc[t] > float(k + 1), value + link * below[q][t], jnp.where(cc[t] > float(k), last * value, value))
                below[q][t] = solved
                b[k, :, cols] = solved
        if k in GROUPS:
            for i, (b, o) in enumerate(((u_b, u_h), (v_b, v_h), (t_b, t_h), (s_b, s_h))):
                stores.append(pltpu.make_async_copy(b.at[k:top], o.at[k:top], sem.at[i, GROUPS.index(k)]))
                stores[-1].start()
            top = k
    for cp in stores:
        cp.wait()


def solution(mesh):
    n_col = mesh.shape['col']
    n_row = mesh.shape['row']

    def step(vel_u, vel_v, value_a11, salinity, surf_eta, trans_u, trans_v, bottom_depth, level_count, avg_weights):
        n_sub = avg_weights.shape[0]
        table = jnp.asarray(solve_table(LEV))
        hbm = pl.BlockSpec(memory_space=pltpu.HBM)
        vmem = pl.BlockSpec(memory_space=pltpu.VMEM)
        smem = pl.BlockSpec(memory_space=pltpu.SMEM)
        V = pltpu.VMEM
        tile = V((NT, RA, L), f32)
        sweep = V((NT, KA, RA, L), f32)
        wide = (NT + 1, XR, L)
        scratch = ([V((NT, KA, PR, L), f32)] * 5 + [V((NT, NR, L), jnp.int32), V((NR, L), f32)]
                   + [V((2, NT, NR + 8, L), f32)] * 2 + [V((4, NT, SLOT, L), f32)] * 4 + [V((NR, L), f32)] * 2 + [V((PR, L), f32)] * 2 + [V((2, PR, L), f32)]
                   + [V((4,) + wide, f32), V((2,) + wide, f32)] + [V((NR, L), f32)] * 2 + [V((3, NR, L), f32)] * 2
                   + [V((NR, L), f32)] * 2 + [V((3, NR, L), f32)] * 2
                   + [V((NR, L), f32)] * 2 + [tile] * 4
                   + [V(wide, f32)] * 9 + [tile] * 2
                   + [pltpu.SMEM((n_sub,), f32), pltpu.SMEM((8 * SLOT,), f32)]
                   + [pltpu.SemaphoreType.DMA((40,)), pltpu.SemaphoreType.DMA((64,)), pltpu.SemaphoreType.DMA((64,))])
        outs = pl.pallas_call(
            functools.partial(ocean_kernel, tuple(mesh.axis_names), n_col, n_row, n_sub),
            out_shape=[tile] * 8 + [sweep] * 4,
            in_specs=[hbm] * 11,
            out_specs=[vmem] * 12,
            scratch_shapes=scratch,
            compiler_params=pltpu.CompilerParams(collective_id=0, has_side_effects=True, vmem_limit_bytes=40 * 1024 * 1024),
        )(*[pltpu.with_memory_space_constraint(a, pltpu.HBM) for a in (vel_u, vel_v, value_a11, salinity, surf_eta, trans_u, trans_v, bottom_depth, level_count, avg_weights, table)])
        eta, tu, tv, gu, gv, cu, cv, cc, xu, xv, xt, xs = [pltpu.with_memory_space_constraint(o, pltpu.VMEM) for o in outs]

        cube = jax.ShapeDtypeStruct((LEV, NR, NC), f32)
        flat = jax.ShapeDtypeStruct((NR, NC), f32)
        return tuple(pl.pallas_call(
            final_kernel,
            out_shape=[flat] * 3 + [cube] * 4,
            in_specs=[smem] + [vmem] * 12,
            out_specs=[hbm] * 7,
            scratch_shapes=[V((3, NR, NC), f32)] + [V((LEV, NR, NC), f32)] * 4 + [pltpu.SemaphoreType.DMA((5, len(GROUPS)))],
            compiler_params=pltpu.CompilerParams(vmem_limit_bytes=24 * 1024 * 1024),
        )(table, xu, xv, xt, xs, gu, gv, cu, cv, cc, eta, tu, tv))

    cube = P(None, 'row', 'col')
    flat = P('row', 'col')
    return jax.shard_map(step, mesh=mesh, in_specs=(cube, cube, cube, cube, flat, flat, flat, flat, flat, P()), out_specs=(flat, flat, flat, cube, cube, cube, cube), check_vma=False)
```
